256 devices in a mesh: view: 16 (over z, core), tile: 16 (over y, x).
Axes of the slice: x: 4, y: 4, z: 8, core: 2. Of those that a mesh axis runs over, the one named last changes fastest.
Arguments:
- params: float32 [59, 262144], P(None, ('view', 'tile')), may hold values from -25 to 25, as said below
- first: float32 [59, 262144], P(None, ('view', 'tile')), may hold values from -0.3 to 0.3
- second: float32 [59, 262144], P(None, ('view', 'tile')), may hold values from 0.0001 to 0.01
- visible: int32 [16, 16384], P(None, ('view', 'tile')), may hold values from 0 to 1023, as said below
- cameras: float32 [16, 11], replicated, as said below
- tile_lists: int32 [16, 32, 1024], P('view', 'tile'), may hold values from 0 to 16383
- tile_blocks: int32 [16, 32], P('view', 'tile'), may hold values from 1 to 8, as said below
- targets: float32 [16, 3, 8192], P('view', None, 'tile'), may hold values from 0 to 1
Outputs:
- new_params: float32 [59, 262144], P(None, ('view', 'tile'))
- new_first: float32 [59, 262144], P(None, ('view', 'tile'))
- new_second: float32 [59, 262144], P(None, ('view', 'tile'))
- rendered: float32 [16, 3, 8192], P('view', None, 'tile')
The draws below stay inside these ranges and needn't reach their ends.
Inputs may be any that keep to these rules, and one draw needn't show every extreme that they name: `visible`: for each view and each owner (a run of 64 entries), distinct local columns of that owner. `tile_blocks`: number of live blocks of 128 entries at the head of each tile's list; the first tile of every view has all 8. `params`: rows 0 to 2 in -25 to 25; rows 3 to 5 in -6 to 2.5; row 6 in 1 to 2; rows 7 to 9 in -1 to 1; row 10 in -7.5 to -5.5; rows 11 to 58 in -1.2 to 1.2. `cameras`: column 0 in 0.5 to 1, columns 1 to 3 in -1 to 1, columns 4 and 5 in -0.3 to 0.3, column 6 in 6 to 9; focal lengths 0.7 to 1.1 times the larger side of the window of 128 by 64 pixels; the principal point within 8 pixels of the window's middle.
All inputs are finite; a program needn't handle non-finite values.
Results may differ from the reference program's by a relative error of at most 0.0003.
Values sent between devices are 32-bit elements; how exact they have to be, the bound alone decides.
No kernel may reach another device: no remote copies, remote signals or barrier semaphores. Data moves between devices by JAX's collectives and lax.ppermute only.
A program may use at most 128 MiB of HBM per device.

```python
import math
import jax
import jax.numpy as jnp
from jax import lax

PARAMS = 59
SIDE = 16
PIX = 256
BLOCK = 128
BLOCKS = 8
WIN_COLS = 8
G_DEV = 1024
VIS_OWN = 64
TILES_DEV = 2
VIEWS = 16
OWNERS = 256
G_ALL = 262144
V_VIEW = 16384
TILES = 32
LIST = 1024
N_TILE = 16


reach_float = (2.0, 6.0, 20.0, 60.0)


reach_whole = (2, 6, 20, 60)


def window_sides():
    return (SIDE * WIN_COLS, SIDE * ((TILES + WIN_COLS - 1) // WIN_COLS))


def turn_matrix(real_part, axis_one, axis_two, axis_three):
    inverse = jax.lax.rsqrt(real_part * real_part + axis_one * axis_one + axis_two * axis_two + axis_three * axis_three)
    real_unit = real_part * inverse
    unit_one = axis_one * inverse
    unit_two = axis_two * inverse
    unit_three = axis_three * inverse
    return ((1.0 - 2.0 * (unit_two * unit_two + unit_three * unit_three), 2.0 * (unit_one * unit_two - real_unit * unit_three), 2.0 * (unit_one * unit_three + real_unit * unit_two)), (2.0 * (unit_one * unit_two + real_unit * unit_three), 1.0 - 2.0 * (unit_one * unit_one + unit_three * unit_three), 2.0 * (unit_two * unit_three - real_unit * unit_one)), (2.0 * (unit_one * unit_three - real_unit * unit_two), 2.0 * (unit_two * unit_three + real_unit * unit_one), 1.0 - 2.0 * (unit_one * unit_one + unit_two * unit_two)))


def camera_table(key):
    keys = jax.random.split(jax.random.fold_in(key, 11), 6)
    width, height = window_sides()
    larger = 1.0 * max(width, height)
    real_part = jax.random.uniform(keys[0], (VIEWS, 1), jnp.float32, 0.5, 1.0)
    axes_part = jax.random.uniform(keys[1], (VIEWS, 3), jnp.float32, -1.0, 1.0)
    shift_side = jax.random.uniform(keys[2], (VIEWS, 2), jnp.float32, -0.3, 0.3)
    shift_depth = jax.random.uniform(keys[3], (VIEWS, 1), jnp.float32, 6.0, 9.0)
    focal = jax.random.uniform(keys[4], (VIEWS, 2), jnp.float32, 0.7, 1.1) * larger
    centre = jnp.array([0.5 * width, 0.5 * height], jnp.float32) + jax.random.uniform(keys[5], (VIEWS, 2), jnp.float32, -8.0, 8.0)
    return jnp.concatenate([real_part, axes_part, shift_side, shift_depth, focal, centre], axis=1)


def layout(key):
    keys = jax.random.split(jax.random.fold_in(key, 12), 5)
    width, height = window_sides()
    shuffled = jax.vmap(lambda single: jax.random.permutation(single, G_DEV))(jax.random.split(keys[0], OWNERS)).astype(jnp.int32)
    across = jax.random.randint(keys[1], (VIEWS, V_VIEW), 0, width, jnp.int32)
    downward = jax.random.randint(keys[2], (VIEWS, V_VIEW), 0, height, jnp.int32)
    kinds = jax.random.randint(keys[3], (VIEWS, V_VIEW), 0, 4, jnp.int32)
    depth_rank = jax.vmap(lambda single: jax.random.permutation(single, V_VIEW))(jax.random.split(keys[4], VIEWS)).astype(jnp.int32)
    return (shuffled, across, downward, kinds, depth_rank)


def draw_cameras(key, part):
    return camera_table(key)


def draw_visible(key, part):
    shuffled, across, downward, kinds, depth_rank = layout(key)
    chosen = shuffled[:, :VIEWS * VIS_OWN].reshape(OWNERS, VIEWS, VIS_OWN)
    return jnp.transpose(chosen, (1, 0, 2)).reshape(VIEWS, OWNERS * VIS_OWN).astype(jnp.int32)


def draw_tile_lists(key, part):
    shuffled, across, downward, kinds, depth_rank = layout(key)
    tie_keys = jax.random.split(jax.random.fold_in(key, 15), VIEWS)
    reach_table = jnp.array(reach_whole, jnp.int32)
    tiles = jnp.arange(TILES, dtype=jnp.int32)
    left_edge = (SIDE * (tiles % WIN_COLS))[:, None]
    top_edge = (SIDE * (tiles // WIN_COLS))[:, None]

    def one_view(inputs):
        row_x, row_y, row_kind, row_rank, tie_key = inputs
        gap_x = jnp.maximum(jnp.maximum(left_edge - row_x[None, :], row_x[None, :] - (left_edge + SIDE - 1)), 0)
        gap_y = jnp.maximum(jnp.maximum(top_edge - row_y[None, :], row_y[None, :] - (top_edge + SIDE - 1)), 0)
        reach = jnp.take(reach_table, row_kind)
        nearness = jnp.minimum((gap_x * gap_x + gap_y * gap_y) * 64 // (reach * reach)[None, :], 16383)
        ties = jax.random.randint(tie_key, (TILES, V_VIEW), 0, 32768, jnp.int32)
        order = jnp.argsort(nearness * 32768 + ties, axis=1, stable=True)[:, :LIST]
        depth = jnp.take(row_rank, order)
        resort = jnp.argsort(depth, axis=1, stable=True)
        return jnp.take_along_axis(order, resort, axis=1).astype(jnp.int32)
    return lax.map(one_view, (across, downward, kinds, depth_rank, tie_keys)).astype(jnp.int32)


def draw_params(key, part):
    shuffled, across, downward, kinds, depth_rank = layout(key)
    cameras = camera_table(key)
    keys = jax.random.split(jax.random.fold_in(key, 13), 8)
    slot_of = jnp.argsort(shuffled, axis=1).reshape(-1).astype(jnp.int32)
    column = jnp.arange(G_ALL, dtype=jnp.int32)
    owner_index = column // G_DEV
    per_view = OWNERS // VIEWS
    is_seen = slot_of < VIEWS * VIS_OWN
    row_index = owner_index % per_view * (VIEWS * VIS_OWN) + owner_index // per_view * VIS_OWN + slot_of % VIS_OWN
    view_index = jnp.where(is_seen, slot_of // VIS_OWN, 0)
    row_index = jnp.where(is_seen, row_index, column % V_VIEW)
    spot_x = across[view_index, row_index].astype(jnp.float32) + jax.random.uniform(keys[0], (G_ALL,), jnp.float32, 0.0, 1.0)
    spot_y = downward[view_index, row_index].astype(jnp.float32) + jax.random.uniform(keys[1], (G_ALL,), jnp.float32, 0.0, 1.0)
    depth = 5.0 + 5.0 * (depth_rank[view_index, row_index].astype(jnp.float32) + 0.5) / V_VIEW
    camera = cameras[view_index]
    turn = turn_matrix(camera[:, 0], camera[:, 1], camera[:, 2], camera[:, 3])
    local_point = ((spot_x - camera[:, 9]) * depth / camera[:, 7] - camera[:, 4], (spot_y - camera[:, 10]) * depth / camera[:, 8] - camera[:, 5], depth - camera[:, 6])
    position = jnp.stack([turn[0][axis_at] * local_point[0] + turn[1][axis_at] * local_point[1] + turn[2][axis_at] * local_point[2] for axis_at in range(3)])
    reach = jnp.take(jnp.array(reach_float, jnp.float32), kinds[view_index, row_index]) * jnp.exp(jax.random.uniform(keys[2], (G_ALL,), jnp.float32, -0.2231, 0.2231))
    base_scale = jnp.log(reach * depth / jnp.sqrt(camera[:, 7] * camera[:, 8]))
    scales = base_scale[None, :] + jax.random.uniform(keys[3], (3, G_ALL), jnp.float32, -0.15, 0.15)
    opacity = jax.random.uniform(keys[4], (1, G_ALL), jnp.float32, -7.5, -5.5)
    colour = jnp.clip(0.3 * jax.random.normal(keys[5], (48, G_ALL), jnp.float32), -1.2, 1.2)
    real_part = jax.random.uniform(keys[6], (1, G_ALL), jnp.float32, 1.0, 2.0)
    others = jax.random.uniform(keys[7], (3, G_ALL), jnp.float32, -1.0, 1.0)
    return jnp.concatenate([position, scales, real_part, others, opacity, colour], axis=0)


def draw_tile_blocks(key, part):
    keys = jax.random.split(jax.random.fold_in(key, 14), 3)
    counts = jax.random.randint(keys[0], (VIEWS, TILES), 1, BLOCKS + 1, jnp.int32)
    others = jax.random.randint(keys[1], (VIEWS, TILES), 1, BLOCKS + 1, jnp.int32)
    heavy = jax.random.randint(keys[2], (VIEWS, TILES // TILES_DEV, 1), 0, 2, jnp.int32)
    heavy = jnp.broadcast_to(heavy, (VIEWS, TILES // TILES_DEV, TILES_DEV)).reshape(VIEWS, TILES)
    counts = jnp.where(heavy > 0, jnp.maximum(counts, others), jnp.minimum(counts, others))
    return counts.at[:, 0].set(BLOCKS).astype(jnp.int32)


def block_levels(key, shape, pieces, least, largest):
    def one(dim, blocks):
        heights = jax.random.uniform(jax.random.fold_in(jax.random.fold_in(key, 6), dim), (blocks,), jnp.float32, least / len(pieces), largest / len(pieces))
        return jnp.repeat(jnp.exp(heights), shape[dim] // blocks).reshape((-1,) + (1,) * (len(shape) - dim - 1))

    factor_of = one(*pieces[0])
    for cut in pieces[1:]:
        factor_of = factor_of * one(*cut)
    return factor_of


def centred(own_key, dims, scale, limit, cuts=(), held_as=jnp.bfloat16):
    level = block_levels(own_key, dims, cuts, -0.22, 0.18) if cuts else 1.0
    drawn = jax.random.normal(own_key, dims, jnp.float32) * scale * level
    return jnp.minimum(jnp.maximum(drawn, -limit), limit).astype(held_as)


def setup_inputs(seed: int = 0) -> dict:
    key_list = jax.random.split(jax.random.key(seed), 9)
    return {
        "params": draw_params(jax.random.fold_in(key_list[8], 71), 0),
        "first": centred(key_list[1], (PARAMS, G_ALL), 0.05, 0.3, ((1, 256),), jnp.float32),
        "second": jnp.clip(jnp.exp(math.log(0.01) - 4.6051702 * jax.random.uniform(key_list[2], (PARAMS, G_ALL), jnp.float32) ** block_levels(key_list[2], (PARAMS, G_ALL), ((1, 256),), -0.2, 0.2)), 0.0001, 0.01),
        "visible": draw_visible(jax.random.fold_in(key_list[8], 71), 0),
        "cameras": draw_cameras(jax.random.fold_in(key_list[8], 71), 0),
        "tile_lists": draw_tile_lists(jax.random.fold_in(key_list[8], 71), 0),
        "tile_blocks": draw_tile_blocks(jax.random.fold_in(key_list[8], 71), 0),
        "targets": jnp.clip(1.0 * jax.random.uniform(key_list[7], (VIEWS, 3, TILES * PIX), jnp.float32) ** block_levels(key_list[7], (VIEWS, 3, TILES * PIX), ((0, 16), (2, 16)), -0.2, 0.2), 0.0, 1.0),
    }


harm_zero = 0.28209479177387814
harm_one = 0.4886025119029199
harm_two = (1.0925484305920792, -1.0925484305920792, 0.31539156525252005, -1.0925484305920792, 0.5462742152960396)
harm_three = (-0.5900435899266435, 2.890611442640554, -0.4570457994644658, 0.3731763325901154, -0.4570457994644658, 1.445305721320277, -0.5900435899266435)
learn_rate = 0.05
beta_first = 0.9
beta_second = 0.999
adam_eps = 1e-08
blur_add = 0.3

def rotation(real_part, axis_one, axis_two, axis_three):
    inverse = lax.rsqrt(real_part * real_part + axis_one * axis_one + axis_two * axis_two + axis_three * axis_three)
    real_unit = real_part * inverse
    unit_one = axis_one * inverse
    unit_two = axis_two * inverse
    unit_three = axis_three * inverse
    return ((1.0 - 2.0 * (unit_two * unit_two + unit_three * unit_three), 2.0 * (unit_one * unit_two - real_unit * unit_three), 2.0 * (unit_one * unit_three + real_unit * unit_two)), (2.0 * (unit_one * unit_two + real_unit * unit_three), 1.0 - 2.0 * (unit_one * unit_one + unit_three * unit_three), 2.0 * (unit_two * unit_three - real_unit * unit_one)), (2.0 * (unit_one * unit_three - real_unit * unit_two), 2.0 * (unit_two * unit_three + real_unit * unit_one), 1.0 - 2.0 * (unit_one * unit_one + unit_two * unit_two)))

def harmonics(first_dir, second_dir, third_dir):
    sq_first = first_dir * first_dir
    sq_second = second_dir * second_dir
    sq_third = third_dir * third_dir
    return [harm_zero, -harm_one * second_dir, harm_one * third_dir, -harm_one * first_dir, harm_two[0] * first_dir * second_dir, harm_two[1] * second_dir * third_dir, harm_two[2] * (2.0 * sq_third - sq_first - sq_second), harm_two[3] * first_dir * third_dir, harm_two[4] * (sq_first - sq_second), harm_three[0] * second_dir * (3.0 * sq_first - sq_second), harm_three[1] * first_dir * second_dir * third_dir, harm_three[2] * second_dir * (4.0 * sq_third - sq_first - sq_second), harm_three[3] * third_dir * (2.0 * sq_third - 3.0 * sq_first - 3.0 * sq_second), harm_three[4] * first_dir * (4.0 * sq_third - sq_first - sq_second), harm_three[5] * third_dir * (sq_first - sq_second), harm_three[6] * first_dir * (sq_first - 3.0 * sq_second)]

def project(raw, camera):
    camera_turn = rotation(camera[0], camera[1], camera[2], camera[3])
    shift_vec = (camera[4], camera[5], camera[6])
    focal_x = camera[7]
    focal_y = camera[8]
    position = (raw[0], raw[1], raw[2])
    viewed = [camera_turn[across][0] * position[0] + camera_turn[across][1] * position[1] + camera_turn[across][2] * position[2] + shift_vec[across] for across in range(3)]
    inverse = 1.0 / viewed[2]
    mean_x = focal_x * viewed[0] * inverse + camera[9]
    mean_y = focal_y * viewed[1] * inverse + camera[10]
    gauss_turn = rotation(raw[6], raw[7], raw[8], raw[9])
    stretch = [jnp.exp(raw[3 + column]) for column in range(3)]
    jac_xx = focal_x * inverse
    jac_xz = -focal_x * viewed[0] * inverse * inverse
    jac_yy = focal_y * inverse
    jac_yz = -focal_y * viewed[1] * inverse * inverse
    leading_x = [jac_xx * camera_turn[0][column] + jac_xz * camera_turn[2][column] for column in range(3)]
    leading_y = [jac_yy * camera_turn[1][column] + jac_yz * camera_turn[2][column] for column in range(3)]
    axes_x = [(leading_x[0] * gauss_turn[0][column] + leading_x[1] * gauss_turn[1][column] + leading_x[2] * gauss_turn[2][column]) * stretch[column] for column in range(3)]
    axes_y = [(leading_y[0] * gauss_turn[0][column] + leading_y[1] * gauss_turn[1][column] + leading_y[2] * gauss_turn[2][column]) * stretch[column] for column in range(3)]
    cov_xx = axes_x[0] * axes_x[0] + axes_x[1] * axes_x[1] + axes_x[2] * axes_x[2] + blur_add
    cov_xy = axes_x[0] * axes_y[0] + axes_x[1] * axes_y[1] + axes_x[2] * axes_y[2]
    cov_yy = axes_y[0] * axes_y[0] + axes_y[1] * axes_y[1] + axes_y[2] * axes_y[2] + blur_add
    determ = cov_xx * cov_yy - cov_xy * cov_xy
    opacity = jax.nn.sigmoid(raw[10])
    camera_eye = [-(camera_turn[0][column] * shift_vec[0] + camera_turn[1][column] * shift_vec[1] + camera_turn[2][column] * shift_vec[2]) for column in range(3)]
    offset = [position[column] - camera_eye[column] for column in range(3)]
    length = lax.rsqrt(offset[0] * offset[0] + offset[1] * offset[1] + offset[2] * offset[2])
    harmonic_terms = harmonics(offset[0] * length, offset[1] * length, offset[2] * length)
    colours = []
    for channel in range(3):
        total = 0.5 + jnp.zeros_like(opacity)
        for harmonic in range(16):
            total = total + raw[11 + 16 * channel + harmonic] * harmonic_terms[harmonic]
        colours.append(total)
    return jnp.stack([mean_x, mean_y, cov_yy / determ, -cov_xy / determ, cov_xx / determ, opacity] + colours)

def composite(rows, anchor_x, anchor_y, count, lazy):
    pixel = jnp.arange(PIX, dtype=jnp.int32)
    pixel_x = (anchor_x + (pixel % SIDE).astype(jnp.float32) + 0.5)[:, None]
    pixel_y = (anchor_y + (pixel // SIDE).astype(jnp.float32) + 0.5)[:, None]
    ahead = (lax.broadcasted_iota(jnp.int32, (BLOCK, BLOCK), 0) < lax.broadcasted_iota(jnp.int32, (BLOCK, BLOCK), 1)).astype(jnp.float32)
    current = (jnp.zeros((PIX,), jnp.float32), jnp.zeros((3, PIX), jnp.float32))
    for block in range(rows.shape[1] // BLOCK):
        piece = rows[:, block * BLOCK:(block + 1) * BLOCK]
        live = (block < count).astype(jnp.float32)

        def advance(holder, piece=piece, live=live):
            carried, image = holder
            delta_x = pixel_x - piece[0][None, :]
            delta_y = pixel_y - piece[1][None, :]
            power = piece[2][None, :] * delta_x * delta_x + 2.0 * piece[3][None, :] * delta_x * delta_y + piece[4][None, :] * delta_y * delta_y
            alpha = piece[5][None, :] * jnp.exp(-0.5 * power) * live
            decay = jnp.log1p(-alpha)
            before = jnp.dot(decay, ahead, precision=lax.Precision.HIGHEST, preferred_element_type=jnp.float32) + carried[:, None]
            weight = alpha * jnp.exp(before)
            image = image + lax.dot_general(piece[6:9], weight, (((1,), (1,)), ((), ())), precision=lax.Precision.HIGHEST, preferred_element_type=jnp.float32)
            return (carried + lax.optimization_barrier(jnp.sum(decay, axis=1)), image)
        if lazy:
            current = lax.cond(block < count, advance, lambda holder: holder, current)
        else:
            current = advance(current)
    return current[1]

def reference(params, first, second, visible, cameras, tile_lists, tile_blocks, targets):
    places = jnp.arange(V_VIEW, dtype=jnp.int32)
    within = places % VIS_OWN
    source_view = places // VIS_OWN % VIEWS
    source_tile = places // (VIEWS * VIS_OWN)
    owner = source_view * N_TILE + source_tile

    def one_view(carry, view):
        grad_total, hits = carry
        local = jnp.take(visible[view], owner * VIS_OWN + within)
        columns = (owner * G_DEV + local).astype(jnp.int32)
        raw = jnp.take(params, columns, axis=1)
        camera = cameras[view]
        projected, pullback = jax.vjp(lambda source: project(source, camera), raw)

        def one_tile(tile_index):
            listed = tile_lists[view, tile_index]
            rows = jnp.take(projected, listed, axis=1)
            anchor_x = (tile_index % WIN_COLS * SIDE).astype(jnp.float32)
            anchor_y = (tile_index // WIN_COLS * SIDE).astype(jnp.float32)
            count = tile_blocks[view, tile_index]
            image, pull = jax.vjp(lambda source: composite(source, anchor_x, anchor_y, count, False), rows)
            goal = lax.dynamic_slice_in_dim(targets[view], tile_index * PIX, PIX, 1)
            rows_grad, = pull(2.0 * (image - goal))
            return (image, rows_grad)
        images, row_grads = lax.map(one_tile, jnp.arange(TILES, dtype=jnp.int32))
        flat = tile_lists[view].reshape(-1)
        spread = jnp.transpose(row_grads, (1, 0, 2)).reshape(9, -1)
        projected_grad = jnp.zeros((9, V_VIEW), jnp.float32).at[:, flat].add(spread)
        raw_grad, = pullback(projected_grad)
        grad_total = grad_total.at[:, columns].add(raw_grad)
        hits = hits.at[columns].add(1.0)
        return ((grad_total, hits), jnp.transpose(images, (1, 0, 2)).reshape(3, TILES * PIX))
    start = (jnp.zeros((PARAMS, G_ALL), jnp.float32), jnp.zeros((G_ALL,), jnp.float32))
    (grad, hits), rendered = lax.scan(one_view, start, jnp.arange(VIEWS, dtype=jnp.int32))
    seen = (hits > 0.5)[None, :]
    moved_first = beta_first * first + (1.0 - beta_first) * grad
    moved_second = beta_second * second + (1.0 - beta_second) * grad * grad
    moved_params = params - learn_rate * moved_first / (jnp.sqrt(moved_second) + adam_eps)
    new_first = jnp.where(seen, moved_first, first)
    new_second = jnp.where(seen, moved_second, second)
    new_params = jnp.where(seen, moved_params, params)
    return (new_params, new_first, new_second, rendered)
```

```python
import functools

import jax
import jax.numpy as jnp
from jax import lax
from jax.experimental import pallas as pl
from jax.experimental.pallas import tpu as pltpu
from jax.sharding import PartitionSpec as P

SIDE = 16
PIX = 256
BLOCK = 128
WIN_COLS = 8


harm_zero = 0.28209479177387814
harm_one = 0.4886025119029199
harm_two = (
    1.0925484305920792,
    -1.0925484305920792,
    0.31539156525252005,
    -1.0925484305920792,
    0.5462742152960396,
)
harm_three = (
    -0.5900435899266435,
    2.890611442640554,
    -0.4570457994644658,
    0.3731763325901154,
    -0.4570457994644658,
    1.445305721320277,
    -0.5900435899266435,
)
learn_rate = 0.05
beta_first = 0.9
beta_second = 0.999
adam_eps = 1e-08
blur_add = 0.3


def rotation(real_part, axis_one, axis_two, axis_three):
    inverse = lax.rsqrt(
        real_part * real_part + axis_one * axis_one + axis_two * axis_two + axis_three * axis_three
    )
    real_unit = real_part * inverse
    unit_one = axis_one * inverse
    unit_two = axis_two * inverse
    unit_three = axis_three * inverse
    return (
        (
            1.0 - 2.0 * (unit_two * unit_two + unit_three * unit_three),
            2.0 * (unit_one * unit_two - real_unit * unit_three),
            2.0 * (unit_one * unit_three + real_unit * unit_two),
        ),
        (
            2.0 * (unit_one * unit_two + real_unit * unit_three),
            1.0 - 2.0 * (unit_one * unit_one + unit_three * unit_three),
            2.0 * (unit_two * unit_three - real_unit * unit_one),
        ),
        (
            2.0 * (unit_one * unit_three - real_unit * unit_two),
            2.0 * (unit_two * unit_three + real_unit * unit_one),
            1.0 - 2.0 * (unit_one * unit_one + unit_two * unit_two),
        ),
    )


def harmonics(first_dir, second_dir, third_dir):
    sq_first = first_dir * first_dir
    sq_second = second_dir * second_dir
    sq_third = third_dir * third_dir
    return [
        harm_zero,
        -harm_one * second_dir,
        harm_one * third_dir,
        -harm_one * first_dir,
        harm_two[0] * first_dir * second_dir,
        harm_two[1] * second_dir * third_dir,
        harm_two[2] * (2.0 * sq_third - sq_first - sq_second),
        harm_two[3] * first_dir * third_dir,
        harm_two[4] * (sq_first - sq_second),
        harm_three[0] * second_dir * (3.0 * sq_first - sq_second),
        harm_three[1] * first_dir * second_dir * third_dir,
        harm_three[2] * second_dir * (4.0 * sq_third - sq_first - sq_second),
        harm_three[3] * third_dir * (2.0 * sq_third - 3.0 * sq_first - 3.0 * sq_second),
        harm_three[4] * first_dir * (4.0 * sq_third - sq_first - sq_second),
        harm_three[5] * third_dir * (sq_first - sq_second),
        harm_three[6] * first_dir * (sq_first - 3.0 * sq_second),
    ]


def project(raw, camera):
    camera_turn = rotation(camera[0], camera[1], camera[2], camera[3])
    shift_vec = (camera[4], camera[5], camera[6])
    focal_x = camera[7]
    focal_y = camera[8]
    position = (raw[0], raw[1], raw[2])
    viewed = [
        camera_turn[across][0] * position[0]
        + camera_turn[across][1] * position[1]
        + camera_turn[across][2] * position[2]
        + shift_vec[across]
        for across in range(3)
    ]
    inverse = 1.0 / viewed[2]
    mean_x = focal_x * viewed[0] * inverse + camera[9]
    mean_y = focal_y * viewed[1] * inverse + camera[10]
    gauss_turn = rotation(raw[6], raw[7], raw[8], raw[9])
    stretch = [jnp.exp(raw[3 + column]) for column in range(3)]
    jac_xx = focal_x * inverse
    jac_xz = -focal_x * viewed[0] * inverse * inverse
    jac_yy = focal_y * inverse
    jac_yz = -focal_y * viewed[1] * inverse * inverse
    leading_x = [
        jac_xx * camera_turn[0][column] + jac_xz * camera_turn[2][column] for column in range(3)
    ]
    leading_y = [
        jac_yy * camera_turn[1][column] + jac_yz * camera_turn[2][column] for column in range(3)
    ]
    axes_x = [
        (
            leading_x[0] * gauss_turn[0][column]
            + leading_x[1] * gauss_turn[1][column]
            + leading_x[2] * gauss_turn[2][column]
        )
        * stretch[column]
        for column in range(3)
    ]
    axes_y = [
        (
            leading_y[0] * gauss_turn[0][column]
            + leading_y[1] * gauss_turn[1][column]
            + leading_y[2] * gauss_turn[2][column]
        )
        * stretch[column]
        for column in range(3)
    ]
    cov_xx = axes_x[0] * axes_x[0] + axes_x[1] * axes_x[1] + axes_x[2] * axes_x[2] + blur_add
    cov_xy = axes_x[0] * axes_y[0] + axes_x[1] * axes_y[1] + axes_x[2] * axes_y[2]
    cov_yy = axes_y[0] * axes_y[0] + axes_y[1] * axes_y[1] + axes_y[2] * axes_y[2] + blur_add
    determ = cov_xx * cov_yy - cov_xy * cov_xy
    opacity = jax.nn.sigmoid(raw[10])
    camera_eye = [
        -(
            camera_turn[0][column] * shift_vec[0]
            + camera_turn[1][column] * shift_vec[1]
            + camera_turn[2][column] * shift_vec[2]
        )
        for column in range(3)
    ]
    offset = [position[column] - camera_eye[column] for column in range(3)]
    length = lax.rsqrt(offset[0] * offset[0] + offset[1] * offset[1] + offset[2] * offset[2])
    harmonic_terms = harmonics(offset[0] * length, offset[1] * length, offset[2] * length)
    colours = []
    for channel in range(3):
        total = 0.5 + jnp.zeros_like(opacity)
        for harmonic in range(16):
            total = total + raw[11 + 16 * channel + harmonic] * harmonic_terms[harmonic]
        colours.append(total)
    return [mean_x, mean_y, cov_yy / determ, -cov_xy / determ, cov_xx / determ, opacity] + colours


F32 = jnp.float32
BF16 = jnp.bfloat16
PARAMS = 59
ROWS = 64
LOG2E = 1.4426950408889634


def iota(shape, dim):
    return lax.broadcasted_iota(jnp.int32, shape, dim)


def parts_of(value, count):
    parts = []
    for _ in range(count):
        part = value.astype(BF16)
        parts.append(part)
        value = value - part.astype(F32)
    return parts


def mm(left, right, dims):
    return lax.dot_general(left, right, (dims, ((), ())), preferred_element_type=F32)


def stacked(rows, width):
    sub = iota((8, width), 0)
    out = jnp.zeros((8, width), F32)
    for place, row in enumerate(rows):
        out = jnp.where(sub == place, jnp.broadcast_to(row, (8, width)), out)
    return out


def seen_columns(ids_ref, first, width):
    row = jnp.concatenate(
        [ids_ref[first + step : first + step + 1, :] for step in range(width // 64)], axis=1
    )
    return (iota((1024, width), 0) == row).astype(BF16)


def camera_arrays(cameras_ref):
    view = 2 * iota((8, 128), 0) + (iota((8, 128), 1) >= 64).astype(jnp.int32)
    masks = [view == index for index in range(16)]
    arrays = []
    for field in range(11):
        array = jnp.full((8, 128), cameras_ref[0, field], F32)
        for index in range(1, 16):
            array = jnp.where(masks[index], cameras_ref[index, field], array)
        arrays.append(array)
    return arrays


def raw_rows(picked_ref):
    return [picked_ref[pl.ds(row, 8, stride=ROWS), :] for row in range(PARAMS)]


def project_kernel(ids_ref, cameras_ref, params_ref, picked_ref, send_ref, swap):
    params = params_ref[...]
    split = parts_of(params, 3)
    for pair in range(4):
        onehot = seen_columns(ids_ref, pair * 4, 256)
        picked = sum(mm(part, onehot, ((1,), (0,))) for part in split)
        picked_ref[pair * 128 : pair * 128 + PARAMS, :] = picked[:, :128]
        picked_ref[pair * 128 + 64 : pair * 128 + 64 + PARAMS, :] = picked[:, 128:]
    values = project(raw_rows(picked_ref), camera_arrays(cameras_ref))
    for place in range(8):
        swap[place * 8 : place * 8 + 8, :] = values[place]
    low = iota((8, 128), 1) < 64
    for pair in range(8):
        main = swap[pl.ds(pair, 8, stride=8), :]
        last = jnp.broadcast_to(values[8][pair : pair + 1, :], (8, 128))
        send_ref[2 * pair] = jnp.where(low, main, pltpu.roll(last, 64, 1))
        send_ref[2 * pair + 1] = jnp.where(low, pltpu.roll(main, 64, 1), last)


def unpack_pair(even, odd):
    low = iota((8, 128), 1) < 64
    main = jnp.where(low, even, pltpu.roll(odd, 64, 1))
    last = jnp.where(low, pltpu.roll(even, 64, 1), odd)
    return main, last[0:1, :]


def spread_kernel(arrived_ref, out_ref):
    for pair in range(8):
        main, last = unpack_pair(arrived_ref[2 * pair], arrived_ref[2 * pair + 1])
        for peer in range(16):
            out_ref[peer, pair * 8 : pair * 8 + 8, :] = main
            out_ref[peer, 64 + pair : 65 + pair, :] = last


def render_kernel(
    place_ref,
    counts_ref,
    lists_ref,
    targets_ref,
    everyone_ref,
    image_ref,
    out_ref,
    table,
    onehot,
    chosen,
    picked,
    alphas,
    weights,
    shades,
    scattered,
):
    count = 2048
    width = 256
    turn = (iota((128, 1024), 0) == (iota((128, 1024), 1) >> 3)).astype(BF16)
    pick_block = iota((8, 1024), 0) == (iota((8, 1024), 1) & 7)
    for tile in range(2):
        listed = lists_ref[tile]
        low_part = mm((listed & 127).astype(F32).astype(BF16), turn, ((1,), (0,)))
        high_part = mm((listed >> 7).astype(F32).astype(BF16), turn, ((1,), (0,)))
        low_row = jnp.sum(jnp.where(pick_block, low_part, 0.0), axis=0, keepdims=True)
        high_row = jnp.sum(jnp.where(pick_block, high_part, 0.0), axis=0, keepdims=True)
        low_row = low_row.astype(jnp.int32)
        high_row = high_row.astype(jnp.int32)
        lane_index = ((high_row >> 3) & 1) * 128 + low_row
        group_index = (high_row >> 4) * 8 + (high_row & 7)
        span = slice(tile * 1024, tile * 1024 + 1024)
        onehot[:, span] = (iota((256, 1024), 0) == lane_index).astype(BF16)
        chosen[:, span] = jnp.broadcast_to(group_index, (8, 1024))

    for half in range(8):
        for side in range(2):
            lanes = slice(side * 128, side * 128 + 128)
            main = parts_of(everyone_ref[2 * half + side, 0:64, :], 3)
            last = parts_of(everyone_ref[2 * half + side, 64:72, :], 3)
            for part in range(3):
                table[part, half * 64 : half * 64 + 64, lanes] = main[part]
                table[part, 512 + half * 8 : 520 + half * 8, lanes] = last[part]

    def gather_chunk(chunk, carry):
        lanes = pl.ds(pl.multiple_of(chunk * width, width), width)
        hot = onehot[:, lanes]
        found = mm(table[0], hot, ((1,), (0,)))
        found = found + mm(table[1], hot, ((1,), (0,)))
        found = found + mm(table[2], hot, ((1,), (0,)))
        group = chosen[:, lanes]
        main = jnp.zeros((8, width), F32)
        last = jnp.zeros((8, width), F32)
        sub = iota((8, width), 0)
        for half in range(8):
            for place in range(8):
                start = half * 64 + place * 8
                main = jnp.where(group == half * 8 + place, found[start : start + 8, :], main)
            last = jnp.where(
                group == half * 8 + sub, found[512 + half * 8 : 520 + half * 8, :], last
            )
        picked[0:8, lanes] = main
        picked[8:16, lanes] = jnp.broadcast_to(jnp.sum(last, axis=0, keepdims=True), (8, width))
        return carry

    lax.fori_loop(0, count // width, gather_chunk, 0)

    pixel = iota((8, PIX), 1)
    pixel_x = (pixel & (SIDE - 1)).astype(F32) + (0.5 - SIDE / 2)
    pixel_y = (pixel >> 4).astype(F32) + (0.5 - SIDE / 2)
    sub = iota((8, PIX), 0)
    basis = jnp.where(sub == 0, 1.0, 0.0)
    for place, row in enumerate(
        [pixel_x, pixel_y, pixel_x * pixel_x, pixel_x * pixel_y, pixel_y * pixel_y]
    ):
        basis = jnp.where(sub == place + 1, row, basis)
    blank = jnp.zeros((8, PIX), F32)
    basis_three = jnp.concatenate([basis, basis, basis, blank], axis=0).astype(BF16)
    basis_once = jnp.concatenate([basis, blank], axis=0).astype(BF16)

    def rows_of(tile):
        span = slice(tile * 1024, tile * 1024 + 1024)
        held = picked[:, span]
        global_tile = place_ref[0] * 2 + tile
        centre_x = (global_tile % WIN_COLS * SIDE + SIDE // 2).astype(F32)
        centre_y = (global_tile // WIN_COLS * SIDE + SIDE // 2).astype(F32)
        rows = [held[place : place + 1, :] for place in range(9)]
        rows[0] = rows[0] - centre_x
        rows[1] = rows[1] - centre_y
        return rows

    block = iota((1, 1024), 1) & 7
    blank_row = jnp.zeros((8, 1024), F32)
    colour_rows = []
    for tile in range(2):
        mean_x, mean_y, con_a, con_b, con_c, opacity, *colour = rows_of(tile)
        live = block < counts_ref[0, tile]
        slope_x = con_a * mean_x + con_b * mean_y
        slope_y = con_b * mean_x + con_c * mean_y
        scale = -0.5 * LOG2E
        level = scale * (slope_x * mean_x + slope_y * mean_y) + jnp.log(opacity) * LOG2E
        terms = [
            jnp.where(live, level, -1000.0),
            jnp.where(live, (-2.0 * scale) * slope_x, 0.0),
            jnp.where(live, (-2.0 * scale) * slope_y, 0.0),
            jnp.where(live, scale * con_a, 0.0),
            jnp.where(live, (2.0 * scale) * con_b, 0.0),
            jnp.where(live, scale * con_c, 0.0),
        ]
        split = [part.astype(F32) for part in parts_of(stacked(terms, 1024), 3)]
        coefficients = jnp.concatenate(split + [blank_row], axis=0).astype(BF16)
        alphas[tile] = mm(coefficients, basis_three, ((0,), (0,)))
        colour_rows.append(stacked(colour, 1024))

    steps = 8

    def advance(outer, held):
        held = list(held)
        for inner in range(steps):
            start = pl.multiple_of((outer * steps + inner) * 8, 8)
            for tile in range(2):
                alpha = jnp.exp2(alphas[tile, pl.ds(start, 8), :])
                weight = alpha * held[tile]
                held[tile] = held[tile] - weight
                alphas[tile, pl.ds(start, 8), :] = alpha
                weights[tile, pl.ds(start, 8), :] = weight
        return tuple(held)

    ones = jnp.ones((8, PIX), F32)
    left = lax.fori_loop(0, 128 // steps, advance, (ones, ones))

    behind = []
    ahead = []
    blame = []
    sub_wide = iota((8, 1024), 0)
    block_wide = iota((8, 1024), 1) & 7
    for tile in range(2):
        colour = colour_rows[tile]
        separate = []
        for channel in range(3):
            row = jnp.broadcast_to(colour[channel : channel + 1, :], (8, 1024))
            separate.append(jnp.where(sub_wide == block_wide, row, 0.0))
        fine, rough = parts_of(jnp.concatenate(separate, axis=0), 2)
        both = jnp.concatenate([fine.astype(F32), rough.astype(F32)], axis=0).astype(BF16)
        first_part, second_part = parts_of(weights[tile], 2)
        sums = mm(both, first_part, ((1,), (0,))) + mm(both, second_part, ((1,), (0,)))
        passed = left[tile]
        total = passed
        for shift in (1, 2, 4):
            total = total * jnp.where(sub >= shift, pltpu.roll(total, shift, 0), 1.0)
        before = jnp.where(sub >= 1, pltpu.roll(total, 1, 0), 1.0)
        ahead.append(before)
        value = jnp.zeros((8, PIX), F32)
        slopes = []
        for channel in range(3):
            own = sums[channel * 8 : channel * 8 + 8, :]
            own = own + sums[24 + channel * 8 : 32 + channel * 8, :]
            image = jnp.sum(own * before, axis=0, keepdims=True)
            lanes = slice(tile * PIX, tile * PIX + PIX)
            image_ref[channel : channel + 1, lanes] = image
            slope = 2.0 * (image - targets_ref[channel : channel + 1, lanes])
            slopes.append(slope)
            value = value + slope * own
        factor = passed
        for shift in (1, 2, 4):
            inside = sub < 8 - shift
            value = value + factor * jnp.where(inside, pltpu.roll(value, 8 - shift, 0), 0.0)
            factor = factor * jnp.where(inside, pltpu.roll(factor, 8 - shift, 0), 1.0)
        behind.append(jnp.where(sub < 7, pltpu.roll(value, 7, 0), 0.0))
        slope_parts = [part.astype(F32) for part in parts_of(stacked(slopes, PIX), 3)]
        colour_parts = [part.astype(F32) for part in parts_of(colour, 3)]
        pairs = [(0, 0), (0, 1), (1, 0), (1, 1), (0, 2), (2, 0)]
        left_side = jnp.concatenate([colour_parts[a] for a, _ in pairs], axis=0).astype(BF16)
        right_side = jnp.concatenate([slope_parts[b] for _, b in pairs], axis=0).astype(BF16)
        shades[tile] = mm(left_side, right_side, ((0,), (0,)))
        blame.append(jnp.concatenate(slope_parts[:2], axis=0).astype(BF16))

    def retreat(outer, held):
        held = list(held)
        for inner in range(steps):
            start = pl.multiple_of((127 - (outer * steps + inner)) * 8, 8)
            for tile in range(2):
                alpha = alphas[tile, pl.ds(start, 8), :]
                weight = weights[tile, pl.ds(start, 8), :] * ahead[tile]
                gap = shades[tile, pl.ds(start, 8), :] - held[tile]
                held[tile] = held[tile] + alpha * gap
                shades[tile, pl.ds(start, 8), :] = weight * gap
                weights[tile, pl.ds(start, 8), :] = weight
        return tuple(held)

    lax.fori_loop(0, 128 // steps, retreat, tuple(behind))

    for tile in range(2):
        moments = sum(
            mm(basis_once, part, ((1,), (1,))) for part in parts_of(shades[tile], 3)
        )
        tints = sum(mm(blame[tile], part, ((1,), (1,))) for part in parts_of(weights[tile], 2))
        tints = tints[0:8, :] + tints[8:16, :]
        mean_x, mean_y, con_a, con_b, con_c, opacity, *_ = rows_of(tile)
        sum_one, sum_x, sum_y, sum_xx, sum_xy, sum_yy = [
            moments[place : place + 1, :] for place in range(6)
        ]
        near_x = sum_x - mean_x * sum_one
        near_y = sum_y - mean_y * sum_one
        near_xx = sum_xx - mean_x * (sum_x + near_x)
        near_xy = sum_xy - mean_x * sum_y - mean_y * near_x
        near_yy = sum_yy - mean_y * (sum_y + near_y)
        grads = [
            con_a * near_x + con_b * near_y,
            con_b * near_x + con_c * near_y,
            -0.5 * near_xx,
            -near_xy,
            -0.5 * near_yy,
            sum_one / opacity,
            tints[0:1, :],
            tints[1:2, :],
        ]
        span = slice(tile * 1024, tile * 1024 + 1024)
        picked[0:8, span] = stacked(grads, 1024)
        picked[8:16, span] = jnp.broadcast_to(tints[2:3, :], (8, 1024))

    def scatter_chunk(chunk, carry):
        lanes = pl.ds(pl.multiple_of(chunk * width, width), width)
        group = chosen[:, lanes]
        sub = iota((8, width), 0)
        main = [part.astype(F32) for part in parts_of(picked[0:8, lanes], 2)]
        last = [part.astype(F32) for part in parts_of(picked[8:16, lanes], 2)]
        for part in range(2):
            for pair in range(32):
                rows = jnp.concatenate(
                    [jnp.where(group == 2 * pair + side, main[part], 0.0) for side in range(2)],
                    axis=0,
                )
                scattered[part, pair * 16 : pair * 16 + 16, lanes] = rows.astype(BF16)
            for pair in range(4):
                rows = jnp.concatenate(
                    [
                        jnp.where(group == (2 * pair + side) * 8 + sub, last[part], 0.0)
                        for side in range(2)
                    ],
                    axis=0,
                )
                scattered[part, 512 + pair * 16 : 528 + pair * 16, lanes] = rows.astype(BF16)
        return carry

    lax.fori_loop(0, count // width, scatter_chunk, 0)
    hot = onehot[...]
    summed = mm(scattered[0], hot, ((1,), (1,))) + mm(scattered[1], hot, ((1,), (1,)))
    for half in range(8):
        for side in range(2):
            lanes = slice(side * 128, side * 128 + 128)
            out_ref[2 * half + side, 0:64, :] = summed[half * 64 : half * 64 + 64, lanes]
            out_ref[2 * half + side, 64:72, :] = summed[
                512 + half * 8 : 520 + half * 8, lanes
            ]


def merge_kernel(arrived_ref, send_ref):
    low = iota((8, 128), 1) < 64
    total = arrived_ref[0]
    for peer in range(1, 16):
        total = total + arrived_ref[peer]
    for pair in range(8):
        main = total[pair * 8 : pair * 8 + 8, :]
        last = jnp.broadcast_to(total[64 + pair : 65 + pair, :], (8, 128))
        send_ref[2 * pair] = jnp.where(low, main, pltpu.roll(last, 64, 1))
        send_ref[2 * pair + 1] = jnp.where(low, pltpu.roll(main, 64, 1), last)


def update_kernel(
    ids_ref,
    cameras_ref,
    arrived_ref,
    picked_ref,
    params_ref,
    first_ref,
    second_ref,
    new_params_ref,
    new_first_ref,
    new_second_ref,
    swap,
    turned,
    onehot,
):
    lasts = []
    for pair in range(8):
        main, last = unpack_pair(arrived_ref[2 * pair], arrived_ref[2 * pair + 1])
        swap[pair * 8 : pair * 8 + 8, :] = main
        lasts.append(last)
    slopes = [swap[pl.ds(place, 8, stride=8), :] for place in range(8)]
    sub = iota((8, 128), 0)
    final = jnp.zeros((8, 128), F32)
    for pair in range(8):
        final = jnp.where(sub == pair, jnp.broadcast_to(lasts[pair], (8, 128)), final)
    slopes.append(final)
    cameras = camera_arrays(cameras_ref)
    _, pullback = jax.vjp(lambda source: project(source, cameras), raw_rows(picked_ref))
    (raw_grads,) = pullback(slopes)
    for row in range(PARAMS):
        turned[pl.ds(row, 8, stride=ROWS), :] = raw_grads[row]
    for row in range(PARAMS, ROWS):
        turned[pl.ds(row, 8, stride=ROWS), :] = jnp.ones((8, 128), F32)
    for pair in range(4):
        onehot[:, pair * 256 : pair * 256 + 256] = seen_columns(ids_ref, pair * 4, 256)
    wide = jnp.concatenate([turned[pair * ROWS : pair * ROWS + ROWS, :] for pair in range(8)], axis=1)
    hot = onehot[...]
    summed = sum(mm(part, hot, ((1,), (1,))) for part in parts_of(wide, 3))
    grad = summed[0:PARAMS, :]
    seen = summed[PARAMS : PARAMS + 1, :] > 0.5
    first = first_ref[...]
    second = second_ref[...]
    params = params_ref[...]
    moved_first = beta_first * first + (1.0 - beta_first) * grad
    moved_second = beta_second * second + (1.0 - beta_second) * grad * grad
    moved_params = params - learn_rate * moved_first / (jnp.sqrt(moved_second) + adam_eps)
    new_first_ref[...] = jnp.where(seen, moved_first, first)
    new_second_ref[...] = jnp.where(seen, moved_second, second)
    new_params_ref[...] = jnp.where(seen, moved_params, params)


SMEM = pl.BlockSpec(memory_space=pltpu.SMEM)
VMEM = pl.BlockSpec(memory_space=pltpu.VMEM)


def f32_shape(*shape):
    return jax.ShapeDtypeStruct(shape, F32)


def project_call(visible, cameras, params):
    return pl.pallas_call(
        project_kernel,
        out_shape=(f32_shape(512, 128), f32_shape(16, 8, 128)),
        in_specs=[VMEM, SMEM, VMEM],
        out_specs=(VMEM, VMEM),
        scratch_shapes=[pltpu.VMEM((64, 128), F32)],
        name="project",
    )(visible, cameras, params)


def spread_call(arrived):
    return pl.pallas_call(
        spread_kernel,
        out_shape=f32_shape(16, 72, 128),
        in_specs=[VMEM],
        out_specs=VMEM,
        name="spread",
    )(arrived)


def render_call(place, counts, lists, targets, everyone):
    return pl.pallas_call(
        render_kernel,
        out_shape=(f32_shape(3, 512), f32_shape(16, 72, 128)),
        in_specs=[SMEM, SMEM, VMEM, VMEM, VMEM],
        out_specs=(VMEM, VMEM),
        scratch_shapes=[
            pltpu.VMEM((3, 576, 256), BF16),
            pltpu.VMEM((256, 2048), BF16),
            pltpu.VMEM((8, 2048), jnp.int32),
            pltpu.VMEM((16, 2048), F32),
            pltpu.VMEM((2, 1024, 256), F32),
            pltpu.VMEM((2, 1024, 256), F32),
            pltpu.VMEM((2, 1024, 256), F32),
            pltpu.VMEM((2, 576, 2048), BF16),
        ],
        name="render",
    )(place, counts, lists, targets, everyone)


def merge_call(arrived):
    return pl.pallas_call(
        merge_kernel,
        out_shape=f32_shape(16, 8, 128),
        in_specs=[VMEM],
        out_specs=VMEM,
        name="merge",
    )(arrived)


def update_call(visible, cameras, arrived, picked, params, first, second):
    shape = f32_shape(*params.shape)
    return pl.pallas_call(
        update_kernel,
        out_shape=(shape, shape, shape),
        in_specs=[VMEM, SMEM, VMEM, VMEM, VMEM, VMEM, VMEM],
        out_specs=(VMEM, VMEM, VMEM),
        scratch_shapes=[
            pltpu.VMEM((64, 128), F32),
            pltpu.VMEM((512, 128), F32),
            pltpu.VMEM((1024, 1024), BF16),
        ],
        name="update",
    )(visible, cameras, arrived, picked, params, first, second)


def shards(params, first, second, visible, cameras, tile_lists, tile_blocks, targets):
    picked, outgoing = project_call(visible, cameras, params)
    arrived = lax.all_to_all(outgoing, "view", 0, 0, tiled=True)
    everyone = lax.all_to_all(spread_call(arrived), "tile", 0, 0, tiled=True)
    place = lax.axis_index("tile").astype(jnp.int32).reshape(1)
    image, sums = render_call(
        place, tile_blocks, tile_lists.reshape(2, 8, 128), targets[0], everyone
    )
    back = lax.all_to_all(sums, "tile", 0, 0, tiled=True)
    returned = lax.all_to_all(merge_call(back), "view", 0, 0, tiled=True)
    new_params, new_first, new_second = update_call(
        visible, cameras, returned, picked, params, first, second
    )
    return (new_params, new_first, new_second, image[None])


def solution(mesh):
    in_specs = (
        P(None, ("view", "tile")),
        P(None, ("view", "tile")),
        P(None, ("view", "tile")),
        P(None, ("view", "tile")),
        P(),
        P("view", "tile", None),
        P("view", "tile"),
        P("view", None, "tile"),
    )
    out_specs = (
        P(None, ("view", "tile")),
        P(None, ("view", "tile")),
        P(None, ("view", "tile")),
        P("view", None, "tile"),
    )
    return jax.shard_map(shards, mesh=mesh, in_specs=in_specs, out_specs=out_specs, check_vma=False)
```

```python
import functools

import jax
import jax.numpy as jnp
from jax import lax
from jax.experimental import pallas as pl
from jax.experimental.pallas import tpu as pltpu
from jax.sharding import PartitionSpec as P

SIDE = 16
PIX = 256
BLOCK = 128
WIN_COLS = 8


harm_zero = 0.28209479177387814
harm_one = 0.4886025119029199
harm_two = (
    1.0925484305920792,
    -1.0925484305920792,
    0.31539156525252005,
    -1.0925484305920792,
    0.5462742152960396,
)
harm_three = (
    -0.5900435899266435,
    2.890611442640554,
    -0.4570457994644658,
    0.3731763325901154,
    -0.4570457994644658,
    1.445305721320277,
    -0.5900435899266435,
)
learn_rate = 0.05
beta_first = 0.9
beta_second = 0.999
adam_eps = 1e-08
blur_add = 0.3


def rotation(real_part, axis_one, axis_two, axis_three):
    inverse = lax.rsqrt(
        real_part * real_part + axis_one * axis_one + axis_two * axis_two + axis_three * axis_three
    )
    real_unit = real_part * inverse
    unit_one = axis_one * inverse
    unit_two = axis_two * inverse
    unit_three = axis_three * inverse
    return (
        (
            1.0 - 2.0 * (unit_two * unit_two + unit_three * unit_three),
            2.0 * (unit_one * unit_two - real_unit * unit_three),
            2.0 * (unit_one * unit_three + real_unit * unit_two),
        ),
        (
            2.0 * (unit_one * unit_two + real_unit * unit_three),
            1.0 - 2.0 * (unit_one * unit_one + unit_three * unit_three),
            2.0 * (unit_two * unit_three - real_unit * unit_one),
        ),
        (
            2.0 * (unit_one * unit_three - real_unit * unit_two),
            2.0 * (unit_two * unit_three + real_unit * unit_one),
            1.0 - 2.0 * (unit_one * unit_one + unit_two * unit_two),
        ),
    )


def harmonics(first_dir, second_dir, third_dir):
    sq_first = first_dir * first_dir
    sq_second = second_dir * second_dir
    sq_third = third_dir * third_dir
    return [
        harm_zero,
        -harm_one * second_dir,
        harm_one * third_dir,
        -harm_one * first_dir,
        harm_two[0] * first_dir * second_dir,
        harm_two[1] * second_dir * third_dir,
        harm_two[2] * (2.0 * sq_third - sq_first - sq_second),
        harm_two[3] * first_dir * third_dir,
        harm_two[4] * (sq_first - sq_second),
        harm_three[0] * second_dir * (3.0 * sq_first - sq_second),
        harm_three[1] * first_dir * second_dir * third_dir,
        harm_three[2] * second_dir * (4.0 * sq_third - sq_first - sq_second),
        harm_three[3] * third_dir * (2.0 * sq_third - 3.0 * sq_first - 3.0 * sq_second),
        harm_three[4] * first_dir * (4.0 * sq_third - sq_first - sq_second),
        harm_three[5] * third_dir * (sq_first - sq_second),
        harm_three[6] * first_dir * (sq_first - 3.0 * sq_second),
    ]


def project(raw, camera):
    camera_turn = rotation(camera[0], camera[1], camera[2], camera[3])
    shift_vec = (camera[4], camera[5], camera[6])
    focal_x = camera[7]
    focal_y = camera[8]
    position = (raw[0], raw[1], raw[2])
    viewed = [
        camera_turn[across][0] * position[0]
        + camera_turn[across][1] * position[1]
        + camera_turn[across][2] * position[2]
        + shift_vec[across]
        for across in range(3)
    ]
    inverse = 1.0 / viewed[2]
    mean_x = focal_x * viewed[0] * inverse + camera[9]
    mean_y = focal_y * viewed[1] * inverse + camera[10]
    gauss_turn = rotation(raw[6], raw[7], raw[8], raw[9])
    stretch = [jnp.exp(raw[3 + column]) for column in range(3)]
    jac_xx = focal_x * inverse
    jac_xz = -focal_x * viewed[0] * inverse * inverse
    jac_yy = focal_y * inverse
    jac_yz = -focal_y * viewed[1] * inverse * inverse
    leading_x = [
        jac_xx * camera_turn[0][column] + jac_xz * camera_turn[2][column] for column in range(3)
    ]
    leading_y = [
        jac_yy * camera_turn[1][column] + jac_yz * camera_turn[2][column] for column in range(3)
    ]
    axes_x = [
        (
            leading_x[0] * gauss_turn[0][column]
            + leading_x[1] * gauss_turn[1][column]
            + leading_x[2] * gauss_turn[2][column]
        )
        * stretch[column]
        for column in range(3)
    ]
    axes_y = [
        (
            leading_y[0] * gauss_turn[0][column]
            + leading_y[1] * gauss_turn[1][column]
            + leading_y[2] * gauss_turn[2][column]
        )
        * stretch[column]
        for column in range(3)
    ]
    cov_xx = axes_x[0] * axes_x[0] + axes_x[1] * axes_x[1] + axes_x[2] * axes_x[2] + blur_add
    cov_xy = axes_x[0] * axes_y[0] + axes_x[1] * axes_y[1] + axes_x[2] * axes_y[2]
    cov_yy = axes_y[0] * axes_y[0] + axes_y[1] * axes_y[1] + axes_y[2] * axes_y[2] + blur_add
    determ = cov_xx * cov_yy - cov_xy * cov_xy
    opacity = jax.nn.sigmoid(raw[10])
    camera_eye = [
        -(
            camera_turn[0][column] * shift_vec[0]
            + camera_turn[1][column] * shift_vec[1]
            + camera_turn[2][column] * shift_vec[2]
        )
        for column in range(3)
    ]
    offset = [position[column] - camera_eye[column] for column in range(3)]
    length = lax.rsqrt(offset[0] * offset[0] + offset[1] * offset[1] + offset[2] * offset[2])
    harmonic_terms = harmonics(offset[0] * length, offset[1] * length, offset[2] * length)
    colours = []
    for channel in range(3):
        total = 0.5 + jnp.zeros_like(opacity)
        for harmonic in range(16):
            total = total + raw[11 + 16 * channel + harmonic] * harmonic_terms[harmonic]
        colours.append(total)
    return [mean_x, mean_y, cov_yy / determ, -cov_xy / determ, cov_xx / determ, opacity] + colours


F32 = jnp.float32
BF16 = jnp.bfloat16
PARAMS = 59
ROWS = 64
LOG2E = 1.4426950408889634


def iota(shape, dim):
    return lax.broadcasted_iota(jnp.int32, shape, dim)


def parts_of(value, count):
    parts = []
    for _ in range(count):
        part = value.astype(BF16)
        parts.append(part)
        value = value - part.astype(F32)
    return parts


def mm(left, right, dims):
    return lax.dot_general(left, right, (dims, ((), ())), preferred_element_type=F32)


def stacked(rows, width):
    sub = iota((8, width), 0)
    out = jnp.zeros((8, width), F32)
    for place, row in enumerate(rows):
        out = jnp.where(sub == place, jnp.broadcast_to(row, (8, width)), out)
    return out


def seen_columns(ids_ref, first, width):
    row = jnp.concatenate(
        [ids_ref[first + step : first + step + 1, :] for step in range(width // 64)], axis=1
    )
    return (iota((1024, width), 0) == row).astype(BF16)


def camera_arrays(cameras_ref):
    view = 2 * iota((8, 128), 0) + (iota((8, 128), 1) >= 64).astype(jnp.int32)
    masks = [view == index for index in range(16)]
    arrays = []
    for field in range(11):
        array = jnp.full((8, 128), cameras_ref[0, field], F32)
        for index in range(1, 16):
            array = jnp.where(masks[index], cameras_ref[index, field], array)
        arrays.append(array)
    return arrays


def raw_rows(picked_ref):
    return [picked_ref[pl.ds(row, 8, stride=ROWS), :] for row in range(PARAMS)]


def project_kernel(ids_ref, cameras_ref, params_ref, picked_ref, send_ref, swap):
    params = params_ref[...]
    split = parts_of(params, 3)
    for pair in range(4):
        onehot = seen_columns(ids_ref, pair * 4, 256)
        picked = sum(mm(part, onehot, ((1,), (0,))) for part in split)
        picked_ref[pair * 128 : pair * 128 + PARAMS, :] = picked[:, :128]
        picked_ref[pair * 128 + 64 : pair * 128 + 64 + PARAMS, :] = picked[:, 128:]
    values = project(raw_rows(picked_ref), camera_arrays(cameras_ref))
    for place in range(8):
        swap[place * 8 : place * 8 + 8, :] = values[place]
    low = iota((8, 128), 1) < 64
    for pair in range(8):
        main = swap[pl.ds(pair, 8, stride=8), :]
        last = jnp.broadcast_to(values[8][pair : pair + 1, :], (8, 128))
        send_ref[2 * pair] = jnp.where(low, main, pltpu.roll(last, 64, 1))
        send_ref[2 * pair + 1] = jnp.where(low, pltpu.roll(main, 64, 1), last)


def unpack_pair(even, odd):
    low = iota((8, 128), 1) < 64
    main = jnp.where(low, even, pltpu.roll(odd, 64, 1))
    last = jnp.where(low, pltpu.roll(even, 64, 1), odd)
    return main, last[0:1, :]


def spread_kernel(arrived_ref, out_ref):
    for pair in range(8):
        main, last = unpack_pair(arrived_ref[2 * pair], arrived_ref[2 * pair + 1])
        for peer in range(16):
            out_ref[peer, pair * 8 : pair * 8 + 8, :] = main
            out_ref[peer, 64 + pair : 65 + pair, :] = last


def render_kernel(
    place_ref,
    counts_ref,
    lists_ref,
    targets_ref,
    everyone_ref,
    image_ref,
    out_ref,
    onehot,
    lanes_of,
    chosen,
    picked,
    alphas,
    weights,
    shades,
    scattered,
):
    count = 2048
    turn = (iota((128, 1024), 0) == (iota((128, 1024), 1) >> 3)).astype(BF16)
    pick_block = iota((8, 1024), 0) == (iota((8, 1024), 1) & 7)
    for tile in range(2):
        blocks = [lists_ref[0, tile : tile + 1, start : start + 128] for start in range(0, 1024, 128)]
        low_part = stacked([(row & 127).astype(F32) for row in blocks], 128)
        high_part = stacked([(row >> 7).astype(F32) for row in blocks], 128)
        low_part = mm(low_part.astype(BF16), turn, ((1,), (0,)))
        high_part = mm(high_part.astype(BF16), turn, ((1,), (0,)))
        low_row = jnp.sum(jnp.where(pick_block, low_part, 0.0), axis=0, keepdims=True)
        high_row = jnp.sum(jnp.where(pick_block, high_part, 0.0), axis=0, keepdims=True)
        low_row = low_row.astype(jnp.int32)
        high_row = high_row.astype(jnp.int32)
        lane_index = ((high_row >> 3) & 1) * 128 + low_row
        span = slice(tile * 1024, tile * 1024 + 1024)
        onehot[:, span] = (iota((256, 1024), 0) == lane_index).astype(BF16)
        lanes_of[:, span] = jnp.broadcast_to(low_row, (8, 1024))
        chosen[:, span] = jnp.broadcast_to(high_row, (8, 1024))

    def gather_chunk(chunk, carry):
        lanes = pl.ds(pl.multiple_of(chunk * 128, 128), 128)
        lane = lanes_of[:, lanes]
        group = chosen[:, lanes]
        sub = iota((8, 128), 0)
        zero = jnp.zeros((8, 128), F32)
        main = [zero, zero, zero, zero]
        last = [zero, zero]
        for peer in range(16):
            for place in range(8):
                found = jnp.take_along_axis(
                    everyone_ref[peer, place * 8 : place * 8 + 8, :], lane, axis=1
                )
                chain = place % 4
                main[chain] = jnp.where(group == peer * 8 + place, found, main[chain])
            found = jnp.take_along_axis(everyone_ref[peer, 64:72, :], lane, axis=1)
            last[peer % 2] = jnp.where(group == peer * 8 + sub, found, last[peer % 2])
        picked[0:8, lanes] = (main[0] + main[1]) + (main[2] + main[3])
        picked[8:16, lanes] = jnp.broadcast_to(
            jnp.sum(last[0] + last[1], axis=0, keepdims=True), (8, 128)
        )
        return carry

    lax.fori_loop(0, count // 128, gather_chunk, 0)

    pixel = iota((8, PIX), 1)
    pixel_x = (pixel & (SIDE - 1)).astype(F32) + (0.5 - SIDE / 2)
    pixel_y = (pixel >> 4).astype(F32) + (0.5 - SIDE / 2)
    sub = iota((8, PIX), 0)
    basis = jnp.where(sub == 0, 1.0, 0.0)
    for place, row in enumerate(
        [pixel_x, pixel_y, pixel_x * pixel_x, pixel_x * pixel_y, pixel_y * pixel_y]
    ):
        basis = jnp.where(sub == place + 1, row, basis)
    blank = jnp.zeros((8, PIX), F32)
    basis_three = jnp.concatenate([basis, basis, basis, blank], axis=0).astype(BF16)
    basis_once = jnp.concatenate([basis, blank], axis=0).astype(BF16)

    def rows_of(tile):
        span = slice(tile * 1024, tile * 1024 + 1024)
        held = picked[:, span]
        global_tile = place_ref[0] * 2 + tile
        centre_x = (global_tile % WIN_COLS * SIDE + SIDE // 2).astype(F32)
        centre_y = (global_tile // WIN_COLS * SIDE + SIDE // 2).astype(F32)
        rows = [held[place : place + 1, :] for place in range(9)]
        rows[0] = rows[0] - centre_x
        rows[1] = rows[1] - centre_y
        return rows

    block = iota((1, 1024), 1) & 7
    blank_row = jnp.zeros((8, 1024), F32)
    colour_rows = []
    for tile in range(2):
        mean_x, mean_y, con_a, con_b, con_c, opacity, *colour = rows_of(tile)
        live = block < counts_ref[0, tile]
        slope_x = con_a * mean_x + con_b * mean_y
        slope_y = con_b * mean_x + con_c * mean_y
        scale = -0.5 * LOG2E
        level = scale * (slope_x * mean_x + slope_y * mean_y) + jnp.log(opacity) * LOG2E
        terms = [
            jnp.where(live, level, -1000.0),
            jnp.where(live, (-2.0 * scale) * slope_x, 0.0),
            jnp.where(live, (-2.0 * scale) * slope_y, 0.0),
            jnp.where(live, scale * con_a, 0.0),
            jnp.where(live, (2.0 * scale) * con_b, 0.0),
            jnp.where(live, scale * con_c, 0.0),
        ]
        split = [part.astype(F32) for part in parts_of(stacked(terms, 1024), 3)]
        coefficients = jnp.concatenate(split + [blank_row], axis=0).astype(BF16)
        alphas[tile] = mm(coefficients, basis_three, ((0,), (0,)))
        colour_rows.append(stacked(colour, 1024))

    steps = 8

    def advance(outer, held):
        held = list(held)
        for inner in range(steps):
            start = pl.multiple_of((outer * steps + inner) * 8, 8)
            for tile in range(2):
                alpha = jnp.exp2(alphas[tile, pl.ds(start, 8), :])
                weight = alpha * held[tile]
                held[tile] = held[tile] * (1.0 - alpha)
                alphas[tile, pl.ds(start, 8), :] = alpha
                weights[tile, pl.ds(start, 8), :] = weight
        return tuple(held)

    ones = jnp.ones((8, PIX), F32)
    left = lax.fori_loop(0, 128 // steps, advance, (ones, ones))

    behind = []
    ahead = []
    blame = []
    sub_wide = iota((8, 1024), 0)
    block_wide = iota((8, 1024), 1) & 7
    for tile in range(2):
        colour = colour_rows[tile]
        separate = []
        for channel in range(3):
            row = jnp.broadcast_to(colour[channel : channel + 1, :], (8, 1024))
            separate.append(jnp.where(sub_wide == block_wide, row, 0.0))
        fine, rough = parts_of(jnp.concatenate(separate, axis=0), 2)
        both = jnp.concatenate([fine.astype(F32), rough.astype(F32)], axis=0).astype(BF16)
        first_part, second_part = parts_of(weights[tile], 2)
        sums = mm(both, first_part, ((1,), (0,))) + mm(both, second_part, ((1,), (0,)))
        passed = left[tile]
        total = passed
        for shift in (1, 2, 4):
            total = total * jnp.where(sub >= shift, pltpu.roll(total, shift, 0), 1.0)
        before = jnp.where(sub >= 1, pltpu.roll(total, 1, 0), 1.0)
        ahead.append(before)
        value = jnp.zeros((8, PIX), F32)
        slopes = []
        for channel in range(3):
            own = sums[channel * 8 : channel * 8 + 8, :]
            own = own + sums[24 + channel * 8 : 32 + channel * 8, :]
            image = jnp.sum(own * before, axis=0, keepdims=True)
            lanes = slice(tile * PIX, tile * PIX + PIX)
            image_ref[channel, :, lanes] = image
            slope = 2.0 * (image - targets_ref[channel, :, lanes])
            slopes.append(slope)
            value = value + slope * own
        factor = passed
        for shift in (1, 2, 4):
            inside = sub < 8 - shift
            value = value + factor * jnp.where(inside, pltpu.roll(value, 8 - shift, 0), 0.0)
            factor = factor * jnp.where(inside, pltpu.roll(factor, 8 - shift, 0), 1.0)
        behind.append(jnp.where(sub < 7, pltpu.roll(value, 7, 0), 0.0))
        slope_parts = [part.astype(F32) for part in parts_of(stacked(slopes, PIX), 3)]
        colour_parts = [part.astype(F32) for part in parts_of(colour, 3)]
        pairs = [(0, 0), (0, 1), (1, 0), (1, 1), (0, 2), (2, 0)]
        left_side = jnp.concatenate([colour_parts[a] for a, _ in pairs], axis=0).astype(BF16)
        right_side = jnp.concatenate([slope_parts[b] for _, b in pairs], axis=0).astype(BF16)
        shades[tile] = mm(left_side, right_side, ((0,), (0,)))
        blame.append(jnp.concatenate(slope_parts[:2], axis=0).astype(BF16))

    def retreat(outer, held):
        held = list(held)
        for inner in range(steps):
            start = pl.multiple_of((127 - (outer * steps + inner)) * 8, 8)
            for tile in range(2):
                alpha = alphas[tile, pl.ds(start, 8), :]
                weight = weights[tile, pl.ds(start, 8), :] * ahead[tile]
                shade = shades[tile, pl.ds(start, 8), :]
                shades[tile, pl.ds(start, 8), :] = weight * (shade - held[tile])
                held[tile] = held[tile] * (1.0 - alpha) + alpha * shade
                weights[tile, pl.ds(start, 8), :] = weight
        return tuple(held)

    lax.fori_loop(0, 128 // steps, retreat, tuple(behind))

    for tile in range(2):
        moments = sum(
            mm(basis_once, part, ((1,), (1,))) for part in parts_of(shades[tile], 3)
        )
        tints = sum(mm(blame[tile], part, ((1,), (1,))) for part in parts_of(weights[tile], 2))
        tints = tints[0:8, :] + tints[8:16, :]
        mean_x, mean_y, con_a, con_b, con_c, opacity, *_ = rows_of(tile)
        sum_one, sum_x, sum_y, sum_xx, sum_xy, sum_yy = [
            moments[place : place + 1, :] for place in range(6)
        ]
        near_x = sum_x - mean_x * sum_one
        near_y = sum_y - mean_y * sum_one
        near_xx = sum_xx - mean_x * (sum_x + near_x)
        near_xy = sum_xy - mean_x * sum_y - mean_y * near_x
        near_yy = sum_yy - mean_y * (sum_y + near_y)
        grads = [
            con_a * near_x + con_b * near_y,
            con_b * near_x + con_c * near_y,
            -0.5 * near_xx,
            -near_xy,
            -0.5 * near_yy,
            sum_one / opacity,
            tints[0:1, :],
            tints[1:2, :],
        ]
        span = slice(tile * 1024, tile * 1024 + 1024)
        picked[0:8, span] = stacked(grads, 1024)
        picked[8:16, span] = jnp.broadcast_to(tints[2:3, :], (8, 1024))

    wide = 256

    def scatter_chunk(chunk, carry):
        lanes = pl.ds(pl.multiple_of(chunk * wide, wide), wide)
        group = chosen[:, lanes]
        group = (group >> 4) * 8 + (group & 7)
        sub = iota((8, wide), 0)
        main = [part.astype(F32) for part in parts_of(picked[0:8, lanes], 2)]
        last = [part.astype(F32) for part in parts_of(picked[8:16, lanes], 2)]
        for pair in range(36):
            for part in range(2):
                if pair < 32:
                    rows = [
                        jnp.where(group == 2 * pair + side, main[part], 0.0) for side in range(2)
                    ]
                else:
                    rows = [
                        jnp.where(group == (2 * pair - 64 + side) * 8 + sub, last[part], 0.0)
                        for side in range(2)
                    ]
                rows = jnp.concatenate(rows, axis=0).astype(BF16)
                scattered[part, pair * 16 : pair * 16 + 16, lanes] = rows
        return carry

    lax.fori_loop(0, count // wide, scatter_chunk, 0)
    hot = onehot[...]
    summed = mm(scattered[0], hot, ((1,), (1,))) + mm(scattered[1], hot, ((1,), (1,)))
    for half in range(8):
        for side in range(2):
            lanes = slice(side * 128, side * 128 + 128)
            out_ref[2 * half + side, 0:64, :] = summed[half * 64 : half * 64 + 64, lanes]
            out_ref[2 * half + side, 64:72, :] = summed[
                512 + half * 8 : 520 + half * 8, lanes
            ]


def merge_kernel(arrived_ref, send_ref):
    low = iota((8, 128), 1) < 64
    total = arrived_ref[0]
    for peer in range(1, 16):
        total = total + arrived_ref[peer]
    for pair in range(8):
        main = total[pair * 8 : pair * 8 + 8, :]
        last = jnp.broadcast_to(total[64 + pair : 65 + pair, :], (8, 128))
        send_ref[2 * pair] = jnp.where(low, main, pltpu.roll(last, 64, 1))
        send_ref[2 * pair + 1] = jnp.where(low, pltpu.roll(main, 64, 1), last)


def update_kernel(
    ids_ref,
    cameras_ref,
    arrived_ref,
    picked_ref,
    params_ref,
    first_ref,
    second_ref,
    new_params_ref,
    new_first_ref,
    new_second_ref,
    swap,
    turned,
    onehot,
):
    lasts = []
    for pair in range(8):
        main, last = unpack_pair(arrived_ref[2 * pair], arrived_ref[2 * pair + 1])
        swap[pair * 8 : pair * 8 + 8, :] = main
        lasts.append(last)
    slopes = [swap[pl.ds(place, 8, stride=8), :] for place in range(8)]
    sub = iota((8, 128), 0)
    final = jnp.zeros((8, 128), F32)
    for pair in range(8):
        final = jnp.where(sub == pair, jnp.broadcast_to(lasts[pair], (8, 128)), final)
    slopes.append(final)
    cameras = camera_arrays(cameras_ref)
    _, pullback = jax.vjp(lambda source: project(source, cameras), raw_rows(picked_ref))
    (raw_grads,) = pullback(slopes)
    for row in range(PARAMS):
        turned[pl.ds(row, 8, stride=ROWS), :] = raw_grads[row]
    for row in range(PARAMS, ROWS):
        turned[pl.ds(row, 8, stride=ROWS), :] = jnp.ones((8, 128), F32)
    for pair in range(4):
        onehot[:, pair * 256 : pair * 256 + 256] = seen_columns(ids_ref, pair * 4, 256)
    wide = jnp.concatenate([turned[pair * ROWS : pair * ROWS + ROWS, :] for pair in range(8)], axis=1)
    hot = onehot[...]
    summed = sum(mm(part, hot, ((1,), (1,))) for part in parts_of(wide, 3))
    grad = summed[0:PARAMS, :]
    seen = summed[PARAMS : PARAMS + 1, :] > 0.5
    first = first_ref[...]
    second = second_ref[...]
    params = params_ref[...]
    moved_first = beta_first * first + (1.0 - beta_first) * grad
    moved_second = beta_second * second + (1.0 - beta_second) * grad * grad
    moved_params = params - learn_rate * moved_first / (jnp.sqrt(moved_second) + adam_eps)
    new_first_ref[...] = jnp.where(seen, moved_first, first)
    new_second_ref[...] = jnp.where(seen, moved_second, second)
    new_params_ref[...] = jnp.where(seen, moved_params, params)


SMEM = pl.BlockSpec(memory_space=pltpu.SMEM)
VMEM = pl.BlockSpec(memory_space=pltpu.VMEM)


def f32_shape(*shape):
    return jax.ShapeDtypeStruct(shape, F32)


def project_call(visible, cameras, params):
    return pl.pallas_call(
        project_kernel,
        out_shape=(f32_shape(512, 128), f32_shape(16, 8, 128)),
        in_specs=[VMEM, SMEM, VMEM],
        out_specs=(VMEM, VMEM),
        scratch_shapes=[pltpu.VMEM((64, 128), F32)],
        name="project",
    )(visible, cameras, params)


def spread_call(arrived):
    return pl.pallas_call(
        spread_kernel,
        out_shape=f32_shape(16, 72, 128),
        in_specs=[VMEM],
        out_specs=VMEM,
        name="spread",
    )(arrived)


def render_call(place, counts, lists, targets, everyone):
    return pl.pallas_call(
        render_kernel,
        out_shape=(f32_shape(3, 1, 512), f32_shape(16, 72, 128)),
        in_specs=[SMEM, SMEM, VMEM, VMEM, VMEM],
        out_specs=(VMEM, VMEM),
        scratch_shapes=[
            pltpu.VMEM((256, 2048), BF16),
            pltpu.VMEM((8, 2048), jnp.int32),
            pltpu.VMEM((8, 2048), jnp.int32),
            pltpu.VMEM((16, 2048), F32),
            pltpu.VMEM((2, 1024, 256), F32),
            pltpu.VMEM((2, 1024, 256), F32),
            pltpu.VMEM((2, 1024, 256), F32),
            pltpu.VMEM((2, 576, 2048), BF16),
        ],
        name="render",
    )(place, counts, lists, targets, everyone)


def merge_call(arrived):
    return pl.pallas_call(
        merge_kernel,
        out_shape=f32_shape(16, 8, 128),
        in_specs=[VMEM],
        out_specs=VMEM,
        name="merge",
    )(arrived)


def update_call(visible, cameras, arrived, picked, params, first, second):
    shape = f32_shape(*params.shape)
    return pl.pallas_call(
        update_kernel,
        out_shape=(shape, shape, shape),
        in_specs=[VMEM, SMEM, VMEM, VMEM, VMEM, VMEM, VMEM],
        out_specs=(VMEM, VMEM, VMEM),
        scratch_shapes=[
            pltpu.VMEM((64, 128), F32),
            pltpu.VMEM((512, 128), F32),
            pltpu.VMEM((1024, 1024), BF16),
        ],
        name="update",
    )(visible, cameras, arrived, picked, params, first, second)


def kept(array):
    return pltpu.with_memory_space_constraint(array, pltpu.VMEM)


def exchanged(array, axis):
    return kept(lax.all_to_all(array, axis, 0, 0, tiled=True))


def shards(params, first, second, visible, cameras, tile_lists, tile_blocks, targets):
    picked, outgoing = project_call(visible, cameras, params)
    everyone = exchanged(spread_call(exchanged(outgoing, "view")), "tile")
    place = lax.axis_index("tile").astype(jnp.int32).reshape(1)
    image, sums = render_call(
        place, tile_blocks, tile_lists, jnp.transpose(targets, (1, 0, 2)), everyone
    )
    returned = exchanged(merge_call(exchanged(sums, "tile")), "view")
    new_params, new_first, new_second = update_call(
        visible, cameras, returned, kept(picked), kept(params), kept(first), kept(second)
    )
    return (new_params, new_first, new_second, jnp.transpose(image, (1, 0, 2)))


def solution(mesh):
    in_specs = (
        P(None, ("view", "tile")),
        P(None, ("view", "tile")),
        P(None, ("view", "tile")),
        P(None, ("view", "tile")),
        P(),
        P("view", "tile", None),
        P("view", "tile"),
        P("view", None, "tile"),
    )
    out_specs = (
        P(None, ("view", "tile")),
        P(None, ("view", "tile")),
        P(None, ("view", "tile")),
        P("view", None, "tile"),
    )
    return jax.shard_map(shards, mesh=mesh, in_specs=in_specs, out_specs=out_specs, check_vma=False)
```

```python
import functools

import jax
import jax.numpy as jnp
from jax import lax
from jax.experimental import pallas as pl
from jax.experimental.pallas import tpu as pltpu
from jax.sharding import PartitionSpec as P

SIDE = 16
PIX = 256
BLOCK = 128
WIN_COLS = 8


harm_zero = 0.28209479177387814
harm_one = 0.4886025119029199
harm_two = (
    1.0925484305920792,
    -1.0925484305920792,
    0.31539156525252005,
    -1.0925484305920792,
    0.5462742152960396,
)
harm_three = (
    -0.5900435899266435,
    2.890611442640554,
    -0.4570457994644658,
    0.3731763325901154,
    -0.4570457994644658,
    1.445305721320277,
    -0.5900435899266435,
)
learn_rate = 0.05
beta_first = 0.9
beta_second = 0.999
adam_eps = 1e-08
blur_add = 0.3


def rotation(real_part, axis_one, axis_two, axis_three):
    inverse = lax.rsqrt(
        real_part * real_part + axis_one * axis_one + axis_two * axis_two + axis_three * axis_three
    )
    real_unit = real_part * inverse
    unit_one = axis_one * inverse
    unit_two = axis_two * inverse
    unit_three = axis_three * inverse
    return (
        (
            1.0 - 2.0 * (unit_two * unit_two + unit_three * unit_three),
            2.0 * (unit_one * unit_two - real_unit * unit_three),
            2.0 * (unit_one * unit_three + real_unit * unit_two),
        ),
        (
            2.0 * (unit_one * unit_two + real_unit * unit_three),
            1.0 - 2.0 * (unit_one * unit_one + unit_three * unit_three),
            2.0 * (unit_two * unit_three - real_unit * unit_one),
        ),
        (
            2.0 * (unit_one * unit_three - real_unit * unit_two),
            2.0 * (unit_two * unit_three + real_unit * unit_one),
            1.0 - 2.0 * (unit_one * unit_one + unit_two * unit_two),
        ),
    )


def harmonics(first_dir, second_dir, third_dir):
    sq_first = first_dir * first_dir
    sq_second = second_dir * second_dir
    sq_third = third_dir * third_dir
    return [
        harm_zero,
        -harm_one * second_dir,
        harm_one * third_dir,
        -harm_one * first_dir,
        harm_two[0] * first_dir * second_dir,
        harm_two[1] * second_dir * third_dir,
        harm_two[2] * (2.0 * sq_third - sq_first - sq_second),
        harm_two[3] * first_dir * third_dir,
        harm_two[4] * (sq_first - sq_second),
        harm_three[0] * second_dir * (3.0 * sq_first - sq_second),
        harm_three[1] * first_dir * second_dir * third_dir,
        harm_three[2] * second_dir * (4.0 * sq_third - sq_first - sq_second),
        harm_three[3] * third_dir * (2.0 * sq_third - 3.0 * sq_first - 3.0 * sq_second),
        harm_three[4] * first_dir * (4.0 * sq_third - sq_first - sq_second),
        harm_three[5] * third_dir * (sq_first - sq_second),
        harm_three[6] * first_dir * (sq_first - 3.0 * sq_second),
    ]


def project(raw, camera):
    camera_turn = rotation(camera[0], camera[1], camera[2], camera[3])
    shift_vec = (camera[4], camera[5], camera[6])
    focal_x = camera[7]
    focal_y = camera[8]
    position = (raw[0], raw[1], raw[2])
    viewed = [
        camera_turn[across][0] * position[0]
        + camera_turn[across][1] * position[1]
        + camera_turn[across][2] * position[2]
        + shift_vec[across]
        for across in range(3)
    ]
    inverse = 1.0 / viewed[2]
    mean_x = focal_x * viewed[0] * inverse + camera[9]
    mean_y = focal_y * viewed[1] * inverse + camera[10]
    gauss_turn = rotation(raw[6], raw[7], raw[8], raw[9])
    stretch = [jnp.exp(raw[3 + column]) for column in range(3)]
    jac_xx = focal_x * inverse
    jac_xz = -focal_x * viewed[0] * inverse * inverse
    jac_yy = focal_y * inverse
    jac_yz = -focal_y * viewed[1] * inverse * inverse
    leading_x = [
        jac_xx * camera_turn[0][column] + jac_xz * camera_turn[2][column] for column in range(3)
    ]
    leading_y = [
        jac_yy * camera_turn[1][column] + jac_yz * camera_turn[2][column] for column in range(3)
    ]
    axes_x = [
        (
            leading_x[0] * gauss_turn[0][column]
            + leading_x[1] * gauss_turn[1][column]
            + leading_x[2] * gauss_turn[2][column]
        )
        * stretch[column]
        for column in range(3)
    ]
    axes_y = [
        (
            leading_y[0] * gauss_turn[0][column]
            + leading_y[1] * gauss_turn[1][column]
            + leading_y[2] * gauss_turn[2][column]
        )
        * stretch[column]
        for column in range(3)
    ]
    cov_xx = axes_x[0] * axes_x[0] + axes_x[1] * axes_x[1] + axes_x[2] * axes_x[2] + blur_add
    cov_xy = axes_x[0] * axes_y[0] + axes_x[1] * axes_y[1] + axes_x[2] * axes_y[2]
    cov_yy = axes_y[0] * axes_y[0] + axes_y[1] * axes_y[1] + axes_y[2] * axes_y[2] + blur_add
    determ = cov_xx * cov_yy - cov_xy * cov_xy
    opacity = jax.nn.sigmoid(raw[10])
    camera_eye = [
        -(
            camera_turn[0][column] * shift_vec[0]
            + camera_turn[1][column] * shift_vec[1]
            + camera_turn[2][column] * shift_vec[2]
        )
        for column in range(3)
    ]
    offset = [position[column] - camera_eye[column] for column in range(3)]
    length = lax.rsqrt(offset[0] * offset[0] + offset[1] * offset[1] + offset[2] * offset[2])
    harmonic_terms = harmonics(offset[0] * length, offset[1] * length, offset[2] * length)
    colours = []
    for channel in range(3):
        total = 0.5 + jnp.zeros_like(opacity)
        for harmonic in range(16):
            total = total + raw[11 + 16 * channel + harmonic] * harmonic_terms[harmonic]
        colours.append(total)
    return [mean_x, mean_y, cov_yy / determ, -cov_xy / determ, cov_xx / determ, opacity] + colours


F32 = jnp.float32
BF16 = jnp.bfloat16
PARAMS = 59
ROWS = 64
LOG2E = 1.4426950408889634


def iota(shape, dim):
    return lax.broadcasted_iota(jnp.int32, shape, dim)


def parts_of(value, count):
    parts = []
    for _ in range(count):
        part = value.astype(BF16)
        parts.append(part)
        value = value - part.astype(F32)
    return parts


def mm(left, right, dims):
    return lax.dot_general(left, right, (dims, ((), ())), preferred_element_type=F32)


def stacked(rows, width):
    sub = iota((8, width), 0)
    out = jnp.zeros((8, width), F32)
    for place, row in enumerate(rows):
        out = jnp.where(sub == place, jnp.broadcast_to(row, (8, width)), out)
    return out


def seen_columns(ids_ref, first, width):
    row = jnp.concatenate(
        [ids_ref[first + step : first + step + 1, :] for step in range(width // 64)], axis=1
    )
    return (iota((1024, width), 0) == row).astype(BF16)


def camera_arrays(cameras_ref):
    view = 2 * iota((8, 128), 0) + (iota((8, 128), 1) >= 64).astype(jnp.int32)
    masks = [view == index for index in range(16)]
    arrays = []
    for field in range(11):
        array = jnp.full((8, 128), cameras_ref[0, field], F32)
        for index in range(1, 16):
            array = jnp.where(masks[index], cameras_ref[index, field], array)
        arrays.append(array)
    return arrays


def raw_rows(picked_ref):
    return [picked_ref[pl.ds(row, 8, stride=ROWS), :] for row in range(PARAMS)]


def project_kernel(ids_ref, cameras_ref, params_ref, picked_ref, send_ref, split, swap):
    for place, part in enumerate(parts_of(params_ref[...], 3)):
        split[place * ROWS : place * ROWS + PARAMS, :] = part
    for pair in range(4):
        onehot = seen_columns(ids_ref, pair * 4, 256)
        three = mm(split[...], onehot, ((1,), (0,)))
        picked = three[0:ROWS] + three[ROWS : 2 * ROWS] + three[2 * ROWS :]
        picked_ref[pair * 128 : pair * 128 + ROWS, :] = picked[:, :128]
        picked_ref[pair * 128 + ROWS : pair * 128 + 2 * ROWS, :] = picked[:, 128:]
    values = project(raw_rows(picked_ref), camera_arrays(cameras_ref))
    for place in range(8):
        swap[place * 8 : place * 8 + 8, :] = values[place]
    low = iota((8, 128), 1) < 64
    for pair in range(8):
        main = swap[pl.ds(pair, 8, stride=8), :]
        last = jnp.broadcast_to(values[8][pair : pair + 1, :], (8, 128))
        send_ref[2 * pair] = jnp.where(low, main, pltpu.roll(last, 64, 1))
        send_ref[2 * pair + 1] = jnp.where(low, pltpu.roll(main, 64, 1), last)


def unpack_pair(even, odd):
    low = iota((8, 128), 1) < 64
    main = jnp.where(low, even, pltpu.roll(odd, 64, 1))
    last = jnp.where(low, pltpu.roll(even, 64, 1), odd)
    return main, last[0:1, :]


def spread_kernel(arrived_ref, out_ref):
    for pair in range(8):
        main, last = unpack_pair(arrived_ref[2 * pair], arrived_ref[2 * pair + 1])
        for peer in range(16):
            out_ref[peer, pair * 8 : pair * 8 + 8, :] = main
            out_ref[peer, 64 + pair : 65 + pair, :] = last


def prepare_kernel(after_ref, ids_ref, lists_ref, columns_ref, onehot_ref, lanes_ref, groups_ref):
    for pair in range(4):
        columns_ref[:, pair * 256 : pair * 256 + 256] = seen_columns(ids_ref, pair * 4, 256)
    turn = (iota((128, 1024), 0) == (iota((128, 1024), 1) >> 3)).astype(BF16)
    pick_block = iota((8, 1024), 0) == (iota((8, 1024), 1) & 7)
    for tile in range(2):
        blocks = [lists_ref[0, tile : tile + 1, start : start + 128] for start in range(0, 1024, 128)]
        low_part = stacked([(row & 127).astype(F32) for row in blocks], 128)
        high_part = stacked([(row >> 7).astype(F32) for row in blocks], 128)
        low_part = mm(low_part.astype(BF16), turn, ((1,), (0,)))
        high_part = mm(high_part.astype(BF16), turn, ((1,), (0,)))
        low_row = jnp.sum(jnp.where(pick_block, low_part, 0.0), axis=0, keepdims=True)
        high_row = jnp.sum(jnp.where(pick_block, high_part, 0.0), axis=0, keepdims=True)
        low_row = low_row.astype(jnp.int32)
        high_row = high_row.astype(jnp.int32)
        lane_index = ((high_row >> 3) & 1) * 128 + low_row
        span = slice(tile * 1024, tile * 1024 + 1024)
        onehot_ref[:, span] = (iota((256, 1024), 0) == lane_index).astype(BF16)
        lanes_ref[:, span] = jnp.broadcast_to(low_row, (8, 1024))
        groups_ref[:, span] = jnp.broadcast_to(high_row, (8, 1024))


def render_kernel(
    place_ref,
    counts_ref,
    onehot,
    lanes_of,
    chosen,
    targets_ref,
    everyone_ref,
    image_ref,
    out_ref,
    picked,
    alphas,
    weights,
    shades,
    summed,
):
    count = 2048
    def gather_chunk(chunk, carry):
        lanes = pl.ds(pl.multiple_of(chunk * 128, 128), 128)
        lane = lanes_of[:, lanes]
        group = chosen[:, lanes]
        sub = iota((8, 128), 0)
        zero = jnp.zeros((8, 128), F32)
        main = [zero, zero, zero, zero]
        last = [zero, zero]
        for peer in range(16):
            for place in range(8):
                found = jnp.take_along_axis(
                    everyone_ref[peer, place * 8 : place * 8 + 8, :], lane, axis=1
                )
                chain = place % 4
                main[chain] = jnp.where(group == peer * 8 + place, found, main[chain])
            found = jnp.take_along_axis(everyone_ref[peer, 64:72, :], lane, axis=1)
            last[peer % 2] = jnp.where(group == peer * 8 + sub, found, last[peer % 2])
        picked[0:8, lanes] = (main[0] + main[1]) + (main[2] + main[3])
        picked[8:16, lanes] = jnp.broadcast_to(
            jnp.sum(last[0] + last[1], axis=0, keepdims=True), (8, 128)
        )
        return carry

    lax.fori_loop(0, count // 128, gather_chunk, 0)

    pixel = iota((8, PIX), 1)
    pixel_x = (pixel & (SIDE - 1)).astype(F32) + (0.5 - SIDE / 2)
    pixel_y = (pixel >> 4).astype(F32) + (0.5 - SIDE / 2)
    sub = iota((8, PIX), 0)
    basis = jnp.where(sub == 0, 1.0, 0.0)
    for place, row in enumerate(
        [pixel_x, pixel_y, pixel_x * pixel_x, pixel_x * pixel_y, pixel_y * pixel_y]
    ):
        basis = jnp.where(sub == place + 1, row, basis)
    blank = jnp.zeros((8, PIX), F32)
    basis_three = jnp.concatenate([basis, basis, basis, blank], axis=0).astype(BF16)
    basis_once = jnp.concatenate([basis, blank], axis=0).astype(BF16)

    def rows_of(tile):
        span = slice(tile * 1024, tile * 1024 + 1024)
        held = picked[:, span]
        global_tile = place_ref[0] * 2 + tile
        centre_x = (global_tile % WIN_COLS * SIDE + SIDE // 2).astype(F32)
        centre_y = (global_tile // WIN_COLS * SIDE + SIDE // 2).astype(F32)
        rows = [held[place : place + 1, :] for place in range(9)]
        rows[0] = rows[0] - centre_x
        rows[1] = rows[1] - centre_y
        return rows

    block = iota((1, 1024), 1) & 7
    blank_row = jnp.zeros((8, 1024), F32)
    colour_rows = []
    for tile in range(2):
        mean_x, mean_y, con_a, con_b, con_c, opacity, *colour = rows_of(tile)
        live = block < counts_ref[0, tile]
        slope_x = con_a * mean_x + con_b * mean_y
        slope_y = con_b * mean_x + con_c * mean_y
        scale = -0.5 * LOG2E
        level = scale * (slope_x * mean_x + slope_y * mean_y) + jnp.log(opacity) * LOG2E
        terms = [
            jnp.where(live, level, -1000.0),
            jnp.where(live, (-2.0 * scale) * slope_x, 0.0),
            jnp.where(live, (-2.0 * scale) * slope_y, 0.0),
            jnp.where(live, scale * con_a, 0.0),
            jnp.where(live, (2.0 * scale) * con_b, 0.0),
            jnp.where(live, scale * con_c, 0.0),
        ]
        split = [part.astype(F32) for part in parts_of(stacked(terms, 1024), 3)]
        coefficients = jnp.concatenate(split + [blank_row], axis=0).astype(BF16)
        alphas[tile] = mm(coefficients, basis_three, ((0,), (0,)))
        colour_rows.append(stacked(colour, 1024))

    steps = 8

    def advance(outer, held):
        held = list(held)
        for inner in range(steps):
            start = pl.multiple_of((outer * steps + inner) * 8, 8)
            for tile in range(2):
                alpha = jnp.exp2(alphas[tile, pl.ds(start, 8), :])
                weight = alpha * held[tile]
                held[tile] = held[tile] * (1.0 - alpha)
                alphas[tile, pl.ds(start, 8), :] = alpha
                weights[tile, pl.ds(start, 8), :] = weight
        return tuple(held)

    ones = jnp.ones((8, PIX), F32)
    left = lax.fori_loop(0, 128 // steps, advance, (ones, ones))

    behind = []
    ahead = []
    blame = []
    sub_wide = iota((8, 1024), 0)
    block_wide = iota((8, 1024), 1) & 7
    for tile in range(2):
        colour = colour_rows[tile]
        separate = []
        for channel in range(3):
            row = jnp.broadcast_to(colour[channel : channel + 1, :], (8, 1024))
            separate.append(jnp.where(sub_wide == block_wide, row, 0.0))
        fine, rough = parts_of(jnp.concatenate(separate, axis=0), 2)
        both = jnp.concatenate([fine.astype(F32), rough.astype(F32)], axis=0).astype(BF16)
        first_part, second_part = parts_of(weights[tile], 2)
        sums = mm(both, first_part, ((1,), (0,))) + mm(both, second_part, ((1,), (0,)))
        passed = left[tile]
        total = passed
        for shift in (1, 2, 4):
            total = total * jnp.where(sub >= shift, pltpu.roll(total, shift, 0), 1.0)
        before = jnp.where(sub >= 1, pltpu.roll(total, 1, 0), 1.0)
        ahead.append(before)
        value = jnp.zeros((8, PIX), F32)
        slopes = []
        for channel in range(3):
            own = sums[channel * 8 : channel * 8 + 8, :]
            own = own + sums[24 + channel * 8 : 32 + channel * 8, :]
            image = jnp.sum(own * before, axis=0, keepdims=True)
            lanes = slice(tile * PIX, tile * PIX + PIX)
            image_ref[channel, :, lanes] = image
            slope = 2.0 * (image - targets_ref[channel, :, lanes])
            slopes.append(slope)
            value = value + slope * own
        factor = passed
        for shift in (1, 2, 4):
            inside = sub < 8 - shift
            value = value + factor * jnp.where(inside, pltpu.roll(value, 8 - shift, 0), 0.0)
            factor = factor * jnp.where(inside, pltpu.roll(factor, 8 - shift, 0), 1.0)
        behind.append(jnp.where(sub < 7, pltpu.roll(value, 7, 0), 0.0))
        slope_parts = [part.astype(F32) for part in parts_of(stacked(slopes, PIX), 3)]
        colour_parts = [part.astype(F32) for part in parts_of(colour, 3)]
        pairs = [(0, 0), (0, 1), (1, 0), (1, 1), (0, 2), (2, 0)]
        left_side = jnp.concatenate([colour_parts[a] for a, _ in pairs], axis=0).astype(BF16)
        right_side = jnp.concatenate([slope_parts[b] for _, b in pairs], axis=0).astype(BF16)
        shades[tile] = mm(left_side, right_side, ((0,), (0,)))
        blame.append(jnp.concatenate(slope_parts[:2], axis=0).astype(BF16))

    def retreat(outer, held):
        held = list(held)
        for inner in range(steps):
            start = pl.multiple_of((127 - (outer * steps + inner)) * 8, 8)
            for tile in range(2):
                alpha = alphas[tile, pl.ds(start, 8), :]
                weight = weights[tile, pl.ds(start, 8), :] * ahead[tile]
                shade = shades[tile, pl.ds(start, 8), :]
                shades[tile, pl.ds(start, 8), :] = weight * (shade - held[tile])
                held[tile] = held[tile] * (1.0 - alpha) + alpha * shade
                weights[tile, pl.ds(start, 8), :] = weight
        return tuple(held)

    lax.fori_loop(0, 128 // steps, retreat, tuple(behind))

    for tile in range(2):
        moments = sum(
            mm(basis_once, part, ((1,), (1,))) for part in parts_of(shades[tile], 3)
        )
        tints = sum(mm(blame[tile], part, ((1,), (1,))) for part in parts_of(weights[tile], 2))
        tints = tints[0:8, :] + tints[8:16, :]
        mean_x, mean_y, con_a, con_b, con_c, opacity, *_ = rows_of(tile)
        sum_one, sum_x, sum_y, sum_xx, sum_xy, sum_yy = [
            moments[place : place + 1, :] for place in range(6)
        ]
        near_x = sum_x - mean_x * sum_one
        near_y = sum_y - mean_y * sum_one
        near_xx = sum_xx - mean_x * (sum_x + near_x)
        near_xy = sum_xy - mean_x * sum_y - mean_y * near_x
        near_yy = sum_yy - mean_y * (sum_y + near_y)
        grads = [
            con_a * near_x + con_b * near_y,
            con_b * near_x + con_c * near_y,
            -0.5 * near_xx,
            -near_xy,
            -0.5 * near_yy,
            sum_one / opacity,
            tints[0:1, :],
            tints[1:2, :],
        ]
        span = slice(tile * 1024, tile * 1024 + 1024)
        picked[0:8, span] = stacked(grads, 1024)
        picked[8:16, span] = jnp.broadcast_to(tints[2:3, :], (8, 1024))

    wide = 512
    for chunk in range(count // wide):
        lanes = slice(chunk * wide, chunk * wide + wide)
        group = chosen[:, lanes]
        group = (group >> 4) * 8 + (group & 7)
        sub = iota((8, wide), 0)
        hot = onehot[:, lanes]
        main = [part.astype(F32) for part in parts_of(picked[0:8, lanes], 2)]
        last = [part.astype(F32) for part in parts_of(picked[8:16, lanes], 2)]
        total = None
        for part in range(2):
            rows = [jnp.where(group == place, main[part], 0.0) for place in range(64)]
            rows += [jnp.where(group == half * 8 + sub, last[part], 0.0) for half in range(8)]
            rows = [
                jnp.concatenate(rows[place : place + 2], axis=0).astype(BF16)
                for place in range(0, 72, 2)
            ]
            product = mm(jnp.concatenate(rows, axis=0), hot, ((1,), (1,)))
            total = product if total is None else total + product
        if chunk == 0:
            summed[...] = total
        elif chunk < count // wide - 1:
            summed[...] = summed[...] + total
        else:
            total = summed[...] + total
    for half in range(8):
        for side in range(2):
            lanes = slice(side * 128, side * 128 + 128)
            out_ref[2 * half + side, 0:64, :] = total[half * 64 : half * 64 + 64, lanes]
            out_ref[2 * half + side, 64:72, :] = total[512 + half * 8 : 520 + half * 8, lanes]


def merge_kernel(arrived_ref, send_ref):
    low = iota((8, 128), 1) < 64
    total = arrived_ref[0]
    for peer in range(1, 16):
        total = total + arrived_ref[peer]
    for pair in range(8):
        main = total[pair * 8 : pair * 8 + 8, :]
        last = jnp.broadcast_to(total[64 + pair : 65 + pair, :], (8, 128))
        send_ref[2 * pair] = jnp.where(low, main, pltpu.roll(last, 64, 1))
        send_ref[2 * pair + 1] = jnp.where(low, pltpu.roll(main, 64, 1), last)


def update_kernel(
    onehot_ref,
    cameras_ref,
    arrived_ref,
    picked_ref,
    params_ref,
    first_ref,
    second_ref,
    new_params_ref,
    new_first_ref,
    new_second_ref,
    swap,
    turned,
):
    lasts = []
    for pair in range(8):
        main, last = unpack_pair(arrived_ref[2 * pair], arrived_ref[2 * pair + 1])
        swap[pair * 8 : pair * 8 + 8, :] = main
        lasts.append(last)
    slopes = [swap[pl.ds(place, 8, stride=8), :] for place in range(8)]
    sub = iota((8, 128), 0)
    final = jnp.zeros((8, 128), F32)
    for pair in range(8):
        final = jnp.where(sub == pair, jnp.broadcast_to(lasts[pair], (8, 128)), final)
    slopes.append(final)
    cameras = camera_arrays(cameras_ref)
    _, pullback = jax.vjp(lambda source: project(source, cameras), raw_rows(picked_ref))
    (raw_grads,) = pullback(slopes)
    for row in range(PARAMS):
        turned[pl.ds(row, 8, stride=ROWS), :] = raw_grads[row]
    for row in range(PARAMS, ROWS):
        turned[pl.ds(row, 8, stride=ROWS), :] = jnp.ones((8, 128), F32)
    wide = jnp.concatenate([turned[pair * ROWS : pair * ROWS + ROWS, :] for pair in range(8)], axis=1)
    split = [part.astype(F32) for part in parts_of(wide, 3)]
    three = mm(jnp.concatenate(split, axis=0).astype(BF16), onehot_ref[...], ((1,), (1,)))
    summed = three[0:ROWS] + three[ROWS : 2 * ROWS] + three[2 * ROWS :]
    grad = summed[0:PARAMS, :]
    seen = summed[PARAMS : PARAMS + 1, :] > 0.5
    first = first_ref[...]
    second = second_ref[...]
    params = params_ref[...]
    moved_first = beta_first * first + (1.0 - beta_first) * grad
    moved_second = beta_second * second + (1.0 - beta_second) * grad * grad
    moved_params = params - learn_rate * moved_first / (jnp.sqrt(moved_second) + adam_eps)
    new_first_ref[...] = jnp.where(seen, moved_first, first)
    new_second_ref[...] = jnp.where(seen, moved_second, second)
    new_params_ref[...] = jnp.where(seen, moved_params, params)


SMEM = pl.BlockSpec(memory_space=pltpu.SMEM)
VMEM = pl.BlockSpec(memory_space=pltpu.VMEM)


def f32_shape(*shape):
    return jax.ShapeDtypeStruct(shape, F32)


def project_call(visible, cameras, params):
    return pl.pallas_call(
        project_kernel,
        out_shape=(f32_shape(512, 128), f32_shape(16, 8, 128)),
        in_specs=[VMEM, SMEM, VMEM],
        out_specs=(VMEM, VMEM),
        scratch_shapes=[pltpu.VMEM((192, 1024), BF16), pltpu.VMEM((64, 128), F32)],
        name="project",
    )(visible, cameras, params)


def spread_call(arrived):
    return pl.pallas_call(
        spread_kernel,
        out_shape=f32_shape(16, 72, 128),
        in_specs=[VMEM],
        out_specs=VMEM,
        name="spread",
    )(arrived)


def prepare_call(after, visible, lists):
    return pl.pallas_call(
        prepare_kernel,
        out_shape=(
            jax.ShapeDtypeStruct((1024, 1024), BF16),
            jax.ShapeDtypeStruct((256, 2048), BF16),
            jax.ShapeDtypeStruct((8, 2048), jnp.int32),
            jax.ShapeDtypeStruct((8, 2048), jnp.int32),
        ),
        in_specs=[pl.BlockSpec(memory_space=pl.ANY), VMEM, VMEM],
        out_specs=(VMEM, VMEM, VMEM, VMEM),
        name="prepare",
    )(after, visible, lists)


def render_call(place, counts, onehot, lanes, groups, targets, everyone):
    return pl.pallas_call(
        render_kernel,
        out_shape=(f32_shape(3, 1, 512), f32_shape(16, 72, 128)),
        in_specs=[SMEM, SMEM, VMEM, VMEM, VMEM, VMEM, VMEM],
        out_specs=(VMEM, VMEM),
        scratch_shapes=[
            pltpu.VMEM((16, 2048), F32),
            pltpu.VMEM((2, 1024, 256), F32),
            pltpu.VMEM((2, 1024, 256), F32),
            pltpu.VMEM((2, 1024, 256), F32),
            pltpu.VMEM((576, 256), F32),
        ],
        name="render",
    )(place, counts, onehot, lanes, groups, targets, everyone)


def merge_call(arrived):
    return pl.pallas_call(
        merge_kernel,
        out_shape=f32_shape(16, 8, 128),
        in_specs=[VMEM],
        out_specs=VMEM,
        name="merge",
    )(arrived)


def update_call(onehot, cameras, arrived, picked, params, first, second):
    shape = f32_shape(*params.shape)
    return pl.pallas_call(
        update_kernel,
        out_shape=(shape, shape, shape),
        in_specs=[VMEM, SMEM, VMEM, VMEM, VMEM, VMEM, VMEM],
        out_specs=(VMEM, VMEM, VMEM),
        scratch_shapes=[
            pltpu.VMEM((64, 128), F32),
            pltpu.VMEM((512, 128), F32),
        ],
        name="update",
    )(onehot, cameras, arrived, picked, params, first, second)


def kept(array):
    return pltpu.with_memory_space_constraint(array, pltpu.VMEM)


def exchanged(array, axis):
    return kept(lax.all_to_all(array, axis, 0, 0, tiled=True))


def shards(params, first, second, visible, cameras, tile_lists, tile_blocks, targets):
    picked, outgoing = project_call(visible, cameras, params)
    block = spread_call(exchanged(outgoing, "view"))
    everyone = exchanged(block, "tile")
    columns, onehot, lanes, groups = [
        kept(table) for table in prepare_call(block, visible, tile_lists)
    ]
    place = lax.axis_index("tile").astype(jnp.int32).reshape(1)
    image, sums = render_call(
        place,
        tile_blocks,
        onehot,
        lanes,
        groups,
        jnp.transpose(targets, (1, 0, 2)),
        everyone,
    )
    returned = exchanged(merge_call(exchanged(sums, "tile")), "view")
    new_params, new_first, new_second = update_call(
        columns, cameras, returned, kept(picked), kept(params), kept(first), kept(second)
    )
    return (new_params, new_first, new_second, jnp.transpose(image, (1, 0, 2)))


def solution(mesh):
    in_specs = (
        P(None, ("view", "tile")),
        P(None, ("view", "tile")),
        P(None, ("view", "tile")),
        P(None, ("view", "tile")),
        P(),
        P("view", "tile", None),
        P("view", "tile"),
        P("view", None, "tile"),
    )
    out_specs = (
        P(None, ("view", "tile")),
        P(None, ("view", "tile")),
        P(None, ("view", "tile")),
        P("view", None, "tile"),
    )
    return jax.shard_map(shards, mesh=mesh, in_specs=in_specs, out_specs=out_specs, check_vma=False)
```

```python
import functools

import jax
import jax.numpy as jnp
from jax import lax
from jax.experimental import pallas as pl
from jax.experimental.pallas import tpu as pltpu
from jax.sharding import PartitionSpec as P

SIDE = 16
PIX = 256
BLOCK = 128
WIN_COLS = 8


harm_zero = 0.28209479177387814
harm_one = 0.4886025119029199
harm_two = (
    1.0925484305920792,
    -1.0925484305920792,
    0.31539156525252005,
    -1.0925484305920792,
    0.5462742152960396,
)
harm_three = (
    -0.5900435899266435,
    2.890611442640554,
    -0.4570457994644658,
    0.3731763325901154,
    -0.4570457994644658,
    1.445305721320277,
    -0.5900435899266435,
)
learn_rate = 0.05
beta_first = 0.9
beta_second = 0.999
adam_eps = 1e-08
blur_add = 0.3


def rotation(real_part, axis_one, axis_two, axis_three):
    inverse = lax.rsqrt(
        real_part * real_part + axis_one * axis_one + axis_two * axis_two + axis_three * axis_three
    )
    real_unit = real_part * inverse
    unit_one = axis_one * inverse
    unit_two = axis_two * inverse
    unit_three = axis_three * inverse
    return (
        (
            1.0 - 2.0 * (unit_two * unit_two + unit_three * unit_three),
            2.0 * (unit_one * unit_two - real_unit * unit_three),
            2.0 * (unit_one * unit_three + real_unit * unit_two),
        ),
        (
            2.0 * (unit_one * unit_two + real_unit * unit_three),
            1.0 - 2.0 * (unit_one * unit_one + unit_three * unit_three),
            2.0 * (unit_two * unit_three - real_unit * unit_one),
        ),
        (
            2.0 * (unit_one * unit_three - real_unit * unit_two),
            2.0 * (unit_two * unit_three + real_unit * unit_one),
            1.0 - 2.0 * (unit_one * unit_one + unit_two * unit_two),
        ),
    )


def harmonics(first_dir, second_dir, third_dir):
    sq_first = first_dir * first_dir
    sq_second = second_dir * second_dir
    sq_third = third_dir * third_dir
    return [
        harm_zero,
        -harm_one * second_dir,
        harm_one * third_dir,
        -harm_one * first_dir,
        harm_two[0] * first_dir * second_dir,
        harm_two[1] * second_dir * third_dir,
        harm_two[2] * (2.0 * sq_third - sq_first - sq_second),
        harm_two[3] * first_dir * third_dir,
        harm_two[4] * (sq_first - sq_second),
        harm_three[0] * second_dir * (3.0 * sq_first - sq_second),
        harm_three[1] * first_dir * second_dir * third_dir,
        harm_three[2] * second_dir * (4.0 * sq_third - sq_first - sq_second),
        harm_three[3] * third_dir * (2.0 * sq_third - 3.0 * sq_first - 3.0 * sq_second),
        harm_three[4] * first_dir * (4.0 * sq_third - sq_first - sq_second),
        harm_three[5] * third_dir * (sq_first - sq_second),
        harm_three[6] * first_dir * (sq_first - 3.0 * sq_second),
    ]


def project(raw, camera):
    camera_turn = rotation(camera[0], camera[1], camera[2], camera[3])
    shift_vec = (camera[4], camera[5], camera[6])
    focal_x = camera[7]
    focal_y = camera[8]
    position = (raw[0], raw[1], raw[2])
    viewed = [
        camera_turn[across][0] * position[0]
        + camera_turn[across][1] * position[1]
        + camera_turn[across][2] * position[2]
        + shift_vec[across]
        for across in range(3)
    ]
    inverse = 1.0 / viewed[2]
    mean_x = focal_x * viewed[0] * inverse + camera[9]
    mean_y = focal_y * viewed[1] * inverse + camera[10]
    gauss_turn = rotation(raw[6], raw[7], raw[8], raw[9])
    stretch = [jnp.exp(raw[3 + column]) for column in range(3)]
    jac_xx = focal_x * inverse
    jac_xz = -focal_x * viewed[0] * inverse * inverse
    jac_yy = focal_y * inverse
    jac_yz = -focal_y * viewed[1] * inverse * inverse
    leading_x = [
        jac_xx * camera_turn[0][column] + jac_xz * camera_turn[2][column] for column in range(3)
    ]
    leading_y = [
        jac_yy * camera_turn[1][column] + jac_yz * camera_turn[2][column] for column in range(3)
    ]
    axes_x = [
        (
            leading_x[0] * gauss_turn[0][column]
            + leading_x[1] * gauss_turn[1][column]
            + leading_x[2] * gauss_turn[2][column]
        )
        * stretch[column]
        for column in range(3)
    ]
    axes_y = [
        (
            leading_y[0] * gauss_turn[0][column]
            + leading_y[1] * gauss_turn[1][column]
            + leading_y[2] * gauss_turn[2][column]
        )
        * stretch[column]
        for column in range(3)
    ]
    cov_xx = axes_x[0] * axes_x[0] + axes_x[1] * axes_x[1] + axes_x[2] * axes_x[2] + blur_add
    cov_xy = axes_x[0] * axes_y[0] + axes_x[1] * axes_y[1] + axes_x[2] * axes_y[2]
    cov_yy = axes_y[0] * axes_y[0] + axes_y[1] * axes_y[1] + axes_y[2] * axes_y[2] + blur_add
    determ = cov_xx * cov_yy - cov_xy * cov_xy
    opacity = jax.nn.sigmoid(raw[10])
    camera_eye = [
        -(
            camera_turn[0][column] * shift_vec[0]
            + camera_turn[1][column] * shift_vec[1]
            + camera_turn[2][column] * shift_vec[2]
        )
        for column in range(3)
    ]
    offset = [position[column] - camera_eye[column] for column in range(3)]
    length = lax.rsqrt(offset[0] * offset[0] + offset[1] * offset[1] + offset[2] * offset[2])
    harmonic_terms = harmonics(offset[0] * length, offset[1] * length, offset[2] * length)
    colours = []
    for channel in range(3):
        total = 0.5 + jnp.zeros_like(opacity)
        for harmonic in range(16):
            total = total + raw[11 + 16 * channel + harmonic] * harmonic_terms[harmonic]
        colours.append(total)
    return [mean_x, mean_y, cov_yy / determ, -cov_xy / determ, cov_xx / determ, opacity] + colours


F32 = jnp.float32
BF16 = jnp.bfloat16
PARAMS = 59
ROWS = 64
LOG2E = 1.4426950408889634
MIB = 1 << 20


def iota(shape, dim):
    return lax.broadcasted_iota(jnp.int32, shape, dim)


def parts_of(value, count):
    parts = []
    for _ in range(count):
        part = value.astype(BF16)
        parts.append(part)
        value = value - part.astype(F32)
    return parts


def mm(left, right, dims):
    return lax.dot_general(left, right, (dims, ((), ())), preferred_element_type=F32)


def stacked(rows, width):
    sub = iota((8, width), 0)
    out = jnp.zeros((8, width), F32)
    for place, row in enumerate(rows):
        out = jnp.where(sub == place, jnp.broadcast_to(row, (8, width)), out)
    return out


def seen_columns(ids_ref, first, width):
    row = jnp.concatenate(
        [ids_ref[first + step : first + step + 1, :] for step in range(width // 64)], axis=1
    )
    return (iota((1024, width), 0) == row).astype(BF16)


def camera_arrays(cameras_ref):
    view = 2 * iota((8, 128), 0) + (iota((8, 128), 1) >= 64).astype(jnp.int32)
    masks = [view == index for index in range(16)]
    arrays = []
    for field in range(11):
        array = jnp.full((8, 128), cameras_ref[0, field], F32)
        for index in range(1, 16):
            array = jnp.where(masks[index], cameras_ref[index, field], array)
        arrays.append(array)
    return arrays


def raw_rows(picked_ref):
    return [picked_ref[pl.ds(row, 8, stride=ROWS), :] for row in range(PARAMS)]


def project_kernel(ids_ref, cameras_ref, params_ref, picked_ref, send_ref, split, swap):
    for place, part in enumerate(parts_of(params_ref[...], 3)):
        split[place * ROWS : place * ROWS + PARAMS, :] = part
    for pair in range(4):
        onehot = seen_columns(ids_ref, pair * 4, 256)
        three = mm(split[...], onehot, ((1,), (0,)))
        picked = three[0:ROWS] + three[ROWS : 2 * ROWS] + three[2 * ROWS :]
        picked_ref[pair * 128 : pair * 128 + ROWS, :] = picked[:, :128]
        picked_ref[pair * 128 + ROWS : pair * 128 + 2 * ROWS, :] = picked[:, 128:]
    values = project(raw_rows(picked_ref), camera_arrays(cameras_ref))
    for place in range(8):
        swap[place * 8 : place * 8 + 8, :] = values[place]
    low = iota((8, 128), 1) < 64
    for pair in range(8):
        main = swap[pl.ds(pair, 8, stride=8), :]
        last = jnp.broadcast_to(values[8][pair : pair + 1, :], (8, 128))
        send_ref[2 * pair] = jnp.where(low, main, pltpu.roll(last, 64, 1))
        send_ref[2 * pair + 1] = jnp.where(low, pltpu.roll(main, 64, 1), last)


def unpack_pair(even, odd):
    low = iota((8, 128), 1) < 64
    main = jnp.where(low, even, pltpu.roll(odd, 64, 1))
    last = jnp.where(low, pltpu.roll(even, 64, 1), odd)
    return main, last[0:1, :]


def spread_kernel(arrived_ref, out_ref):
    for pair in range(8):
        main, last = unpack_pair(arrived_ref[2 * pair], arrived_ref[2 * pair + 1])
        for peer in range(16):
            out_ref[peer, pair * 8 : pair * 8 + 8, :] = main
            out_ref[peer, 64 + pair : 65 + pair, :] = last


def columns_kernel(after_ref, ids_ref, columns_ref):
    for pair in range(4):
        columns_ref[:, pair * 256 : pair * 256 + 256] = seen_columns(ids_ref, pair * 4, 256)


def prepare_kernel(after_ref, lists_ref, onehot_ref, lanes_ref, groups_ref):
    turn = (iota((128, 1024), 0) == (iota((128, 1024), 1) >> 3)).astype(BF16)
    pick_block = iota((8, 1024), 0) == (iota((8, 1024), 1) & 7)
    for tile in range(2):
        blocks = [lists_ref[0, tile : tile + 1, start : start + 128] for start in range(0, 1024, 128)]
        low_part = stacked([(row & 127).astype(F32) for row in blocks], 128)
        high_part = stacked([(row >> 7).astype(F32) for row in blocks], 128)
        low_part = mm(low_part.astype(BF16), turn, ((1,), (0,)))
        high_part = mm(high_part.astype(BF16), turn, ((1,), (0,)))
        low_row = jnp.sum(jnp.where(pick_block, low_part, 0.0), axis=0, keepdims=True)
        high_row = jnp.sum(jnp.where(pick_block, high_part, 0.0), axis=0, keepdims=True)
        low_row = low_row.astype(jnp.int32)
        high_row = high_row.astype(jnp.int32)
        lane_index = ((high_row >> 3) & 1) * 128 + low_row
        span = slice(tile * 1024, tile * 1024 + 1024)
        onehot_ref[:, span] = (iota((256, 1024), 0) == lane_index).astype(BF16)
        lanes_ref[:, span] = low_row
        groups_ref[:, span] = high_row


def render_kernel(
    place_ref,
    counts_ref,
    onehot,
    lanes_of,
    chosen,
    targets_ref,
    everyone_ref,
    image_ref,
    out_ref,
    picked,
    alphas,
    weights,
    shades,
    summed,
):
    count = 2048
    def gather_chunk(chunk, carry):
        lanes = pl.ds(pl.multiple_of(chunk * 128, 128), 128)
        lane = jnp.broadcast_to(lanes_of[:, lanes], (8, 128))
        group = jnp.broadcast_to(chosen[:, lanes], (8, 128))
        sub = iota((8, 128), 0)
        zero = jnp.zeros((8, 128), F32)
        main = [zero, zero, zero, zero]
        last = [zero, zero]
        for peer in range(16):
            for place in range(8):
                found = jnp.take_along_axis(
                    everyone_ref[peer, place * 8 : place * 8 + 8, :], lane, axis=1
                )
                chain = place % 4
                main[chain] = jnp.where(group == peer * 8 + place, found, main[chain])
            found = jnp.take_along_axis(everyone_ref[peer, 64:72, :], lane, axis=1)
            last[peer % 2] = jnp.where(group == peer * 8 + sub, found, last[peer % 2])
        picked[0:8, lanes] = (main[0] + main[1]) + (main[2] + main[3])
        picked[8:16, lanes] = jnp.broadcast_to(
            jnp.sum(last[0] + last[1], axis=0, keepdims=True), (8, 128)
        )
        return carry

    lax.fori_loop(0, count // 128, gather_chunk, 0)

    pixel = iota((8, PIX), 1)
    pixel_x = (pixel & (SIDE - 1)).astype(F32) + (0.5 - SIDE / 2)
    pixel_y = (pixel >> 4).astype(F32) + (0.5 - SIDE / 2)
    sub = iota((8, PIX), 0)
    basis = jnp.where(sub == 0, 1.0, 0.0)
    for place, row in enumerate(
        [pixel_x, pixel_y, pixel_x * pixel_x, pixel_x * pixel_y, pixel_y * pixel_y]
    ):
        basis = jnp.where(sub == place + 1, row, basis)
    blank = jnp.zeros((8, PIX), F32)
    basis_three = jnp.concatenate([basis, basis, basis, blank], axis=0).astype(BF16)
    basis_once = jnp.concatenate([basis, blank], axis=0).astype(BF16)

    def rows_of(tile):
        span = slice(tile * 1024, tile * 1024 + 1024)
        held = picked[:, span]
        global_tile = place_ref[0] * 2 + tile
        centre_x = (global_tile % WIN_COLS * SIDE + SIDE // 2).astype(F32)
        centre_y = (global_tile // WIN_COLS * SIDE + SIDE // 2).astype(F32)
        rows = [held[place : place + 1, :] for place in range(9)]
        rows[0] = rows[0] - centre_x
        rows[1] = rows[1] - centre_y
        return rows

    block = iota((1, 1024), 1) & 7
    blank_row = jnp.zeros((8, 1024), F32)
    colour_rows = []
    for tile in range(2):
        mean_x, mean_y, con_a, con_b, con_c, opacity, *colour = rows_of(tile)
        live = block < counts_ref[0, tile]
        slope_x = con_a * mean_x + con_b * mean_y
        slope_y = con_b * mean_x + con_c * mean_y
        scale = -0.5 * LOG2E
        level = scale * (slope_x * mean_x + slope_y * mean_y) + jnp.log(opacity) * LOG2E
        terms = [
            jnp.where(live, level, -1000.0),
            jnp.where(live, (-2.0 * scale) * slope_x, 0.0),
            jnp.where(live, (-2.0 * scale) * slope_y, 0.0),
            jnp.where(live, scale * con_a, 0.0),
            jnp.where(live, (2.0 * scale) * con_b, 0.0),
            jnp.where(live, scale * con_c, 0.0),
        ]
        split = [part.astype(F32) for part in parts_of(stacked(terms, 1024), 3)]
        coefficients = jnp.concatenate(split + [blank_row], axis=0).astype(BF16)
        alphas[tile] = mm(coefficients, basis_three, ((0,), (0,)))
        colour_rows.append(stacked(colour, 1024))

    steps = 8

    def advance(outer, held):
        held = list(held)
        for inner in range(steps):
            start = pl.multiple_of((outer * steps + inner) * 8, 8)
            for tile in range(2):
                alpha = jnp.exp2(alphas[tile, pl.ds(start, 8), :])
                weight = alpha * held[tile]
                held[tile] = held[tile] * (1.0 - alpha)
                alphas[tile, pl.ds(start, 8), :] = alpha
                weights[tile, pl.ds(start, 8), :] = weight
        return tuple(held)

    ones = jnp.ones((8, PIX), F32)
    left = lax.fori_loop(0, 128 // steps, advance, (ones, ones))

    behind = []
    ahead = []
    blame = []
    sub_wide = iota((8, 1024), 0)
    block_wide = iota((8, 1024), 1) & 7
    for tile in range(2):
        colour = colour_rows[tile]
        separate = []
        for channel in range(3):
            row = jnp.broadcast_to(colour[channel : channel + 1, :], (8, 1024))
            separate.append(jnp.where(sub_wide == block_wide, row, 0.0))
        fine, rough = parts_of(jnp.concatenate(separate, axis=0), 2)
        both = jnp.concatenate([fine.astype(F32), rough.astype(F32)], axis=0).astype(BF16)
        first_part, second_part = parts_of(weights[tile], 2)
        sums = mm(both, first_part, ((1,), (0,))) + mm(both, second_part, ((1,), (0,)))
        passed = left[tile]
        total = passed
        for shift in (1, 2, 4):
            total = total * jnp.where(sub >= shift, pltpu.roll(total, shift, 0), 1.0)
        before = jnp.where(sub >= 1, pltpu.roll(total, 1, 0), 1.0)
        ahead.append(before)
        value = jnp.zeros((8, PIX), F32)
        slopes = []
        for channel in range(3):
            own = sums[channel * 8 : channel * 8 + 8, :]
            own = own + sums[24 + channel * 8 : 32 + channel * 8, :]
            image = jnp.sum(own * before, axis=0, keepdims=True)
            lanes = slice(tile * PIX, tile * PIX + PIX)
            image_ref[channel, :, lanes] = image
            slope = 2.0 * (image - targets_ref[channel, :, lanes])
            slopes.append(slope)
            value = value + slope * own
        factor = passed
        for shift in (1, 2, 4):
            inside = sub < 8 - shift
            value = value + factor * jnp.where(inside, pltpu.roll(value, 8 - shift, 0), 0.0)
            factor = factor * jnp.where(inside, pltpu.roll(factor, 8 - shift, 0), 1.0)
        behind.append(jnp.where(sub < 7, pltpu.roll(value, 7, 0), 0.0))
        slope_parts = [part.astype(F32) for part in parts_of(stacked(slopes, PIX), 3)]
        colour_parts = [part.astype(F32) for part in parts_of(colour, 3)]
        pairs = [(0, 0), (0, 1), (1, 0), (1, 1), (0, 2), (2, 0)]
        left_side = jnp.concatenate([colour_parts[a] for a, _ in pairs], axis=0).astype(BF16)
        right_side = jnp.concatenate([slope_parts[b] for _, b in pairs], axis=0).astype(BF16)
        shades[tile] = mm(left_side, right_side, ((0,), (0,)))
        blame.append(jnp.concatenate(slope_parts[:2], axis=0).astype(BF16))

    def retreat(outer, held):
        held = list(held)
        for inner in range(steps):
            start = pl.multiple_of((127 - (outer * steps + inner)) * 8, 8)
            for tile in range(2):
                alpha = alphas[tile, pl.ds(start, 8), :]
                weight = weights[tile, pl.ds(start, 8), :] * ahead[tile]
                shade = shades[tile, pl.ds(start, 8), :]
                shades[tile, pl.ds(start, 8), :] = weight * (shade - held[tile])
                held[tile] = held[tile] * (1.0 - alpha) + alpha * shade
                weights[tile, pl.ds(start, 8), :] = weight
        return tuple(held)

    lax.fori_loop(0, 128 // steps, retreat, tuple(behind))

    for tile in range(2):
        moments = sum(
            mm(basis_once, part, ((1,), (1,))) for part in parts_of(shades[tile], 3)
        )
        tints = sum(mm(blame[tile], part, ((1,), (1,))) for part in parts_of(weights[tile], 2))
        tints = tints[0:8, :] + tints[8:16, :]
        mean_x, mean_y, con_a, con_b, con_c, opacity, *_ = rows_of(tile)
        sum_one, sum_x, sum_y, sum_xx, sum_xy, sum_yy = [
            moments[place : place + 1, :] for place in range(6)
        ]
        near_x = sum_x - mean_x * sum_one
        near_y = sum_y - mean_y * sum_one
        near_xx = sum_xx - mean_x * (sum_x + near_x)
        near_xy = sum_xy - mean_x * sum_y - mean_y * near_x
        near_yy = sum_yy - mean_y * (sum_y + near_y)
        grads = [
            con_a * near_x + con_b * near_y,
            con_b * near_x + con_c * near_y,
            -0.5 * near_xx,
            -near_xy,
            -0.5 * near_yy,
            sum_one / opacity,
            tints[0:1, :],
            tints[1:2, :],
        ]
        span = slice(tile * 1024, tile * 1024 + 1024)
        picked[0:8, span] = stacked(grads, 1024)
        picked[8:16, span] = jnp.broadcast_to(tints[2:3, :], (8, 1024))

    wide = 512
    for chunk in range(count // wide):
        lanes = slice(chunk * wide, chunk * wide + wide)
        group = chosen[:, lanes]
        group = jnp.broadcast_to((group >> 4) * 8 + (group & 7), (8, wide))
        sub = iota((8, wide), 0)
        hot = onehot[:, lanes]
        main = [part.astype(F32) for part in parts_of(picked[0:8, lanes], 2)]
        last = [part.astype(F32) for part in parts_of(picked[8:16, lanes], 2)]
        total = None
        for part in range(2):
            rows = [jnp.where(group == place, main[part], 0.0) for place in range(64)]
            rows += [jnp.where(group == half * 8 + sub, last[part], 0.0) for half in range(8)]
            rows = [
                jnp.concatenate(rows[place : place + 2], axis=0).astype(BF16)
                for place in range(0, 72, 2)
            ]
            product = mm(jnp.concatenate(rows, axis=0), hot, ((1,), (1,)))
            total = product if total is None else total + product
        if chunk == 0:
            summed[...] = total
        elif chunk < count // wide - 1:
            summed[...] = summed[...] + total
        else:
            total = summed[...] + total
    for half in range(8):
        for side in range(2):
            lanes = slice(side * 128, side * 128 + 128)
            out_ref[2 * half + side, 0:64, :] = total[half * 64 : half * 64 + 64, lanes]
            out_ref[2 * half + side, 64:72, :] = total[512 + half * 8 : 520 + half * 8, lanes]


def merge_kernel(arrived_ref, send_ref):
    low = iota((8, 128), 1) < 64
    total = arrived_ref[0]
    for peer in range(1, 16):
        total = total + arrived_ref[peer]
    for pair in range(8):
        main = total[pair * 8 : pair * 8 + 8, :]
        last = jnp.broadcast_to(total[64 + pair : 65 + pair, :], (8, 128))
        send_ref[2 * pair] = jnp.where(low, main, pltpu.roll(last, 64, 1))
        send_ref[2 * pair + 1] = jnp.where(low, pltpu.roll(main, 64, 1), last)


def update_kernel(
    onehot_ref,
    cameras_ref,
    arrived_ref,
    picked_ref,
    params_ref,
    first_ref,
    second_ref,
    new_params_ref,
    new_first_ref,
    new_second_ref,
    swap,
    turned,
):
    lasts = []
    for pair in range(8):
        main, last = unpack_pair(arrived_ref[2 * pair], arrived_ref[2 * pair + 1])
        swap[pair * 8 : pair * 8 + 8, :] = main
        lasts.append(last)
    slopes = [swap[pl.ds(place, 8, stride=8), :] for place in range(8)]
    sub = iota((8, 128), 0)
    final = jnp.zeros((8, 128), F32)
    for pair in range(8):
        final = jnp.where(sub == pair, jnp.broadcast_to(lasts[pair], (8, 128)), final)
    slopes.append(final)
    cameras = camera_arrays(cameras_ref)
    _, pullback = jax.vjp(lambda source: project(source, cameras), raw_rows(picked_ref))
    (raw_grads,) = pullback(slopes)
    for row in range(PARAMS):
        turned[pl.ds(row, 8, stride=ROWS), :] = raw_grads[row]
    for row in range(PARAMS, ROWS):
        turned[pl.ds(row, 8, stride=ROWS), :] = jnp.ones((8, 128), F32)
    wide = jnp.concatenate([turned[pair * ROWS : pair * ROWS + ROWS, :] for pair in range(8)], axis=1)
    split = [part.astype(F32) for part in parts_of(wide, 3)]
    three = mm(jnp.concatenate(split, axis=0).astype(BF16), onehot_ref[...], ((1,), (1,)))
    summed = three[0:ROWS] + three[ROWS : 2 * ROWS] + three[2 * ROWS :]
    grad = summed[0:PARAMS, :]
    seen = summed[PARAMS : PARAMS + 1, :] > 0.5
    first = first_ref[...]
    second = second_ref[...]
    params = params_ref[...]
    moved_first = beta_first * first + (1.0 - beta_first) * grad
    moved_second = beta_second * second + (1.0 - beta_second) * grad * grad
    moved_params = params - learn_rate * moved_first / (jnp.sqrt(moved_second) + adam_eps)
    new_first_ref[...] = jnp.where(seen, moved_first, first)
    new_second_ref[...] = jnp.where(seen, moved_second, second)
    new_params_ref[...] = jnp.where(seen, moved_params, params)


SMEM = pl.BlockSpec(memory_space=pltpu.SMEM)
VMEM = pl.BlockSpec(memory_space=pltpu.VMEM)


def f32_shape(*shape):
    return jax.ShapeDtypeStruct(shape, F32)


def project_call(visible, cameras, params):
    return pl.pallas_call(
        project_kernel,
        out_shape=(f32_shape(512, 128), f32_shape(16, 8, 128)),
        in_specs=[VMEM, SMEM, VMEM],
        out_specs=(VMEM, VMEM),
        scratch_shapes=[pltpu.VMEM((192, 1024), BF16), pltpu.VMEM((64, 128), F32)],
        compiler_params=pltpu.CompilerParams(vmem_limit_bytes=12 * MIB),
        name="project",
    )(visible, cameras, params)


def spread_call(arrived):
    return pl.pallas_call(
        spread_kernel,
        out_shape=f32_shape(16, 72, 128),
        in_specs=[VMEM],
        out_specs=VMEM,
        compiler_params=pltpu.CompilerParams(vmem_limit_bytes=6 * MIB),
        name="spread",
    )(arrived)


def columns_call(after, visible):
    return pl.pallas_call(
        columns_kernel,
        out_shape=jax.ShapeDtypeStruct((1024, 1024), BF16),
        in_specs=[pl.BlockSpec(memory_space=pl.ANY), VMEM],
        out_specs=VMEM,
        compiler_params=pltpu.CompilerParams(vmem_limit_bytes=8 * MIB),
        name="columns",
    )(after, visible)


def prepare_call(after, lists):
    return pl.pallas_call(
        prepare_kernel,
        out_shape=(
            jax.ShapeDtypeStruct((256, 2048), BF16),
            jax.ShapeDtypeStruct((1, 2048), jnp.int32),
            jax.ShapeDtypeStruct((1, 2048), jnp.int32),
        ),
        in_specs=[pl.BlockSpec(memory_space=pl.ANY), VMEM],
        out_specs=(VMEM, VMEM, VMEM),
        compiler_params=pltpu.CompilerParams(vmem_limit_bytes=16 * MIB),
        name="prepare",
    )(after, lists)


def render_call(place, counts, onehot, lanes, groups, targets, everyone):
    return pl.pallas_call(
        render_kernel,
        out_shape=(f32_shape(3, 1, 512), f32_shape(16, 72, 128)),
        in_specs=[SMEM, SMEM, VMEM, VMEM, VMEM, VMEM, VMEM],
        out_specs=(VMEM, VMEM),
        scratch_shapes=[
            pltpu.VMEM((16, 2048), F32),
            pltpu.VMEM((2, 1024, 256), F32),
            pltpu.VMEM((2, 1024, 256), F32),
            pltpu.VMEM((2, 1024, 256), F32),
            pltpu.VMEM((576, 256), F32),
        ],
        compiler_params=pltpu.CompilerParams(vmem_limit_bytes=24 * MIB),
        name="render",
    )(place, counts, onehot, lanes, groups, targets, everyone)


def merge_call(arrived):
    return pl.pallas_call(
        merge_kernel,
        out_shape=f32_shape(16, 8, 128),
        in_specs=[VMEM],
        out_specs=VMEM,
        compiler_params=pltpu.CompilerParams(vmem_limit_bytes=6 * MIB),
        name="merge",
    )(arrived)


def update_call(onehot, cameras, arrived, picked, params, first, second):
    shape = f32_shape(*params.shape)
    return pl.pallas_call(
        update_kernel,
        out_shape=(shape, shape, shape),
        in_specs=[VMEM, SMEM, VMEM, VMEM, VMEM, VMEM, VMEM],
        out_specs=(VMEM, VMEM, VMEM),
        scratch_shapes=[
            pltpu.VMEM((64, 128), F32),
            pltpu.VMEM((512, 128), F32),
        ],
        compiler_params=pltpu.CompilerParams(vmem_limit_bytes=16 * MIB),
        name="update",
    )(onehot, cameras, arrived, picked, params, first, second)


def kept(array):
    return pltpu.with_memory_space_constraint(array, pltpu.VMEM)


def exchanged(array, axis):
    return kept(lax.all_to_all(array, axis, 0, 0, tiled=True))


def shards(params, first, second, visible, cameras, tile_lists, tile_blocks, targets):
    picked, outgoing = project_call(visible, cameras, params)
    block = spread_call(exchanged(outgoing, "view"))
    everyone = exchanged(block, "tile")
    onehot, lanes, groups = [kept(table) for table in prepare_call(block, tile_lists)]
    place = lax.axis_index("tile").astype(jnp.int32).reshape(1)
    image, sums = render_call(
        place,
        tile_blocks,
        onehot,
        lanes,
        groups,
        jnp.transpose(targets, (1, 0, 2)),
        everyone,
    )
    merged = merge_call(exchanged(sums, "tile"))
    returned = exchanged(merged, "view")
    columns = kept(columns_call(merged, visible))
    new_params, new_first, new_second = update_call(
        columns, cameras, returned, kept(picked), kept(params), kept(first), kept(second)
    )
    return (new_params, new_first, new_second, jnp.transpose(image, (1, 0, 2)))


def solution(mesh):
    in_specs = (
        P(None, ("view", "tile")),
        P(None, ("view", "tile")),
        P(None, ("view", "tile")),
        P(None, ("view", "tile")),
        P(),
        P("view", "tile", None),
        P("view", "tile"),
        P("view", None, "tile"),
    )
    out_specs = (
        P(None, ("view", "tile")),
        P(None, ("view", "tile")),
        P(None, ("view", "tile")),
        P("view", None, "tile"),
    )
    return jax.shard_map(shards, mesh=mesh, in_specs=in_specs, out_specs=out_specs, check_vma=False)
```

```python
import functools

import jax
import jax.numpy as jnp
from jax import lax
from jax.experimental import pallas as pl
from jax.experimental.pallas import tpu as pltpu
from jax.sharding import PartitionSpec as P

SIDE = 16
PIX = 256
BLOCK = 128
WIN_COLS = 8


harm_zero = 0.28209479177387814
harm_one = 0.4886025119029199
harm_two = (
    1.0925484305920792,
    -1.0925484305920792,
    0.31539156525252005,
    -1.0925484305920792,
    0.5462742152960396,
)
harm_three = (
    -0.5900435899266435,
    2.890611442640554,
    -0.4570457994644658,
    0.3731763325901154,
    -0.4570457994644658,
    1.445305721320277,
    -0.5900435899266435,
)
learn_rate = 0.05
beta_first = 0.9
beta_second = 0.999
adam_eps = 1e-08
blur_add = 0.3


def rotation(real_part, axis_one, axis_two, axis_three):
    inverse = lax.rsqrt(
        real_part * real_part + axis_one * axis_one + axis_two * axis_two + axis_three * axis_three
    )
    real_unit = real_part * inverse
    unit_one = axis_one * inverse
    unit_two = axis_two * inverse
    unit_three = axis_three * inverse
    return (
        (
            1.0 - 2.0 * (unit_two * unit_two + unit_three * unit_three),
            2.0 * (unit_one * unit_two - real_unit * unit_three),
            2.0 * (unit_one * unit_three + real_unit * unit_two),
        ),
        (
            2.0 * (unit_one * unit_two + real_unit * unit_three),
            1.0 - 2.0 * (unit_one * unit_one + unit_three * unit_three),
            2.0 * (unit_two * unit_three - real_unit * unit_one),
        ),
        (
            2.0 * (unit_one * unit_three - real_unit * unit_two),
            2.0 * (unit_two * unit_three + real_unit * unit_one),
            1.0 - 2.0 * (unit_one * unit_one + unit_two * unit_two),
        ),
    )


def harmonics(first_dir, second_dir, third_dir):
    sq_first = first_dir * first_dir
    sq_second = second_dir * second_dir
    sq_third = third_dir * third_dir
    return [
        harm_zero,
        -harm_one * second_dir,
        harm_one * third_dir,
        -harm_one * first_dir,
        harm_two[0] * first_dir * second_dir,
        harm_two[1] * second_dir * third_dir,
        harm_two[2] * (2.0 * sq_third - sq_first - sq_second),
        harm_two[3] * first_dir * third_dir,
        harm_two[4] * (sq_first - sq_second),
        harm_three[0] * second_dir * (3.0 * sq_first - sq_second),
        harm_three[1] * first_dir * second_dir * third_dir,
        harm_three[2] * second_dir * (4.0 * sq_third - sq_first - sq_second),
        harm_three[3] * third_dir * (2.0 * sq_third - 3.0 * sq_first - 3.0 * sq_second),
        harm_three[4] * first_dir * (4.0 * sq_third - sq_first - sq_second),
        harm_three[5] * third_dir * (sq_first - sq_second),
        harm_three[6] * first_dir * (sq_first - 3.0 * sq_second),
    ]


def project(raw, camera):
    camera_turn = rotation(camera[0], camera[1], camera[2], camera[3])
    shift_vec = (camera[4], camera[5], camera[6])
    focal_x = camera[7]
    focal_y = camera[8]
    position = (raw[0], raw[1], raw[2])
    viewed = [
        camera_turn[across][0] * position[0]
        + camera_turn[across][1] * position[1]
        + camera_turn[across][2] * position[2]
        + shift_vec[across]
        for across in range(3)
    ]
    inverse = 1.0 / viewed[2]
    mean_x = focal_x * viewed[0] * inverse + camera[9]
    mean_y = focal_y * viewed[1] * inverse + camera[10]
    gauss_turn = rotation(raw[6], raw[7], raw[8], raw[9])
    stretch = [jnp.exp(raw[3 + column]) for column in range(3)]
    jac_xx = focal_x * inverse
    jac_xz = -focal_x * viewed[0] * inverse * inverse
    jac_yy = focal_y * inverse
    jac_yz = -focal_y * viewed[1] * inverse * inverse
    leading_x = [
        jac_xx * camera_turn[0][column] + jac_xz * camera_turn[2][column] for column in range(3)
    ]
    leading_y = [
        jac_yy * camera_turn[1][column] + jac_yz * camera_turn[2][column] for column in range(3)
    ]
    axes_x = [
        (
            leading_x[0] * gauss_turn[0][column]
            + leading_x[1] * gauss_turn[1][column]
            + leading_x[2] * gauss_turn[2][column]
        )
        * stretch[column]
        for column in range(3)
    ]
    axes_y = [
        (
            leading_y[0] * gauss_turn[0][column]
            + leading_y[1] * gauss_turn[1][column]
            + leading_y[2] * gauss_turn[2][column]
        )
        * stretch[column]
        for column in range(3)
    ]
    cov_xx = axes_x[0] * axes_x[0] + axes_x[1] * axes_x[1] + axes_x[2] * axes_x[2] + blur_add
    cov_xy = axes_x[0] * axes_y[0] + axes_x[1] * axes_y[1] + axes_x[2] * axes_y[2]
    cov_yy = axes_y[0] * axes_y[0] + axes_y[1] * axes_y[1] + axes_y[2] * axes_y[2] + blur_add
    determ = cov_xx * cov_yy - cov_xy * cov_xy
    opacity = jax.nn.sigmoid(raw[10])
    camera_eye = [
        -(
            camera_turn[0][column] * shift_vec[0]
            + camera_turn[1][column] * shift_vec[1]
            + camera_turn[2][column] * shift_vec[2]
        )
        for column in range(3)
    ]
    offset = [position[column] - camera_eye[column] for column in range(3)]
    length = lax.rsqrt(offset[0] * offset[0] + offset[1] * offset[1] + offset[2] * offset[2])
    harmonic_terms = harmonics(offset[0] * length, offset[1] * length, offset[2] * length)
    colours = []
    for channel in range(3):
        total = 0.5 + jnp.zeros_like(opacity)
        for harmonic in range(16):
            total = total + raw[11 + 16 * channel + harmonic] * harmonic_terms[harmonic]
        colours.append(total)
    return [mean_x, mean_y, cov_yy / determ, -cov_xy / determ, cov_xx / determ, opacity] + colours


F32 = jnp.float32
BF16 = jnp.bfloat16
PARAMS = 59
ROWS = 64
LOG2E = 1.4426950408889634
MIB = 1 << 20
MIXED = 8


def iota(shape, dim):
    return lax.broadcasted_iota(jnp.int32, shape, dim)


def parts_of(value, count):
    parts = []
    for _ in range(count):
        part = value.astype(BF16)
        parts.append(part)
        value = value - part.astype(F32)
    return parts


def mm(left, right, dims):
    return lax.dot_general(left, right, (dims, ((), ())), preferred_element_type=F32)


def stacked(rows, width):
    sub = iota((8, width), 0)
    out = jnp.zeros((8, width), F32)
    for place, row in enumerate(rows):
        out = jnp.where(sub == place, jnp.broadcast_to(row, (8, width)), out)
    return out


def seen_columns(ids_ref, first, width):
    row = jnp.concatenate(
        [ids_ref[first + step : first + step + 1, :] for step in range(width // 64)], axis=1
    )
    return (iota((1024, width), 0) == row).astype(BF16)


def camera_arrays(cameras_ref):
    view = 2 * iota((8, 128), 0) + (iota((8, 128), 1) >= 64).astype(jnp.int32)
    masks = [view == index for index in range(16)]
    arrays = []
    for field in range(11):
        array = jnp.full((8, 128), cameras_ref[0, field], F32)
        for index in range(1, 16):
            array = jnp.where(masks[index], cameras_ref[index, field], array)
        arrays.append(array)
    return arrays


def raw_rows(picked_ref):
    return [picked_ref[pl.ds(row, 8, stride=ROWS), :] for row in range(PARAMS)]


def project_kernel(ids_ref, cameras_ref, params_ref, picked_ref, send_ref, split, swap):
    for place, part in enumerate(parts_of(params_ref[...], 3)):
        split[place * ROWS : place * ROWS + PARAMS, :] = part
    for pair in range(4):
        onehot = seen_columns(ids_ref, pair * 4, 256)
        three = mm(split[...], onehot, ((1,), (0,)))
        picked = three[0:ROWS] + three[ROWS : 2 * ROWS] + three[2 * ROWS :]
        picked_ref[pair * 128 : pair * 128 + ROWS, :] = picked[:, :128]
        picked_ref[pair * 128 + ROWS : pair * 128 + 2 * ROWS, :] = picked[:, 128:]
    values = project(raw_rows(picked_ref), camera_arrays(cameras_ref))
    for place in range(8):
        swap[place * 8 : place * 8 + 8, :] = values[place]
    low = iota((8, 128), 1) < 64
    for pair in range(8):
        main = swap[pl.ds(pair, 8, stride=8), :]
        last = jnp.broadcast_to(values[8][pair : pair + 1, :], (8, 128))
        send_ref[2 * pair] = jnp.where(low, main, pltpu.roll(last, 64, 1))
        send_ref[2 * pair + 1] = jnp.where(low, pltpu.roll(main, 64, 1), last)


def unpack_pair(even, odd):
    low = iota((8, 128), 1) < 64
    main = jnp.where(low, even, pltpu.roll(odd, 64, 1))
    last = jnp.where(low, pltpu.roll(even, 64, 1), odd)
    return main, last[0:1, :]


def spread_kernel(arrived_ref, out_ref):
    for pair in range(8):
        main, last = unpack_pair(arrived_ref[2 * pair], arrived_ref[2 * pair + 1])
        for peer in range(16):
            out_ref[peer, pair * 8 : pair * 8 + 8, :] = main
            out_ref[peer, 64 + pair : 65 + pair, :] = last


def columns_kernel(after_ref, ids_ref, columns_ref):
    for pair in range(4):
        columns_ref[:, pair * 256 : pair * 256 + 256] = seen_columns(ids_ref, pair * 4, 256)


def prepare_kernel(after_ref, lists_ref, onehot_ref, lanes_ref, groups_ref):
    turn = (iota((128, 1024), 0) == (iota((128, 1024), 1) >> 3)).astype(BF16)
    pick_block = iota((8, 1024), 0) == (iota((8, 1024), 1) & 7)
    for tile in range(2):
        blocks = [lists_ref[0, tile : tile + 1, start : start + 128] for start in range(0, 1024, 128)]
        low_part = stacked([(row & 127).astype(F32) for row in blocks], 128)
        high_part = stacked([(row >> 7).astype(F32) for row in blocks], 128)
        low_part = mm(low_part.astype(BF16), turn, ((1,), (0,)))
        high_part = mm(high_part.astype(BF16), turn, ((1,), (0,)))
        low_row = jnp.sum(jnp.where(pick_block, low_part, 0.0), axis=0, keepdims=True)
        high_row = jnp.sum(jnp.where(pick_block, high_part, 0.0), axis=0, keepdims=True)
        low_row = low_row.astype(jnp.int32)
        high_row = high_row.astype(jnp.int32)
        lane_index = ((high_row >> 3) & 1) * 128 + low_row
        span = slice(tile * 1024, tile * 1024 + 1024)
        onehot_ref[:, span] = (iota((256, 1024), 0) == lane_index).astype(BF16)
        lanes_ref[:, span] = low_row
        groups_ref[:, span] = high_row


def render_kernel(
    place_ref,
    counts_ref,
    onehot,
    lanes_of,
    chosen,
    targets_ref,
    everyone_ref,
    image_ref,
    out_ref,
    picked,
    alphas,
    weights,
    shades,
    summed,
    table,
):
    count = 2048
    for half in range(MIXED // 2):
        for side in range(2):
            lanes = slice(side * 128, side * 128 + 128)
            main = parts_of(everyone_ref[2 * half + side, 0:64, :], 3)
            last = parts_of(everyone_ref[2 * half + side, 64:72, :], 3)
            for part in range(3):
                table[part, half * 64 : half * 64 + 64, lanes] = main[part]
                start = MIXED * 32 + half * 8
                table[part, start : start + 8, lanes] = last[part]

    def gather_chunk(chunk, carry):
        lanes = pl.ds(pl.multiple_of(chunk * 256, 256), 256)
        hot = onehot[:, lanes]
        found = mm(table[0], hot, ((1,), (0,)))
        found = found + mm(table[1], hot, ((1,), (0,)))
        found = found + mm(table[2], hot, ((1,), (0,)))
        both = jnp.broadcast_to(chosen[:, lanes], (8, 256))
        pair = (both >> 4) * 8 + (both & 7)
        sub = iota((8, 256), 0)
        zero = jnp.zeros((8, 256), F32)
        main = [zero, zero]
        last = zero
        for half in range(MIXED // 2):
            for place in range(8):
                start = half * 64 + place * 8
                main[place % 2] = jnp.where(
                    pair == half * 8 + place, found[start : start + 8, :], main[place % 2]
                )
            start = MIXED * 32 + half * 8
            last = jnp.where(pair == half * 8 + sub, found[start : start + 8, :], last)
        main = main[0] + main[1]
        sub = iota((8, 128), 0)
        zero = jnp.zeros((8, 128), F32)
        for side in range(2):
            cut = slice(side * 128, side * 128 + 128)
            lanes = pl.ds(pl.multiple_of(chunk * 256 + side * 128, 128), 128)
            lane = jnp.broadcast_to(lanes_of[:, lanes], (8, 128))
            group = both[:, cut]
            chains = [main[:, cut], zero, zero, zero]
            ends = [last[:, cut], zero]
            for peer in range(MIXED, 16):
                for place in range(8):
                    value = jnp.take_along_axis(
                        everyone_ref[peer, place * 8 : place * 8 + 8, :], lane, axis=1
                    )
                    chain = place % 4
                    chains[chain] = jnp.where(group == peer * 8 + place, value, chains[chain])
                value = jnp.take_along_axis(everyone_ref[peer, 64:72, :], lane, axis=1)
                ends[peer % 2] = jnp.where(group == peer * 8 + sub, value, ends[peer % 2])
            picked[0:8, lanes] = (chains[0] + chains[1]) + (chains[2] + chains[3])
            picked[8:16, lanes] = jnp.broadcast_to(
                jnp.sum(ends[0] + ends[1], axis=0, keepdims=True), (8, 128)
            )
        return carry

    lax.fori_loop(0, count // 256, gather_chunk, 0)

    pixel = iota((8, PIX), 1)
    pixel_x = (pixel & (SIDE - 1)).astype(F32) + (0.5 - SIDE / 2)
    pixel_y = (pixel >> 4).astype(F32) + (0.5 - SIDE / 2)
    sub = iota((8, PIX), 0)
    basis = jnp.where(sub == 0, 1.0, 0.0)
    for place, row in enumerate(
        [pixel_x, pixel_y, pixel_x * pixel_x, pixel_x * pixel_y, pixel_y * pixel_y]
    ):
        basis = jnp.where(sub == place + 1, row, basis)
    blank = jnp.zeros((8, PIX), F32)
    basis_three = jnp.concatenate([basis, basis, basis, blank], axis=0).astype(BF16)
    basis_once = jnp.concatenate([basis, blank], axis=0).astype(BF16)

    def rows_of(tile):
        span = slice(tile * 1024, tile * 1024 + 1024)
        held = picked[:, span]
        global_tile = place_ref[0] * 2 + tile
        centre_x = (global_tile % WIN_COLS * SIDE + SIDE // 2).astype(F32)
        centre_y = (global_tile // WIN_COLS * SIDE + SIDE // 2).astype(F32)
        rows = [held[place : place + 1, :] for place in range(9)]
        rows[0] = rows[0] - centre_x
        rows[1] = rows[1] - centre_y
        return rows

    block = iota((1, 1024), 1) & 7
    blank_row = jnp.zeros((8, 1024), F32)
    colour_rows = []
    for tile in range(2):
        mean_x, mean_y, con_a, con_b, con_c, opacity, *colour = rows_of(tile)
        live = block < counts_ref[0, tile]
        slope_x = con_a * mean_x + con_b * mean_y
        slope_y = con_b * mean_x + con_c * mean_y
        scale = -0.5 * LOG2E
        level = scale * (slope_x * mean_x + slope_y * mean_y) + jnp.log(opacity) * LOG2E
        terms = [
            jnp.where(live, level, -1000.0),
            jnp.where(live, (-2.0 * scale) * slope_x, 0.0),
            jnp.where(live, (-2.0 * scale) * slope_y, 0.0),
            jnp.where(live, scale * con_a, 0.0),
            jnp.where(live, (2.0 * scale) * con_b, 0.0),
            jnp.where(live, scale * con_c, 0.0),
        ]
        split = [part.astype(F32) for part in parts_of(stacked(terms, 1024), 3)]
        coefficients = jnp.concatenate(split + [blank_row], axis=0).astype(BF16)
        alphas[tile] = mm(coefficients, basis_three, ((0,), (0,)))
        colour_rows.append(stacked(colour, 1024))

    steps = 8

    def advance(outer, held):
        held = list(held)
        for inner in range(steps):
            start = pl.multiple_of((outer * steps + inner) * 8, 8)
            for tile in range(2):
                alpha = jnp.exp2(alphas[tile, pl.ds(start, 8), :])
                weight = alpha * held[tile]
                held[tile] = held[tile] * (1.0 - alpha)
                weights[tile, pl.ds(start, 8), :] = weight
        return tuple(held)

    ones = jnp.ones((8, PIX), F32)
    left = lax.fori_loop(0, 128 // steps, advance, (ones, ones))

    behind = []
    ahead = []
    blame = []
    sub_wide = iota((8, 1024), 0)
    block_wide = iota((8, 1024), 1) & 7
    for tile in range(2):
        colour = colour_rows[tile]
        separate = []
        for channel in range(3):
            row = jnp.broadcast_to(colour[channel : channel + 1, :], (8, 1024))
            separate.append(jnp.where(sub_wide == block_wide, row, 0.0))
        fine, rough = parts_of(jnp.concatenate(separate, axis=0), 2)
        both = jnp.concatenate([fine.astype(F32), rough.astype(F32)], axis=0).astype(BF16)
        first_part, second_part = parts_of(weights[tile], 2)
        sums = mm(both, first_part, ((1,), (0,))) + mm(both, second_part, ((1,), (0,)))
        passed = left[tile]
        total = passed
        for shift in (1, 2, 4):
            total = total * jnp.where(sub >= shift, pltpu.roll(total, shift, 0), 1.0)
        before = jnp.where(sub >= 1, pltpu.roll(total, 1, 0), 1.0)
        ahead.append(before)
        value = jnp.zeros((8, PIX), F32)
        slopes = []
        for channel in range(3):
            own = sums[channel * 8 : channel * 8 + 8, :]
            own = own + sums[24 + channel * 8 : 32 + channel * 8, :]
            image = jnp.sum(own * before, axis=0, keepdims=True)
            lanes = slice(tile * PIX, tile * PIX + PIX)
            image_ref[channel, :, lanes] = image
            slope = 2.0 * (image - targets_ref[channel, :, lanes])
            slopes.append(slope)
            value = value + slope * own
        factor = passed
        for shift in (1, 2, 4):
            inside = sub < 8 - shift
            value = value + factor * jnp.where(inside, pltpu.roll(value, 8 - shift, 0), 0.0)
            factor = factor * jnp.where(inside, pltpu.roll(factor, 8 - shift, 0), 1.0)
        behind.append(jnp.where(sub < 7, pltpu.roll(value, 7, 0), 0.0))
        slope_parts = [part.astype(F32) for part in parts_of(stacked(slopes, PIX), 3)]
        colour_parts = [part.astype(F32) for part in parts_of(colour, 3)]
        pairs = [(0, 0), (0, 1), (1, 0), (1, 1), (0, 2), (2, 0)]
        left_side = jnp.concatenate([colour_parts[a] for a, _ in pairs], axis=0).astype(BF16)
        right_side = jnp.concatenate([slope_parts[b] for _, b in pairs], axis=0).astype(BF16)
        shades[tile] = mm(left_side, right_side, ((0,), (0,)))
        blame.append(jnp.concatenate(slope_parts[:2], axis=0).astype(BF16))

    def retreat(outer, held):
        held = list(held)
        for inner in range(steps):
            start = pl.multiple_of((127 - (outer * steps + inner)) * 8, 8)
            for tile in range(2):
                alpha = jnp.exp2(alphas[tile, pl.ds(start, 8), :])
                weight = weights[tile, pl.ds(start, 8), :] * ahead[tile]
                shade = shades[tile, pl.ds(start, 8), :]
                shades[tile, pl.ds(start, 8), :] = weight * (shade - held[tile])
                held[tile] = held[tile] * (1.0 - alpha) + alpha * shade
                weights[tile, pl.ds(start, 8), :] = weight
        return tuple(held)

    lax.fori_loop(0, 128 // steps, retreat, tuple(behind))

    for tile in range(2):
        moments = sum(
            mm(basis_once, part, ((1,), (1,))) for part in parts_of(shades[tile], 3)
        )
        tints = sum(mm(blame[tile], part, ((1,), (1,))) for part in parts_of(weights[tile], 2))
        tints = tints[0:8, :] + tints[8:16, :]
        mean_x, mean_y, con_a, con_b, con_c, opacity, *_ = rows_of(tile)
        sum_one, sum_x, sum_y, sum_xx, sum_xy, sum_yy = [
            moments[place : place + 1, :] for place in range(6)
        ]
        near_x = sum_x - mean_x * sum_one
        near_y = sum_y - mean_y * sum_one
        near_xx = sum_xx - mean_x * (sum_x + near_x)
        near_xy = sum_xy - mean_x * sum_y - mean_y * near_x
        near_yy = sum_yy - mean_y * (sum_y + near_y)
        grads = [
            con_a * near_x + con_b * near_y,
            con_b * near_x + con_c * near_y,
            -0.5 * near_xx,
            -near_xy,
            -0.5 * near_yy,
            sum_one / opacity,
            tints[0:1, :],
            tints[1:2, :],
        ]
        span = slice(tile * 1024, tile * 1024 + 1024)
        picked[0:8, span] = stacked(grads, 1024)
        picked[8:16, span] = jnp.broadcast_to(tints[2:3, :], (8, 1024))

    wide = 512
    for chunk in range(count // wide):
        lanes = slice(chunk * wide, chunk * wide + wide)
        group = chosen[:, lanes]
        group = jnp.broadcast_to((group >> 4) * 8 + (group & 7), (8, wide))
        sub = iota((8, wide), 0)
        hot = onehot[:, lanes]
        main = [part.astype(F32) for part in parts_of(picked[0:8, lanes], 2)]
        last = [part.astype(F32) for part in parts_of(picked[8:16, lanes], 2)]
        total = None
        for part in range(2):
            rows = [jnp.where(group == place, main[part], 0.0) for place in range(64)]
            rows += [jnp.where(group == half * 8 + sub, last[part], 0.0) for half in range(8)]
            rows = [
                jnp.concatenate(rows[place : place + 2], axis=0).astype(BF16)
                for place in range(0, 72, 2)
            ]
            product = mm(jnp.concatenate(rows, axis=0), hot, ((1,), (1,)))
            total = product if total is None else total + product
        if chunk == 0:
            summed[...] = total
        elif chunk < count // wide - 1:
            summed[...] = summed[...] + total
        else:
            total = summed[...] + total
    for half in range(8):
        for side in range(2):
            lanes = slice(side * 128, side * 128 + 128)
            out_ref[2 * half + side, 0:64, :] = total[half * 64 : half * 64 + 64, lanes]
            out_ref[2 * half + side, 64:72, :] = total[512 + half * 8 : 520 + half * 8, lanes]


def merge_kernel(arrived_ref, send_ref):
    low = iota((8, 128), 1) < 64
    total = arrived_ref[0]
    for peer in range(1, 16):
        total = total + arrived_ref[peer]
    for pair in range(8):
        main = total[pair * 8 : pair * 8 + 8, :]
        last = jnp.broadcast_to(total[64 + pair : 65 + pair, :], (8, 128))
        send_ref[2 * pair] = jnp.where(low, main, pltpu.roll(last, 64, 1))
        send_ref[2 * pair + 1] = jnp.where(low, pltpu.roll(main, 64, 1), last)


def update_kernel(
    onehot_ref,
    cameras_ref,
    arrived_ref,
    picked_ref,
    params_ref,
    first_ref,
    second_ref,
    new_params_ref,
    new_first_ref,
    new_second_ref,
    swap,
    turned,
    stage,
    leaving,
):
    lasts = []
    for pair in range(8):
        main, last = unpack_pair(arrived_ref[2 * pair], arrived_ref[2 * pair + 1])
        swap[pair * 8 : pair * 8 + 8, :] = main
        lasts.append(last)
    slopes = [swap[pl.ds(place, 8, stride=8), :] for place in range(8)]
    sub = iota((8, 128), 0)
    final = jnp.zeros((8, 128), F32)
    for pair in range(8):
        final = jnp.where(sub == pair, jnp.broadcast_to(lasts[pair], (8, 128)), final)
    slopes.append(final)
    cameras = camera_arrays(cameras_ref)
    _, pullback = jax.vjp(lambda source: project(source, cameras), raw_rows(picked_ref))
    (raw_grads,) = pullback(slopes)
    for row in range(PARAMS):
        turned[pl.ds(row, 8, stride=ROWS), :] = raw_grads[row]
    for row in range(PARAMS, ROWS):
        turned[pl.ds(row, 8, stride=ROWS), :] = jnp.ones((8, 128), F32)
    wide = jnp.concatenate([turned[pair * ROWS : pair * ROWS + ROWS, :] for pair in range(8)], axis=1)
    split = [part.astype(F32) for part in parts_of(wide, 3)]
    three = mm(jnp.concatenate(split, axis=0).astype(BF16), onehot_ref[...], ((1,), (1,)))
    summed = three[0:ROWS] + three[ROWS : 2 * ROWS] + three[2 * ROWS :]
    seen = summed[PARAMS : PARAMS + 1, :] > 0.5
    outs = (new_params_ref, new_first_ref, new_second_ref)
    copies = []
    for place, start in enumerate(range(0, PARAMS, 16)):
        rows = slice(start, min(start + 16, PARAMS))
        grad = summed[rows, :]
        first = first_ref[rows, :]
        second = second_ref[rows, :]
        params = params_ref[rows, :]
        moved_first = beta_first * first + (1.0 - beta_first) * grad
        moved_second = beta_second * second + (1.0 - beta_second) * grad * grad
        moved_params = params - learn_rate * moved_first / (jnp.sqrt(moved_second) + adam_eps)
        values = (
            jnp.where(seen, moved_params, params),
            jnp.where(seen, moved_first, first),
            jnp.where(seen, moved_second, second),
        )
        for kind in range(3):
            stage[kind, rows, :] = values[kind]
            copy = pltpu.make_async_copy(
                stage.at[kind, rows, :], outs[kind].at[rows, :], leaving.at[kind, place]
            )
            copy.start()
            copies.append(copy)
    for copy in copies:
        copy.wait()


SMEM = pl.BlockSpec(memory_space=pltpu.SMEM)
VMEM = pl.BlockSpec(memory_space=pltpu.VMEM)


def f32_shape(*shape):
    return jax.ShapeDtypeStruct(shape, F32)


def project_call(visible, cameras, params):
    return pl.pallas_call(
        project_kernel,
        out_shape=(f32_shape(512, 128), f32_shape(16, 8, 128)),
        in_specs=[VMEM, SMEM, VMEM],
        out_specs=(VMEM, VMEM),
        scratch_shapes=[pltpu.VMEM((192, 1024), BF16), pltpu.VMEM((64, 128), F32)],
        compiler_params=pltpu.CompilerParams(vmem_limit_bytes=12 * MIB),
        name="project",
    )(visible, cameras, params)


def spread_call(arrived):
    return pl.pallas_call(
        spread_kernel,
        out_shape=f32_shape(16, 72, 128),
        in_specs=[VMEM],
        out_specs=VMEM,
        compiler_params=pltpu.CompilerParams(vmem_limit_bytes=6 * MIB),
        name="spread",
    )(arrived)


def columns_call(after, visible):
    return pl.pallas_call(
        columns_kernel,
        out_shape=jax.ShapeDtypeStruct((1024, 1024), BF16),
        in_specs=[pl.BlockSpec(memory_space=pl.ANY), VMEM],
        out_specs=VMEM,
        compiler_params=pltpu.CompilerParams(vmem_limit_bytes=8 * MIB),
        name="columns",
    )(after, visible)


def prepare_call(after, lists):
    return pl.pallas_call(
        prepare_kernel,
        out_shape=(
            jax.ShapeDtypeStruct((256, 2048), BF16),
            jax.ShapeDtypeStruct((1, 2048), jnp.int32),
            jax.ShapeDtypeStruct((1, 2048), jnp.int32),
        ),
        in_specs=[pl.BlockSpec(memory_space=pl.ANY), VMEM],
        out_specs=(VMEM, VMEM, VMEM),
        compiler_params=pltpu.CompilerParams(vmem_limit_bytes=16 * MIB),
        name="prepare",
    )(after, lists)


def render_call(place, counts, onehot, lanes, groups, targets, everyone):
    return pl.pallas_call(
        render_kernel,
        out_shape=(f32_shape(3, 1, 512), f32_shape(16, 72, 128)),
        in_specs=[SMEM, SMEM, VMEM, VMEM, VMEM, VMEM, VMEM],
        out_specs=(VMEM, VMEM),
        scratch_shapes=[
            pltpu.VMEM((16, 2048), F32),
            pltpu.VMEM((2, 1024, 256), F32),
            pltpu.VMEM((2, 1024, 256), F32),
            pltpu.VMEM((2, 1024, 256), F32),
            pltpu.VMEM((576, 256), F32),
            pltpu.VMEM((3, MIXED * 36, 256), BF16),
        ],
        compiler_params=pltpu.CompilerParams(vmem_limit_bytes=24 * MIB),
        name="render",
    )(place, counts, onehot, lanes, groups, targets, everyone)


def merge_call(arrived):
    return pl.pallas_call(
        merge_kernel,
        out_shape=f32_shape(16, 8, 128),
        in_specs=[VMEM],
        out_specs=VMEM,
        compiler_params=pltpu.CompilerParams(vmem_limit_bytes=6 * MIB),
        name="merge",
    )(arrived)


def update_call(onehot, cameras, arrived, picked, params, first, second):
    shape = f32_shape(*params.shape)
    return pl.pallas_call(
        update_kernel,
        out_shape=(shape, shape, shape),
        in_specs=[VMEM, SMEM, VMEM, VMEM, VMEM, VMEM, VMEM],
        out_specs=(pl.BlockSpec(memory_space=pl.ANY),) * 3,
        scratch_shapes=[
            pltpu.VMEM((64, 128), F32),
            pltpu.VMEM((512, 128), F32),
            pltpu.VMEM((3, PARAMS, 1024), F32),
            pltpu.SemaphoreType.DMA((3, 4)),
        ],
        compiler_params=pltpu.CompilerParams(vmem_limit_bytes=16 * MIB),
        name="update",
    )(onehot, cameras, arrived, picked, params, first, second)


def kept(array):
    return pltpu.with_memory_space_constraint(array, pltpu.VMEM)


def exchanged(array, axis):
    return kept(lax.all_to_all(array, axis, 0, 0, tiled=True))


def shards(params, first, second, visible, cameras, tile_lists, tile_blocks, targets):
    picked, outgoing = project_call(
        *[pltpu.with_memory_space_constraint(array, pltpu.HBM) for array in (visible, cameras, params)]
    )
    block = spread_call(exchanged(outgoing, "view"))
    everyone = exchanged(block, "tile")
    onehot, lanes, groups = [kept(table) for table in prepare_call(block, tile_lists)]
    place = lax.axis_index("tile").astype(jnp.int32).reshape(1)
    image, sums = render_call(
        place,
        tile_blocks,
        onehot,
        lanes,
        groups,
        jnp.transpose(targets, (1, 0, 2)),
        everyone,
    )
    merged = merge_call(exchanged(sums, "tile"))
    returned = exchanged(merged, "view")
    columns = kept(columns_call(merged, visible))
    new_params, new_first, new_second = update_call(
        columns, cameras, returned, kept(picked), kept(params), kept(first), kept(second)
    )
    return (new_params, new_first, new_second, jnp.transpose(image, (1, 0, 2)))


def solution(mesh):
    in_specs = (
        P(None, ("view", "tile")),
        P(None, ("view", "tile")),
        P(None, ("view", "tile")),
        P(None, ("view", "tile")),
        P(),
        P("view", "tile", None),
        P("view", "tile"),
        P("view", None, "tile"),
    )
    out_specs = (
        P(None, ("view", "tile")),
        P(None, ("view", "tile")),
        P(None, ("view", "tile")),
        P("view", None, "tile"),
    )
    return jax.shard_map(shards, mesh=mesh, in_specs=in_specs, out_specs=out_specs, check_vma=False)
```

```python
import functools

import jax
import jax.numpy as jnp
from jax import lax
from jax.experimental import pallas as pl
from jax.experimental.pallas import tpu as pltpu
from jax.sharding import PartitionSpec as P

SIDE = 16
PIX = 256
BLOCK = 128
WIN_COLS = 8


harm_zero = 0.28209479177387814
harm_one = 0.4886025119029199
harm_two = (
    1.0925484305920792,
    -1.0925484305920792,
    0.31539156525252005,
    -1.0925484305920792,
    0.5462742152960396,
)
harm_three = (
    -0.5900435899266435,
    2.890611442640554,
    -0.4570457994644658,
    0.3731763325901154,
    -0.4570457994644658,
    1.445305721320277,
    -0.5900435899266435,
)
learn_rate = 0.05
beta_first = 0.9
beta_second = 0.999
adam_eps = 1e-08
blur_add = 0.3


def rotation(real_part, axis_one, axis_two, axis_three):
    inverse = lax.rsqrt(
        real_part * real_part + axis_one * axis_one + axis_two * axis_two + axis_three * axis_three
    )
    real_unit = real_part * inverse
    unit_one = axis_one * inverse
    unit_two = axis_two * inverse
    unit_three = axis_three * inverse
    return (
        (
            1.0 - 2.0 * (unit_two * unit_two + unit_three * unit_three),
            2.0 * (unit_one * unit_two - real_unit * unit_three),
            2.0 * (unit_one * unit_three + real_unit * unit_two),
        ),
        (
            2.0 * (unit_one * unit_two + real_unit * unit_three),
            1.0 - 2.0 * (unit_one * unit_one + unit_three * unit_three),
            2.0 * (unit_two * unit_three - real_unit * unit_one),
        ),
        (
            2.0 * (unit_one * unit_three - real_unit * unit_two),
            2.0 * (unit_two * unit_three + real_unit * unit_one),
            1.0 - 2.0 * (unit_one * unit_one + unit_two * unit_two),
        ),
    )


def harmonics(first_dir, second_dir, third_dir):
    sq_first = first_dir * first_dir
    sq_second = second_dir * second_dir
    sq_third = third_dir * third_dir
    return [
        harm_zero,
        -harm_one * second_dir,
        harm_one * third_dir,
        -harm_one * first_dir,
        harm_two[0] * first_dir * second_dir,
        harm_two[1] * second_dir * third_dir,
        harm_two[2] * (2.0 * sq_third - sq_first - sq_second),
        harm_two[3] * first_dir * third_dir,
        harm_two[4] * (sq_first - sq_second),
        harm_three[0] * second_dir * (3.0 * sq_first - sq_second),
        harm_three[1] * first_dir * second_dir * third_dir,
        harm_three[2] * second_dir * (4.0 * sq_third - sq_first - sq_second),
        harm_three[3] * third_dir * (2.0 * sq_third - 3.0 * sq_first - 3.0 * sq_second),
        harm_three[4] * first_dir * (4.0 * sq_third - sq_first - sq_second),
        harm_three[5] * third_dir * (sq_first - sq_second),
        harm_three[6] * first_dir * (sq_first - 3.0 * sq_second),
    ]


def project(raw, camera):
    camera_turn = rotation(camera[0], camera[1], camera[2], camera[3])
    shift_vec = (camera[4], camera[5], camera[6])
    focal_x = camera[7]
    focal_y = camera[8]
    position = (raw[0], raw[1], raw[2])
    viewed = [
        camera_turn[across][0] * position[0]
        + camera_turn[across][1] * position[1]
        + camera_turn[across][2] * position[2]
        + shift_vec[across]
        for across in range(3)
    ]
    inverse = 1.0 / viewed[2]
    mean_x = focal_x * viewed[0] * inverse + camera[9]
    mean_y = focal_y * viewed[1] * inverse + camera[10]
    gauss_turn = rotation(raw[6], raw[7], raw[8], raw[9])
    stretch = [jnp.exp(raw[3 + column]) for column in range(3)]
    jac_xx = focal_x * inverse
    jac_xz = -focal_x * viewed[0] * inverse * inverse
    jac_yy = focal_y * inverse
    jac_yz = -focal_y * viewed[1] * inverse * inverse
    leading_x = [
        jac_xx * camera_turn[0][column] + jac_xz * camera_turn[2][column] for column in range(3)
    ]
    leading_y = [
        jac_yy * camera_turn[1][column] + jac_yz * camera_turn[2][column] for column in range(3)
    ]
    axes_x = [
        (
            leading_x[0] * gauss_turn[0][column]
            + leading_x[1] * gauss_turn[1][column]
            + leading_x[2] * gauss_turn[2][column]
        )
        * stretch[column]
        for column in range(3)
    ]
    axes_y = [
        (
            leading_y[0] * gauss_turn[0][column]
            + leading_y[1] * gauss_turn[1][column]
            + leading_y[2] * gauss_turn[2][column]
        )
        * stretch[column]
        for column in range(3)
    ]
    cov_xx = axes_x[0] * axes_x[0] + axes_x[1] * axes_x[1] + axes_x[2] * axes_x[2] + blur_add
    cov_xy = axes_x[0] * axes_y[0] + axes_x[1] * axes_y[1] + axes_x[2] * axes_y[2]
    cov_yy = axes_y[0] * axes_y[0] + axes_y[1] * axes_y[1] + axes_y[2] * axes_y[2] + blur_add
    determ = cov_xx * cov_yy - cov_xy * cov_xy
    opacity = jax.nn.sigmoid(raw[10])
    camera_eye = [
        -(
            camera_turn[0][column] * shift_vec[0]
            + camera_turn[1][column] * shift_vec[1]
            + camera_turn[2][column] * shift_vec[2]
        )
        for column in range(3)
    ]
    offset = [position[column] - camera_eye[column] for column in range(3)]
    length = lax.rsqrt(offset[0] * offset[0] + offset[1] * offset[1] + offset[2] * offset[2])
    harmonic_terms = harmonics(offset[0] * length, offset[1] * length, offset[2] * length)
    colours = []
    for channel in range(3):
        total = 0.5 + jnp.zeros_like(opacity)
        for harmonic in range(16):
            total = total + raw[11 + 16 * channel + harmonic] * harmonic_terms[harmonic]
        colours.append(total)
    return [mean_x, mean_y, cov_yy / determ, -cov_xy / determ, cov_xx / determ, opacity] + colours


F32 = jnp.float32
BF16 = jnp.bfloat16
PARAMS = 59
ROWS = 64
LOG2E = 1.4426950408889634
MIB = 1 << 20
MIXED = 8


def iota(shape, dim):
    return lax.broadcasted_iota(jnp.int32, shape, dim)


def parts_of(value, count):
    parts = []
    for _ in range(count):
        part = value.astype(BF16)
        parts.append(part)
        value = value - part.astype(F32)
    return parts


def mm(left, right, dims):
    return lax.dot_general(left, right, (dims, ((), ())), preferred_element_type=F32)


def stacked(rows, width):
    sub = iota((8, width), 0)
    out = jnp.zeros((8, width), F32)
    for place, row in enumerate(rows):
        out = jnp.where(sub == place, jnp.broadcast_to(row, (8, width)), out)
    return out


def seen_columns(ids_ref, first, width):
    row = jnp.concatenate(
        [ids_ref[first + step : first + step + 1, :] for step in range(width // 64)], axis=1
    )
    return (iota((1024, width), 0) == row).astype(BF16)


def camera_arrays(cameras_ref):
    view = 2 * iota((8, 128), 0) + (iota((8, 128), 1) >= 64).astype(jnp.int32)
    masks = [view == index for index in range(16)]
    arrays = []
    for field in range(11):
        array = jnp.full((8, 128), cameras_ref[0, field], F32)
        for index in range(1, 16):
            array = jnp.where(masks[index], cameras_ref[index, field], array)
        arrays.append(array)
    return arrays


def raw_rows(picked_ref):
    return [picked_ref[pl.ds(row, 8, stride=ROWS), :] for row in range(PARAMS)]


def project_kernel(
    ids_ref, cameras_ref, params_ref, saved_ref, send_ref, split, swap, picked_ref, leaving
):
    for place, part in enumerate(parts_of(params_ref[...], 3)):
        split[place * ROWS : place * ROWS + PARAMS, :] = part
    for pair in range(4):
        onehot = seen_columns(ids_ref, pair * 4, 256)
        three = mm(split[...], onehot, ((1,), (0,)))
        picked = three[0:ROWS] + three[ROWS : 2 * ROWS] + three[2 * ROWS :]
        picked_ref[pair * 128 : pair * 128 + ROWS, :] = picked[:, :128]
        picked_ref[pair * 128 + ROWS : pair * 128 + 2 * ROWS, :] = picked[:, 128:]
    copy = pltpu.make_async_copy(picked_ref, saved_ref, leaving)
    copy.start()
    values = project(raw_rows(picked_ref), camera_arrays(cameras_ref))
    for place in range(8):
        swap[place * 8 : place * 8 + 8, :] = values[place]
    low = iota((8, 128), 1) < 64
    for pair in range(8):
        main = swap[pl.ds(pair, 8, stride=8), :]
        last = jnp.broadcast_to(values[8][pair : pair + 1, :], (8, 128))
        send_ref[2 * pair] = jnp.where(low, main, pltpu.roll(last, 64, 1))
        send_ref[2 * pair + 1] = jnp.where(low, pltpu.roll(main, 64, 1), last)
    copy.wait()


def unpack_pair(even, odd):
    low = iota((8, 128), 1) < 64
    main = jnp.where(low, even, pltpu.roll(odd, 64, 1))
    last = jnp.where(low, pltpu.roll(even, 64, 1), odd)
    return main, last[0:1, :]


def spread_kernel(arrived_ref, out_ref):
    for pair in range(8):
        main, last = unpack_pair(arrived_ref[2 * pair], arrived_ref[2 * pair + 1])
        for peer in range(16):
            out_ref[peer, pair * 8 : pair * 8 + 8, :] = main
            out_ref[peer, 64 + pair : 65 + pair, :] = last


def as_columns(row):
    return jnp.transpose(jnp.broadcast_to(row.astype(F32), (128, 128))).astype(jnp.int32)


def columns_kernel(after_ref, ids_ref, cameras_ref, picked_ref, columns_ref, spread_ref):
    for pair in range(8):
        row = jnp.concatenate(
            [ids_ref[2 * pair : 2 * pair + 1, :], ids_ref[2 * pair + 1 : 2 * pair + 2, :]], axis=1
        )
        column = as_columns(row)
        for start in range(0, 1024, 128):
            hot = (iota((128, 128), 1) + start == column).astype(BF16)
            columns_ref[pair * 128 : pair * 128 + 128, start : start + 128] = hot
    for place, array in enumerate(raw_rows(picked_ref) + camera_arrays(cameras_ref)):
        spread_ref[place] = array


def prepare_kernel(after_ref, lists_ref, onehot_ref, turned_ref, lanes_ref, groups_ref):
    turn = (iota((128, 1024), 0) == (iota((128, 1024), 1) >> 3)).astype(BF16)
    pick_block = iota((8, 1024), 0) == (iota((8, 1024), 1) & 7)
    for tile in range(2):
        blocks = [lists_ref[0, tile : tile + 1, start : start + 128] for start in range(0, 1024, 128)]
        low_part = stacked([(row & 127).astype(F32) for row in blocks], 128)
        high_part = stacked([(row >> 7).astype(F32) for row in blocks], 128)
        low_part = mm(low_part.astype(BF16), turn, ((1,), (0,)))
        high_part = mm(high_part.astype(BF16), turn, ((1,), (0,)))
        low_row = jnp.sum(jnp.where(pick_block, low_part, 0.0), axis=0, keepdims=True)
        high_row = jnp.sum(jnp.where(pick_block, high_part, 0.0), axis=0, keepdims=True)
        low_row = low_row.astype(jnp.int32)
        high_row = high_row.astype(jnp.int32)
        lane_index = ((high_row >> 3) & 1) * 128 + low_row
        span = slice(tile * 1024, tile * 1024 + 1024)
        onehot_ref[:, span] = (iota((256, 1024), 0) == lane_index).astype(BF16)
        for start in range(0, 1024, 128):
            column = as_columns(lane_index[:, start : start + 128])
            lanes = iota((128, 128), 1)
            rows = slice(tile * 1024 + start, tile * 1024 + start + 128)
            turned_ref[rows, 0:128] = (lanes == column).astype(BF16)
            turned_ref[rows, 128:256] = (lanes + 128 == column).astype(BF16)
        lanes_ref[:, span] = low_row
        groups_ref[:, span] = high_row


def render_kernel(
    place_ref,
    counts_ref,
    onehot,
    turned,
    lanes_of,
    chosen,
    targets_ref,
    everyone_ref,
    image_ref,
    out_ref,
    picked,
    alphas,
    weights,
    shades,
    summed,
    table,
):
    count = 2048
    for half in range(MIXED // 2):
        for side in range(2):
            lanes = slice(side * 128, side * 128 + 128)
            main = parts_of(everyone_ref[2 * half + side, 0:64, :], 3)
            last = parts_of(everyone_ref[2 * half + side, 64:72, :], 3)
            for part in range(3):
                table[part, half * 64 : half * 64 + 64, lanes] = main[part]
                start = MIXED * 32 + half * 8
                table[part, start : start + 8, lanes] = last[part]

    def gather_chunk(chunk, carry):
        lanes = pl.ds(chunk * 256, 256)
        hot = onehot[:, lanes]
        found = mm(table[0], hot, ((1,), (0,)))
        found = found + mm(table[1], hot, ((1,), (0,)))
        found = found + mm(table[2], hot, ((1,), (0,)))
        both = jnp.broadcast_to(chosen[:, lanes], (8, 256))
        pair = (both >> 4) * 8 + (both & 7)
        sub = iota((8, 256), 0)
        zero = jnp.zeros((8, 256), F32)
        main = [zero, zero]
        last = zero
        for half in range(MIXED // 2):
            for place in range(8):
                start = half * 64 + place * 8
                main[place % 2] = jnp.where(
                    pair == half * 8 + place, found[start : start + 8, :], main[place % 2]
                )
            start = MIXED * 32 + half * 8
            last = jnp.where(pair == half * 8 + sub, found[start : start + 8, :], last)
        main = main[0] + main[1]
        sub = iota((8, 128), 0)
        zero = jnp.zeros((8, 128), F32)
        for side in range(2):
            cut = slice(side * 128, side * 128 + 128)
            lanes = pl.ds(chunk * 256 + side * 128, 128)
            lane = jnp.broadcast_to(lanes_of[:, lanes], (8, 128))
            group = both[:, cut]
            chains = [main[:, cut], zero, zero, zero]
            ends = [last[:, cut], zero]
            for peer in range(MIXED, 16):
                for place in range(8):
                    value = jnp.take_along_axis(
                        everyone_ref[peer, place * 8 : place * 8 + 8, :], lane, axis=1
                    )
                    chain = place % 4
                    chains[chain] = jnp.where(group == peer * 8 + place, value, chains[chain])
                value = jnp.take_along_axis(everyone_ref[peer, 64:72, :], lane, axis=1)
                ends[peer % 2] = jnp.where(group == peer * 8 + sub, value, ends[peer % 2])
            picked[0:8, lanes] = (chains[0] + chains[1]) + (chains[2] + chains[3])
            picked[8:16, lanes] = jnp.broadcast_to(
                jnp.sum(ends[0] + ends[1], axis=0, keepdims=True), (8, 128)
            )
        return carry

    for chunk in range(8):
        gather_chunk(chunk, 0)

    pixel = iota((8, PIX), 1)
    pixel_x = (pixel & (SIDE - 1)).astype(F32) + (0.5 - SIDE / 2)
    pixel_y = (pixel >> 4).astype(F32) + (0.5 - SIDE / 2)
    sub = iota((8, PIX), 0)
    basis = jnp.where(sub == 0, 1.0, 0.0)
    for place, row in enumerate(
        [pixel_x, pixel_y, pixel_x * pixel_x, pixel_x * pixel_y, pixel_y * pixel_y]
    ):
        basis = jnp.where(sub == place + 1, row, basis)
    blank = jnp.zeros((8, PIX), F32)
    basis_three = jnp.concatenate([basis, basis, basis, blank], axis=0).astype(BF16)
    basis_once = jnp.concatenate([basis, blank], axis=0).astype(BF16)

    def rows_of(tile):
        span = slice(tile * 1024, tile * 1024 + 1024)
        held = picked[:, span]
        global_tile = place_ref[0] * 2 + tile
        centre_x = (global_tile % WIN_COLS * SIDE + SIDE // 2).astype(F32)
        centre_y = (global_tile // WIN_COLS * SIDE + SIDE // 2).astype(F32)
        rows = [held[place : place + 1, :] for place in range(9)]
        rows[0] = rows[0] - centre_x
        rows[1] = rows[1] - centre_y
        return rows

    block = iota((1, 1024), 1) & 7
    blank_row = jnp.zeros((8, 1024), F32)
    colour_rows = []
    for tile in range(2):
        mean_x, mean_y, con_a, con_b, con_c, opacity, *colour = rows_of(tile)
        live = block < counts_ref[0, tile]
        slope_x = con_a * mean_x + con_b * mean_y
        slope_y = con_b * mean_x + con_c * mean_y
        scale = -0.5 * LOG2E
        level = scale * (slope_x * mean_x + slope_y * mean_y) + jnp.log(opacity) * LOG2E
        terms = [
            jnp.where(live, level, -1000.0),
            jnp.where(live, (-2.0 * scale) * slope_x, 0.0),
            jnp.where(live, (-2.0 * scale) * slope_y, 0.0),
            jnp.where(live, scale * con_a, 0.0),
            jnp.where(live, (2.0 * scale) * con_b, 0.0),
            jnp.where(live, scale * con_c, 0.0),
        ]
        split = [part.astype(F32) for part in parts_of(stacked(terms, 1024), 3)]
        coefficients = jnp.concatenate(split + [blank_row], axis=0).astype(BF16)
        alphas[tile] = mm(coefficients, basis_three, ((0,), (0,)))
        colour_rows.append(stacked(colour, 1024))

    steps = 8

    def advance(outer, held):
        held = list(held)
        for inner in range(steps):
            start = pl.multiple_of((outer * steps + inner) * 8, 8)
            for tile in range(2):
                alpha = jnp.exp2(alphas[tile, pl.ds(start, 8), :])
                weight = alpha * held[tile]
                held[tile] = held[tile] * (1.0 - alpha)
                weights[tile, pl.ds(start, 8), :] = weight
        return tuple(held)

    ones = jnp.ones((8, PIX), F32)
    left = lax.fori_loop(0, 128 // steps, advance, (ones, ones))

    behind = []
    ahead = []
    blame = []
    sub_wide = iota((8, 1024), 0)
    block_wide = iota((8, 1024), 1) & 7
    for tile in range(2):
        colour = colour_rows[tile]
        separate = []
        for channel in range(3):
            row = jnp.broadcast_to(colour[channel : channel + 1, :], (8, 1024))
            separate.append(jnp.where(sub_wide == block_wide, row, 0.0))
        fine, rough = parts_of(jnp.concatenate(separate, axis=0), 2)
        both = jnp.concatenate([fine.astype(F32), rough.astype(F32)], axis=0).astype(BF16)
        first_part, second_part = parts_of(weights[tile], 2)
        sums = mm(both, first_part, ((1,), (0,))) + mm(both, second_part, ((1,), (0,)))
        passed = left[tile]
        total = passed
        for shift in (1, 2, 4):
            total = total * jnp.where(sub >= shift, pltpu.roll(total, shift, 0), 1.0)
        before = jnp.where(sub >= 1, pltpu.roll(total, 1, 0), 1.0)
        ahead.append(before)
        value = jnp.zeros((8, PIX), F32)
        slopes = []
        for channel in range(3):
            own = sums[channel * 8 : channel * 8 + 8, :]
            own = own + sums[24 + channel * 8 : 32 + channel * 8, :]
            image = jnp.sum(own * before, axis=0, keepdims=True)
            lanes = slice(tile * PIX, tile * PIX + PIX)
            image_ref[channel, :, lanes] = image
            slope = 2.0 * (image - targets_ref[channel, :, lanes])
            slopes.append(slope)
            value = value + slope * own
        factor = passed
        for shift in (1, 2, 4):
            inside = sub < 8 - shift
            value = value + factor * jnp.where(inside, pltpu.roll(value, 8 - shift, 0), 0.0)
            factor = factor * jnp.where(inside, pltpu.roll(factor, 8 - shift, 0), 1.0)
        behind.append(jnp.where(sub < 7, pltpu.roll(value, 7, 0), 0.0))
        slope_parts = [part.astype(F32) for part in parts_of(stacked(slopes, PIX), 3)]
        colour_parts = [part.astype(F32) for part in parts_of(colour, 3)]
        pairs = [(0, 0), (0, 1), (1, 0), (1, 1), (0, 2), (2, 0)]
        left_side = jnp.concatenate([colour_parts[a] for a, _ in pairs], axis=0).astype(BF16)
        right_side = jnp.concatenate([slope_parts[b] for _, b in pairs], axis=0).astype(BF16)
        shades[tile] = mm(left_side, right_side, ((0,), (0,)))
        blame.append(jnp.concatenate(slope_parts[:2], axis=0).astype(BF16))

    def retreat(outer, held):
        held = list(held)
        for inner in range(steps):
            start = pl.multiple_of((127 - (outer * steps + inner)) * 8, 8)
            for tile in range(2):
                alpha = jnp.exp2(alphas[tile, pl.ds(start, 8), :])
                weight = weights[tile, pl.ds(start, 8), :] * ahead[tile]
                shade = shades[tile, pl.ds(start, 8), :]
                shades[tile, pl.ds(start, 8), :] = weight * (shade - held[tile])
                held[tile] = held[tile] * (1.0 - alpha) + alpha * shade
                weights[tile, pl.ds(start, 8), :] = weight
        return tuple(held)

    lax.fori_loop(0, 128 // steps, retreat, tuple(behind))

    for tile in range(2):
        moments = sum(
            mm(basis_once, part, ((1,), (1,))) for part in parts_of(shades[tile], 3)
        )
        tints = sum(mm(blame[tile], part, ((1,), (1,))) for part in parts_of(weights[tile], 2))
        tints = tints[0:8, :] + tints[8:16, :]
        mean_x, mean_y, con_a, con_b, con_c, opacity, *_ = rows_of(tile)
        sum_one, sum_x, sum_y, sum_xx, sum_xy, sum_yy = [
            moments[place : place + 1, :] for place in range(6)
        ]
        near_x = sum_x - mean_x * sum_one
        near_y = sum_y - mean_y * sum_one
        near_xx = sum_xx - mean_x * (sum_x + near_x)
        near_xy = sum_xy - mean_x * sum_y - mean_y * near_x
        near_yy = sum_yy - mean_y * (sum_y + near_y)
        grads = [
            con_a * near_x + con_b * near_y,
            con_b * near_x + con_c * near_y,
            -0.5 * near_xx,
            -near_xy,
            -0.5 * near_yy,
            sum_one / opacity,
            tints[0:1, :],
            tints[1:2, :],
        ]
        span = slice(tile * 1024, tile * 1024 + 1024)
        picked[0:8, span] = stacked(grads, 1024)
        picked[8:16, span] = jnp.broadcast_to(tints[2:3, :], (8, 1024))

    wide = 512
    for chunk in range(count // wide):
        lanes = slice(chunk * wide, chunk * wide + wide)
        group = chosen[:, lanes]
        group = jnp.broadcast_to((group >> 4) * 8 + (group & 7), (8, wide))
        sub = iota((8, wide), 0)
        main = [part.astype(F32) for part in parts_of(picked[0:8, lanes], 2)]
        last = [part.astype(F32) for part in parts_of(picked[8:16, lanes], 2)]
        sides = []
        for part in range(2):
            rows = [jnp.where(group == place, main[part], 0.0) for place in range(64)]
            rows += [jnp.where(group == half * 8 + sub, last[part], 0.0) for half in range(8)]
            sides += [
                jnp.concatenate(rows[place : place + 2], axis=0).astype(BF16)
                for place in range(0, 72, 2)
            ]
        total = mm(jnp.concatenate(sides, axis=0), turned[lanes, :], ((1,), (0,)))
        total = total[0:576] + total[576:]
        if chunk == 0:
            summed[...] = total
        elif chunk < count // wide - 1:
            summed[...] = summed[...] + total
        else:
            total = summed[...] + total
    for half in range(8):
        for side in range(2):
            lanes = slice(side * 128, side * 128 + 128)
            out_ref[2 * half + side, 0:64, :] = total[half * 64 : half * 64 + 64, lanes]
            out_ref[2 * half + side, 64:72, :] = total[512 + half * 8 : 520 + half * 8, lanes]


def merge_kernel(arrived_ref, send_ref):
    low = iota((8, 128), 1) < 64
    total = arrived_ref[0]
    for peer in range(1, 16):
        total = total + arrived_ref[peer]
    for pair in range(8):
        main = total[pair * 8 : pair * 8 + 8, :]
        last = jnp.broadcast_to(total[64 + pair : 65 + pair, :], (8, 128))
        send_ref[2 * pair] = jnp.where(low, main, pltpu.roll(last, 64, 1))
        send_ref[2 * pair + 1] = jnp.where(low, pltpu.roll(main, 64, 1), last)


def update_kernel(
    onehot_ref,
    spread_ref,
    arrived_ref,
    params_ref,
    first_ref,
    second_ref,
    new_params_ref,
    new_first_ref,
    new_second_ref,
    swap,
    turned,
    stage,
    leaving,
):
    lasts = []
    for pair in range(8):
        main, last = unpack_pair(arrived_ref[2 * pair], arrived_ref[2 * pair + 1])
        swap[pair * 8 : pair * 8 + 8, :] = main
        lasts.append(last)
    slopes = [swap[pl.ds(place, 8, stride=8), :] for place in range(8)]
    sub = iota((8, 128), 0)
    final = jnp.zeros((8, 128), F32)
    for pair in range(8):
        final = jnp.where(sub == pair, jnp.broadcast_to(lasts[pair], (8, 128)), final)
    slopes.append(final)
    arrays = [spread_ref[place] for place in range(PARAMS + 11)]
    cameras = arrays[PARAMS:]
    _, pullback = jax.vjp(lambda source: project(source, cameras), arrays[:PARAMS])
    (raw_grads,) = pullback(slopes)
    for row in range(PARAMS):
        turned[pl.ds(row, 8, stride=ROWS), :] = raw_grads[row]
    for row in range(PARAMS, ROWS):
        turned[pl.ds(row, 8, stride=ROWS), :] = jnp.ones((8, 128), F32)
    wide = jnp.concatenate([turned[pair * ROWS : pair * ROWS + ROWS, :] for pair in range(8)], axis=1)
    split = [part.astype(F32) for part in parts_of(wide, 3)]
    three = mm(jnp.concatenate(split, axis=0).astype(BF16), onehot_ref[...], ((1,), (0,)))
    summed = three[0:ROWS] + three[ROWS : 2 * ROWS] + three[2 * ROWS :]
    seen = summed[PARAMS : PARAMS + 1, :] > 0.5
    outs = (new_params_ref, new_first_ref, new_second_ref)
    copies = []
    for place, start in enumerate(range(0, PARAMS, 16)):
        rows = slice(start, min(start + 16, PARAMS))
        grad = summed[rows, :]
        first = first_ref[rows, :]
        second = second_ref[rows, :]
        params = params_ref[rows, :]
        moved_first = beta_first * first + (1.0 - beta_first) * grad
        moved_second = beta_second * second + (1.0 - beta_second) * grad * grad
        moved_params = params - learn_rate * moved_first / (jnp.sqrt(moved_second) + adam_eps)
        values = (
            jnp.where(seen, moved_params, params),
            jnp.where(seen, moved_first, first),
            jnp.where(seen, moved_second, second),
        )
        for kind in range(3):
            stage[kind, rows, :] = values[kind]
            copy = pltpu.make_async_copy(
                stage.at[kind, rows, :], outs[kind].at[rows, :], leaving.at[kind, place]
            )
            copy.start()
            copies.append(copy)
    for copy in copies:
        copy.wait()


SMEM = pl.BlockSpec(memory_space=pltpu.SMEM)
VMEM = pl.BlockSpec(memory_space=pltpu.VMEM)


def f32_shape(*shape):
    return jax.ShapeDtypeStruct(shape, F32)


def project_call(visible, cameras, params):
    return pl.pallas_call(
        project_kernel,
        out_shape=(pltpu.HBM((512, 128), F32), f32_shape(16, 8, 128)),
        in_specs=[VMEM, SMEM, VMEM],
        out_specs=(pl.BlockSpec(memory_space=pltpu.HBM), VMEM),
        scratch_shapes=[
            pltpu.VMEM((192, 1024), BF16),
            pltpu.VMEM((64, 128), F32),
            pltpu.VMEM((512, 128), F32),
            pltpu.SemaphoreType.DMA,
        ],
        compiler_params=pltpu.CompilerParams(vmem_limit_bytes=12 * MIB),
        name="project",
    )(visible, cameras, params)


def spread_call(arrived):
    return pl.pallas_call(
        spread_kernel,
        out_shape=f32_shape(16, 72, 128),
        in_specs=[VMEM],
        out_specs=VMEM,
        compiler_params=pltpu.CompilerParams(vmem_limit_bytes=6 * MIB),
        name="spread",
    )(arrived)


def columns_call(after, visible, cameras, picked):
    return pl.pallas_call(
        columns_kernel,
        out_shape=(jax.ShapeDtypeStruct((1024, 1024), BF16), f32_shape(PARAMS + 11, 8, 128)),
        in_specs=[pl.BlockSpec(memory_space=pl.ANY), VMEM, SMEM, VMEM],
        out_specs=(VMEM, VMEM),
        compiler_params=pltpu.CompilerParams(vmem_limit_bytes=8 * MIB),
        name="columns",
    )(after, visible, cameras, picked)


def prepare_call(after, lists):
    return pl.pallas_call(
        prepare_kernel,
        out_shape=(
            jax.ShapeDtypeStruct((256, 2048), BF16),
            jax.ShapeDtypeStruct((2048, 256), BF16),
            jax.ShapeDtypeStruct((1, 2048), jnp.int32),
            jax.ShapeDtypeStruct((1, 2048), jnp.int32),
        ),
        in_specs=[pl.BlockSpec(memory_space=pl.ANY), VMEM],
        out_specs=(VMEM, VMEM, VMEM, VMEM),
        compiler_params=pltpu.CompilerParams(vmem_limit_bytes=16 * MIB),
        name="prepare",
    )(after, lists)


def render_call(place, counts, onehot, turned, lanes, groups, targets, everyone):
    return pl.pallas_call(
        render_kernel,
        out_shape=(f32_shape(3, 1, 512), f32_shape(16, 72, 128)),
        in_specs=[SMEM, SMEM, VMEM, VMEM, VMEM, VMEM, VMEM, VMEM],
        out_specs=(VMEM, VMEM),
        scratch_shapes=[
            pltpu.VMEM((16, 2048), F32),
            pltpu.VMEM((2, 1024, 256), F32),
            pltpu.VMEM((2, 1024, 256), F32),
            pltpu.VMEM((2, 1024, 256), F32),
            pltpu.VMEM((576, 256), F32),
            pltpu.VMEM((3, MIXED * 36, 256), BF16),
        ],
        compiler_params=pltpu.CompilerParams(vmem_limit_bytes=24 * MIB),
        name="render",
    )(place, counts, onehot, turned, lanes, groups, targets, everyone)


def merge_call(arrived):
    return pl.pallas_call(
        merge_kernel,
        out_shape=f32_shape(16, 8, 128),
        in_specs=[VMEM],
        out_specs=VMEM,
        compiler_params=pltpu.CompilerParams(vmem_limit_bytes=6 * MIB),
        name="merge",
    )(arrived)


def update_call(onehot, spread, arrived, params, first, second):
    shape = f32_shape(*params.shape)
    return pl.pallas_call(
        update_kernel,
        out_shape=(shape, shape, shape),
        in_specs=[VMEM] * 6,
        out_specs=(pl.BlockSpec(memory_space=pl.ANY),) * 3,
        scratch_shapes=[
            pltpu.VMEM((64, 128), F32),
            pltpu.VMEM((512, 128), F32),
            pltpu.VMEM((3, PARAMS, 1024), F32),
            pltpu.SemaphoreType.DMA((3, 4)),
        ],
        compiler_params=pltpu.CompilerParams(vmem_limit_bytes=16 * MIB),
        name="update",
    )(onehot, spread, arrived, params, first, second)


def kept(array):
    return pltpu.with_memory_space_constraint(array, pltpu.VMEM)


def exchanged(array, axis):
    return kept(lax.all_to_all(array, axis, 0, 0, tiled=True))


def shards(params, first, second, visible, cameras, tile_lists, tile_blocks, targets):
    picked, outgoing = project_call(
        *[pltpu.with_memory_space_constraint(array, pltpu.HBM) for array in (visible, cameras, params)]
    )
    block = spread_call(exchanged(outgoing, "view"))
    everyone = exchanged(block, "tile")
    onehot, turned, lanes, groups = [kept(table) for table in prepare_call(block, tile_lists)]
    place = lax.axis_index("tile").astype(jnp.int32).reshape(1)
    image, sums = render_call(
        place,
        tile_blocks,
        onehot,
        turned,
        lanes,
        groups,
        jnp.transpose(targets, (1, 0, 2)),
        everyone,
    )
    merged = merge_call(exchanged(sums, "tile"))
    returned = exchanged(merged, "view")
    columns, rows = columns_call(merged, visible, cameras, picked)
    new_params, new_first, new_second = update_call(
        kept(columns), kept(rows), returned, kept(params), kept(first), kept(second)
    )
    return (new_params, new_first, new_second, jnp.transpose(image, (1, 0, 2)))


def solution(mesh):
    in_specs = (
        P(None, ("view", "tile")),
        P(None, ("view", "tile")),
        P(None, ("view", "tile")),
        P(None, ("view", "tile")),
        P(),
        P("view", "tile", None),
        P("view", "tile"),
        P("view", None, "tile"),
    )
    out_specs = (
        P(None, ("view", "tile")),
        P(None, ("view", "tile")),
        P(None, ("view", "tile")),
        P("view", None, "tile"),
    )
    return jax.shard_map(shards, mesh=mesh, in_specs=in_specs, out_specs=out_specs, check_vma=False)
```

```python
import functools

import jax
import jax.numpy as jnp
from jax import lax
from jax.experimental import pallas as pl
from jax.experimental.pallas import tpu as pltpu
from jax.sharding import PartitionSpec as P

SIDE = 16
PIX = 256
BLOCK = 128
WIN_COLS = 8


harm_zero = 0.28209479177387814
harm_one = 0.4886025119029199
harm_two = (
    1.0925484305920792,
    -1.0925484305920792,
    0.31539156525252005,
    -1.0925484305920792,
    0.5462742152960396,
)
harm_three = (
    -0.5900435899266435,
    2.890611442640554,
    -0.4570457994644658,
    0.3731763325901154,
    -0.4570457994644658,
    1.445305721320277,
    -0.5900435899266435,
)
learn_rate = 0.05
beta_first = 0.9
beta_second = 0.999
adam_eps = 1e-08
blur_add = 0.3


def rotation(real_part, axis_one, axis_two, axis_three):
    inverse = lax.rsqrt(
        real_part * real_part + axis_one * axis_one + axis_two * axis_two + axis_three * axis_three
    )
    real_unit = real_part * inverse
    unit_one = axis_one * inverse
    unit_two = axis_two * inverse
    unit_three = axis_three * inverse
    return (
        (
            1.0 - 2.0 * (unit_two * unit_two + unit_three * unit_three),
            2.0 * (unit_one * unit_two - real_unit * unit_three),
            2.0 * (unit_one * unit_three + real_unit * unit_two),
        ),
        (
            2.0 * (unit_one * unit_two + real_unit * unit_three),
            1.0 - 2.0 * (unit_one * unit_one + unit_three * unit_three),
            2.0 * (unit_two * unit_three - real_unit * unit_one),
        ),
        (
            2.0 * (unit_one * unit_three - real_unit * unit_two),
            2.0 * (unit_two * unit_three + real_unit * unit_one),
            1.0 - 2.0 * (unit_one * unit_one + unit_two * unit_two),
        ),
    )


def harmonics(first_dir, second_dir, third_dir):
    sq_first = first_dir * first_dir
    sq_second = second_dir * second_dir
    sq_third = third_dir * third_dir
    return [
        harm_zero,
        -harm_one * second_dir,
        harm_one * third_dir,
        -harm_one * first_dir,
        harm_two[0] * first_dir * second_dir,
        harm_two[1] * second_dir * third_dir,
        harm_two[2] * (2.0 * sq_third - sq_first - sq_second),
        harm_two[3] * first_dir * third_dir,
        harm_two[4] * (sq_first - sq_second),
        harm_three[0] * second_dir * (3.0 * sq_first - sq_second),
        harm_three[1] * first_dir * second_dir * third_dir,
        harm_three[2] * second_dir * (4.0 * sq_third - sq_first - sq_second),
        harm_three[3] * third_dir * (2.0 * sq_third - 3.0 * sq_first - 3.0 * sq_second),
        harm_three[4] * first_dir * (4.0 * sq_third - sq_first - sq_second),
        harm_three[5] * third_dir * (sq_first - sq_second),
        harm_three[6] * first_dir * (sq_first - 3.0 * sq_second),
    ]


def project(raw, camera):
    camera_turn = rotation(camera[0], camera[1], camera[2], camera[3])
    shift_vec = (camera[4], camera[5], camera[6])
    focal_x = camera[7]
    focal_y = camera[8]
    position = (raw[0], raw[1], raw[2])
    viewed = [
        camera_turn[across][0] * position[0]
        + camera_turn[across][1] * position[1]
        + camera_turn[across][2] * position[2]
        + shift_vec[across]
        for across in range(3)
    ]
    inverse = 1.0 / viewed[2]
    mean_x = focal_x * viewed[0] * inverse + camera[9]
    mean_y = focal_y * viewed[1] * inverse + camera[10]
    gauss_turn = rotation(raw[6], raw[7], raw[8], raw[9])
    stretch = [jnp.exp(raw[3 + column]) for column in range(3)]
    jac_xx = focal_x * inverse
    jac_xz = -focal_x * viewed[0] * inverse * inverse
    jac_yy = focal_y * inverse
    jac_yz = -focal_y * viewed[1] * inverse * inverse
    leading_x = [
        jac_xx * camera_turn[0][column] + jac_xz * camera_turn[2][column] for column in range(3)
    ]
    leading_y = [
        jac_yy * camera_turn[1][column] + jac_yz * camera_turn[2][column] for column in range(3)
    ]
    axes_x = [
        (
            leading_x[0] * gauss_turn[0][column]
            + leading_x[1] * gauss_turn[1][column]
            + leading_x[2] * gauss_turn[2][column]
        )
        * stretch[column]
        for column in range(3)
    ]
    axes_y = [
        (
            leading_y[0] * gauss_turn[0][column]
            + leading_y[1] * gauss_turn[1][column]
            + leading_y[2] * gauss_turn[2][column]
        )
        * stretch[column]
        for column in range(3)
    ]
    cov_xx = axes_x[0] * axes_x[0] + axes_x[1] * axes_x[1] + axes_x[2] * axes_x[2] + blur_add
    cov_xy = axes_x[0] * axes_y[0] + axes_x[1] * axes_y[1] + axes_x[2] * axes_y[2]
    cov_yy = axes_y[0] * axes_y[0] + axes_y[1] * axes_y[1] + axes_y[2] * axes_y[2] + blur_add
    determ = cov_xx * cov_yy - cov_xy * cov_xy
    opacity = jax.nn.sigmoid(raw[10])
    camera_eye = [
        -(
            camera_turn[0][column] * shift_vec[0]
            + camera_turn[1][column] * shift_vec[1]
            + camera_turn[2][column] * shift_vec[2]
        )
        for column in range(3)
    ]
    offset = [position[column] - camera_eye[column] for column in range(3)]
    length = lax.rsqrt(offset[0] * offset[0] + offset[1] * offset[1] + offset[2] * offset[2])
    harmonic_terms = harmonics(offset[0] * length, offset[1] * length, offset[2] * length)
    colours = []
    for channel in range(3):
        total = 0.5 + jnp.zeros_like(opacity)
        for harmonic in range(16):
            total = total + raw[11 + 16 * channel + harmonic] * harmonic_terms[harmonic]
        colours.append(total)
    return [mean_x, mean_y, cov_yy / determ, -cov_xy / determ, cov_xx / determ, opacity] + colours


F32 = jnp.float32
BF16 = jnp.bfloat16
PARAMS = 59
ROWS = 64
LOG2E = 1.4426950408889634
MIB = 1 << 20
MIXED = 8


def iota(shape, dim):
    return lax.broadcasted_iota(jnp.int32, shape, dim)


def parts_of(value, count):
    parts = []
    for _ in range(count):
        part = value.astype(BF16)
        parts.append(part)
        value = value - part.astype(F32)
    return parts


def mm(left, right, dims):
    return lax.dot_general(left, right, (dims, ((), ())), preferred_element_type=F32)


def stacked(rows, width):
    sub = iota((8, width), 0)
    out = jnp.zeros((8, width), F32)
    for place, row in enumerate(rows):
        out = jnp.where(sub == place, jnp.broadcast_to(row, (8, width)), out)
    return out


def seen_columns(ids_ref, first, width):
    row = jnp.concatenate(
        [ids_ref[first + step : first + step + 1, :] for step in range(width // 64)], axis=1
    )
    return (iota((1024, width), 0) == row).astype(BF16)


def camera_arrays(cameras_ref):
    view = 2 * iota((8, 128), 0) + (iota((8, 128), 1) >= 64).astype(jnp.int32)
    masks = [view == index for index in range(16)]
    arrays = []
    for field in range(11):
        array = jnp.full((8, 128), cameras_ref[0, field], F32)
        for index in range(1, 16):
            array = jnp.where(masks[index], cameras_ref[index, field], array)
        arrays.append(array)
    return arrays


def raw_rows(picked_ref):
    return [picked_ref[pl.ds(row, 8, stride=ROWS), :] for row in range(PARAMS)]


def pick_rows(ids_ref, params_ref, split, picked_ref):
    for place, part in enumerate(parts_of(params_ref[...], 3)):
        split[place * ROWS : place * ROWS + PARAMS, :] = part
    for pair in range(4):
        onehot = seen_columns(ids_ref, pair * 4, 256)
        three = mm(split[...], onehot, ((1,), (0,)))
        picked = three[0:ROWS] + three[ROWS : 2 * ROWS] + three[2 * ROWS :]
        picked_ref[pair * 128 : pair * 128 + ROWS, :] = picked[:, :128]
        picked_ref[pair * 128 + ROWS : pair * 128 + 2 * ROWS, :] = picked[:, 128:]


def project_kernel(ids_ref, cameras_ref, params_ref, send_ref, split, swap, picked_ref):
    pick_rows(ids_ref, params_ref, split, picked_ref)
    values = project(raw_rows(picked_ref), camera_arrays(cameras_ref))
    for place in range(8):
        swap[place * 8 : place * 8 + 8, :] = values[place]
    low = iota((8, 128), 1) < 64
    for pair in range(8):
        main = swap[pl.ds(pair, 8, stride=8), :]
        last = jnp.broadcast_to(values[8][pair : pair + 1, :], (8, 128))
        send_ref[2 * pair] = jnp.where(low, main, pltpu.roll(last, 64, 1))
        send_ref[2 * pair + 1] = jnp.where(low, pltpu.roll(main, 64, 1), last)


def unpack_pair(even, odd):
    low = iota((8, 128), 1) < 64
    main = jnp.where(low, even, pltpu.roll(odd, 64, 1))
    last = jnp.where(low, pltpu.roll(even, 64, 1), odd)
    return main, last[0:1, :]


def spread_kernel(arrived_ref, out_ref):
    for pair in range(8):
        main, last = unpack_pair(arrived_ref[2 * pair], arrived_ref[2 * pair + 1])
        for peer in range(16):
            out_ref[peer, pair * 8 : pair * 8 + 8, :] = main
            out_ref[peer, 64 + pair : 65 + pair, :] = last


def as_columns(row):
    return jnp.transpose(jnp.broadcast_to(row.astype(F32), (128, 128))).astype(jnp.int32)


def columns_kernel(after_ref, ids_ref, columns_ref):
    for pair in range(8):
        row = jnp.concatenate(
            [ids_ref[2 * pair : 2 * pair + 1, :], ids_ref[2 * pair + 1 : 2 * pair + 2, :]], axis=1
        )
        column = as_columns(row)
        for start in range(0, 1024, 128):
            hot = (iota((128, 128), 1) + start == column).astype(BF16)
            columns_ref[pair * 128 : pair * 128 + 128, start : start + 128] = hot


def prepare_kernel(
    after_ref,
    ids_ref,
    cameras_ref,
    params_ref,
    lists_ref,
    rows_ref,
    onehot_ref,
    turned_ref,
    lanes_ref,
    groups_ref,
    split,
    picked_ref,
):
    pick_rows(ids_ref, params_ref, split, picked_ref)
    for place, array in enumerate(raw_rows(picked_ref) + camera_arrays(cameras_ref)):
        rows_ref[place] = array

    turn = (iota((128, 1024), 0) == (iota((128, 1024), 1) >> 3)).astype(BF16)
    pick_block = iota((8, 1024), 0) == (iota((8, 1024), 1) & 7)
    for tile in range(2):
        blocks = [lists_ref[0, tile : tile + 1, start : start + 128] for start in range(0, 1024, 128)]
        low_part = stacked([(row & 127).astype(F32) for row in blocks], 128)
        high_part = stacked([(row >> 7).astype(F32) for row in blocks], 128)
        low_part = mm(low_part.astype(BF16), turn, ((1,), (0,)))
        high_part = mm(high_part.astype(BF16), turn, ((1,), (0,)))
        low_row = jnp.sum(jnp.where(pick_block, low_part, 0.0), axis=0, keepdims=True)
        high_row = jnp.sum(jnp.where(pick_block, high_part, 0.0), axis=0, keepdims=True)
        low_row = low_row.astype(jnp.int32)
        high_row = high_row.astype(jnp.int32)
        lane_index = ((high_row >> 3) & 1) * 128 + low_row
        span = slice(tile * 1024, tile * 1024 + 1024)
        onehot_ref[:, span] = (iota((256, 1024), 0) == lane_index).astype(BF16)
        for start in range(0, 1024, 128):
            column = as_columns(lane_index[:, start : start + 128])
            lanes = iota((128, 128), 1)
            rows = slice(tile * 1024 + start, tile * 1024 + start + 128)
            turned_ref[rows, 0:128] = (lanes == column).astype(BF16)
            turned_ref[rows, 128:256] = (lanes + 128 == column).astype(BF16)
        lanes_ref[:, span] = low_row
        groups_ref[:, span] = high_row


def render_kernel(
    place_ref,
    counts_ref,
    onehot,
    turned,
    lanes_of,
    chosen,
    targets_ref,
    everyone_ref,
    image_ref,
    out_ref,
    picked,
    alphas,
    weights,
    shades,
    summed,
    table,
):
    count = 2048
    for half in range(MIXED // 2):
        for side in range(2):
            lanes = slice(side * 128, side * 128 + 128)
            main = parts_of(everyone_ref[2 * half + side, 0:64, :], 3)
            last = parts_of(everyone_ref[2 * half + side, 64:72, :], 3)
            for part in range(3):
                table[part, half * 64 : half * 64 + 64, lanes] = main[part]
                start = MIXED * 32 + half * 8
                table[part, start : start + 8, lanes] = last[part]

    def gather_chunk(chunk, carry):
        lanes = pl.ds(chunk * 256, 256)
        hot = onehot[:, lanes]
        found = mm(table[0], hot, ((1,), (0,)))
        found = found + mm(table[1], hot, ((1,), (0,)))
        found = found + mm(table[2], hot, ((1,), (0,)))
        both = jnp.broadcast_to(chosen[:, lanes], (8, 256))
        pair = (both >> 4) * 8 + (both & 7)
        sub = iota((8, 256), 0)
        zero = jnp.zeros((8, 256), F32)
        main = [zero, zero]
        last = zero
        for half in range(MIXED // 2):
            for place in range(8):
                start = half * 64 + place * 8
                main[place % 2] = jnp.where(
                    pair == half * 8 + place, found[start : start + 8, :], main[place % 2]
                )
            start = MIXED * 32 + half * 8
            last = jnp.where(pair == half * 8 + sub, found[start : start + 8, :], last)
        main = main[0] + main[1]
        sub = iota((8, 128), 0)
        zero = jnp.zeros((8, 128), F32)
        for side in range(2):
            cut = slice(side * 128, side * 128 + 128)
            lanes = pl.ds(chunk * 256 + side * 128, 128)
            lane = jnp.broadcast_to(lanes_of[:, lanes], (8, 128))
            group = both[:, cut]
            chains = [main[:, cut], zero, zero, zero]
            ends = [last[:, cut], zero]
            for peer in range(MIXED, 16):
                for place in range(8):
                    value = jnp.take_along_axis(
                        everyone_ref[peer, place * 8 : place * 8 + 8, :], lane, axis=1
                    )
                    chain = place % 4
                    chains[chain] = jnp.where(group == peer * 8 + place, value, chains[chain])
                value = jnp.take_along_axis(everyone_ref[peer, 64:72, :], lane, axis=1)
                ends[peer % 2] = jnp.where(group == peer * 8 + sub, value, ends[peer % 2])
            picked[0:8, lanes] = (chains[0] + chains[1]) + (chains[2] + chains[3])
            picked[8:16, lanes] = jnp.broadcast_to(
                jnp.sum(ends[0] + ends[1], axis=0, keepdims=True), (8, 128)
            )
        return carry

    for chunk in range(8):
        gather_chunk(chunk, 0)

    pixel = iota((8, PIX), 1)
    pixel_x = (pixel & (SIDE - 1)).astype(F32) + (0.5 - SIDE / 2)
    pixel_y = (pixel >> 4).astype(F32) + (0.5 - SIDE / 2)
    sub = iota((8, PIX), 0)
    basis = jnp.where(sub == 0, 1.0, 0.0)
    for place, row in enumerate(
        [pixel_x, pixel_y, pixel_x * pixel_x, pixel_x * pixel_y, pixel_y * pixel_y]
    ):
        basis = jnp.where(sub == place + 1, row, basis)
    blank = jnp.zeros((8, PIX), F32)
    basis_three = jnp.concatenate([basis, basis, basis, blank], axis=0).astype(BF16)
    basis_once = jnp.concatenate([basis, blank], axis=0).astype(BF16)

    def rows_of(tile):
        span = slice(tile * 1024, tile * 1024 + 1024)
        held = picked[:, span]
        global_tile = place_ref[0] * 2 + tile
        centre_x = (global_tile % WIN_COLS * SIDE + SIDE // 2).astype(F32)
        centre_y = (global_tile // WIN_COLS * SIDE + SIDE // 2).astype(F32)
        rows = [held[place : place + 1, :] for place in range(9)]
        rows[0] = rows[0] - centre_x
        rows[1] = rows[1] - centre_y
        return rows

    block = iota((1, 1024), 1) & 7
    blank_row = jnp.zeros((8, 1024), F32)
    colour_rows = []
    for tile in range(2):
        mean_x, mean_y, con_a, con_b, con_c, opacity, *colour = rows_of(tile)
        live = block < counts_ref[0, tile]
        slope_x = con_a * mean_x + con_b * mean_y
        slope_y = con_b * mean_x + con_c * mean_y
        scale = -0.5 * LOG2E
        level = scale * (slope_x * mean_x + slope_y * mean_y) + jnp.log(opacity) * LOG2E
        terms = [
            jnp.where(live, level, -1000.0),
            jnp.where(live, (-2.0 * scale) * slope_x, 0.0),
            jnp.where(live, (-2.0 * scale) * slope_y, 0.0),
            jnp.where(live, scale * con_a, 0.0),
            jnp.where(live, (2.0 * scale) * con_b, 0.0),
            jnp.where(live, scale * con_c, 0.0),
        ]
        split = [part.astype(F32) for part in parts_of(stacked(terms, 1024), 3)]
        coefficients = jnp.concatenate(split + [blank_row], axis=0).astype(BF16)
        alphas[tile] = mm(coefficients, basis_three, ((0,), (0,)))
        colour_rows.append(stacked(colour, 1024))

    steps = 8

    def advance(outer, held):
        held = list(held)
        for inner in range(steps):
            start = pl.multiple_of((outer * steps + inner) * 8, 8)
            for tile in range(2):
                alpha = jnp.exp2(alphas[tile, pl.ds(start, 8), :])
                weight = alpha * held[tile]
                held[tile] = held[tile] * (1.0 - alpha)
                weights[tile, pl.ds(start, 8), :] = weight
        return tuple(held)

    ones = jnp.ones((8, PIX), F32)
    left = lax.fori_loop(0, 128 // steps, advance, (ones, ones))

    behind = []
    ahead = []
    blame = []
    sub_wide = iota((8, 1024), 0)
    block_wide = iota((8, 1024), 1) & 7
    for tile in range(2):
        colour = colour_rows[tile]
        separate = []
        for channel in range(3):
            row = jnp.broadcast_to(colour[channel : channel + 1, :], (8, 1024))
            separate.append(jnp.where(sub_wide == block_wide, row, 0.0))
        fine, rough = parts_of(jnp.concatenate(separate, axis=0), 2)
        both = jnp.concatenate([fine.astype(F32), rough.astype(F32)], axis=0).astype(BF16)
        first_part, second_part = parts_of(weights[tile], 2)
        sums = mm(both, first_part, ((1,), (0,))) + mm(both, second_part, ((1,), (0,)))
        passed = left[tile]
        total = passed
        for shift in (1, 2, 4):
            total = total * jnp.where(sub >= shift, pltpu.roll(total, shift, 0), 1.0)
        before = jnp.where(sub >= 1, pltpu.roll(total, 1, 0), 1.0)
        ahead.append(before)
        value = jnp.zeros((8, PIX), F32)
        slopes = []
        for channel in range(3):
            own = sums[channel * 8 : channel * 8 + 8, :]
            own = own + sums[24 + channel * 8 : 32 + channel * 8, :]
            image = jnp.sum(own * before, axis=0, keepdims=True)
            lanes = slice(tile * PIX, tile * PIX + PIX)
            image_ref[channel, :, lanes] = image
            slope = 2.0 * (image - targets_ref[channel, :, lanes])
            slopes.append(slope)
            value = value + slope * own
        factor = passed
        for shift in (1, 2, 4):
            inside = sub < 8 - shift
            value = value + factor * jnp.where(inside, pltpu.roll(value, 8 - shift, 0), 0.0)
            factor = factor * jnp.where(inside, pltpu.roll(factor, 8 - shift, 0), 1.0)
        behind.append(jnp.where(sub < 7, pltpu.roll(value, 7, 0), 0.0))
        slope_parts = [part.astype(F32) for part in parts_of(stacked(slopes, PIX), 3)]
        colour_parts = [part.astype(F32) for part in parts_of(colour, 3)]
        pairs = [(0, 0), (0, 1), (1, 0), (1, 1), (0, 2), (2, 0)]
        left_side = jnp.concatenate([colour_parts[a] for a, _ in pairs], axis=0).astype(BF16)
        right_side = jnp.concatenate([slope_parts[b] for _, b in pairs], axis=0).astype(BF16)
        shades[tile] = mm(left_side, right_side, ((0,), (0,)))
        blame.append(jnp.concatenate(slope_parts[:2], axis=0).astype(BF16))

    def retreat(outer, held):
        held = list(held)
        for inner in range(steps):
            start = pl.multiple_of((127 - (outer * steps + inner)) * 8, 8)
            for tile in range(2):
                alpha = jnp.exp2(alphas[tile, pl.ds(start, 8), :])
                weight = weights[tile, pl.ds(start, 8), :] * ahead[tile]
                shade = shades[tile, pl.ds(start, 8), :]
                shades[tile, pl.ds(start, 8), :] = weight * (shade - held[tile])
                held[tile] = held[tile] * (1.0 - alpha) + alpha * shade
                weights[tile, pl.ds(start, 8), :] = weight
        return tuple(held)

    lax.fori_loop(0, 128 // steps, retreat, tuple(behind))

    for tile in range(2):
        moments = sum(
            mm(basis_once, part, ((1,), (1,))) for part in parts_of(shades[tile], 2)
        )
        tints = sum(mm(blame[tile], part, ((1,), (1,))) for part in parts_of(weights[tile], 2))
        tints = tints[0:8, :] + tints[8:16, :]
        mean_x, mean_y, con_a, con_b, con_c, opacity, *_ = rows_of(tile)
        sum_one, sum_x, sum_y, sum_xx, sum_xy, sum_yy = [
            moments[place : place + 1, :] for place in range(6)
        ]
        near_x = sum_x - mean_x * sum_one
        near_y = sum_y - mean_y * sum_one
        near_xx = sum_xx - mean_x * (sum_x + near_x)
        near_xy = sum_xy - mean_x * sum_y - mean_y * near_x
        near_yy = sum_yy - mean_y * (sum_y + near_y)
        grads = [
            con_a * near_x + con_b * near_y,
            con_b * near_x + con_c * near_y,
            -0.5 * near_xx,
            -near_xy,
            -0.5 * near_yy,
            sum_one / opacity,
            tints[0:1, :],
            tints[1:2, :],
        ]
        span = slice(tile * 1024, tile * 1024 + 1024)
        picked[0:8, span] = stacked(grads, 1024)
        picked[8:16, span] = jnp.broadcast_to(tints[2:3, :], (8, 1024))

    wide = 512
    for chunk in range(count // wide):
        lanes = slice(chunk * wide, chunk * wide + wide)
        group = chosen[:, lanes]
        group = jnp.broadcast_to((group >> 4) * 8 + (group & 7), (8, wide))
        sub = iota((8, wide), 0)
        main = [part.astype(F32) for part in parts_of(picked[0:8, lanes], 2)]
        last = [part.astype(F32) for part in parts_of(picked[8:16, lanes], 2)]
        sides = []
        for part in range(2):
            rows = [jnp.where(group == place, main[part], 0.0) for place in range(64)]
            rows += [jnp.where(group == half * 8 + sub, last[part], 0.0) for half in range(8)]
            sides += [
                jnp.concatenate(rows[place : place + 2], axis=0).astype(BF16)
                for place in range(0, 72, 2)
            ]
        total = mm(jnp.concatenate(sides, axis=0), turned[lanes, :], ((1,), (0,)))
        total = total[0:576] + total[576:]
        if chunk == 0:
            summed[...] = total
        elif chunk < count // wide - 1:
            summed[...] = summed[...] + total
        else:
            total = summed[...] + total
    for half in range(8):
        for side in range(2):
            lanes = slice(side * 128, side * 128 + 128)
            out_ref[2 * half + side, 0:64, :] = total[half * 64 : half * 64 + 64, lanes]
            out_ref[2 * half + side, 64:72, :] = total[512 + half * 8 : 520 + half * 8, lanes]


def merge_kernel(arrived_ref, send_ref):
    low = iota((8, 128), 1) < 64
    total = arrived_ref[0]
    for peer in range(1, 16):
        total = total + arrived_ref[peer]
    for pair in range(8):
        main = total[pair * 8 : pair * 8 + 8, :]
        last = jnp.broadcast_to(total[64 + pair : 65 + pair, :], (8, 128))
        send_ref[2 * pair] = jnp.where(low, main, pltpu.roll(last, 64, 1))
        send_ref[2 * pair + 1] = jnp.where(low, pltpu.roll(main, 64, 1), last)


def update_kernel(
    onehot_ref,
    spread_ref,
    arrived_ref,
    params_ref,
    first_ref,
    second_ref,
    new_params_ref,
    new_first_ref,
    new_second_ref,
    swap,
    turned,
    stage,
    leaving,
):
    lasts = []
    for pair in range(8):
        main, last = unpack_pair(arrived_ref[2 * pair], arrived_ref[2 * pair + 1])
        swap[pair * 8 : pair * 8 + 8, :] = main
        lasts.append(last)
    slopes = [swap[pl.ds(place, 8, stride=8), :] for place in range(8)]
    sub = iota((8, 128), 0)
    final = jnp.zeros((8, 128), F32)
    for pair in range(8):
        final = jnp.where(sub == pair, jnp.broadcast_to(lasts[pair], (8, 128)), final)
    slopes.append(final)
    arrays = [spread_ref[place] for place in range(PARAMS + 11)]
    cameras = arrays[PARAMS:]
    _, pullback = jax.vjp(lambda source: project(source, cameras), arrays[:PARAMS])
    (raw_grads,) = pullback(slopes)
    for row in range(PARAMS):
        turned[pl.ds(row, 8, stride=ROWS), :] = raw_grads[row]
    for row in range(PARAMS, ROWS):
        turned[pl.ds(row, 8, stride=ROWS), :] = jnp.ones((8, 128), F32)
    wide = jnp.concatenate([turned[pair * ROWS : pair * ROWS + ROWS, :] for pair in range(8)], axis=1)
    split = [part.astype(F32) for part in parts_of(wide, 3)]
    three = mm(jnp.concatenate(split, axis=0).astype(BF16), onehot_ref[...], ((1,), (0,)))
    summed = three[0:ROWS] + three[ROWS : 2 * ROWS] + three[2 * ROWS :]
    seen = summed[PARAMS : PARAMS + 1, :] > 0.5
    outs = (new_params_ref, new_first_ref, new_second_ref)
    copies = []
    for place, start in enumerate(range(0, PARAMS, 16)):
        rows = slice(start, min(start + 16, PARAMS))
        grad = summed[rows, :]
        first = first_ref[rows, :]
        second = second_ref[rows, :]
        params = params_ref[rows, :]
        moved_first = beta_first * first + (1.0 - beta_first) * grad
        moved_second = beta_second * second + (1.0 - beta_second) * grad * grad
        moved_params = params - learn_rate * moved_first / (jnp.sqrt(moved_second) + adam_eps)
        values = (
            jnp.where(seen, moved_params, params),
            jnp.where(seen, moved_first, first),
            jnp.where(seen, moved_second, second),
        )
        for kind in range(3):
            stage[kind, rows, :] = values[kind]
            copy = pltpu.make_async_copy(
                stage.at[kind, rows, :], outs[kind].at[rows, :], leaving.at[kind, place]
            )
            copy.start()
            copies.append(copy)
    for copy in copies:
        copy.wait()


SMEM = pl.BlockSpec(memory_space=pltpu.SMEM)
VMEM = pl.BlockSpec(memory_space=pltpu.VMEM)


def f32_shape(*shape):
    return jax.ShapeDtypeStruct(shape, F32)


def project_call(visible, cameras, params):
    return pl.pallas_call(
        project_kernel,
        out_shape=f32_shape(16, 8, 128),
        in_specs=[VMEM, SMEM, VMEM],
        out_specs=VMEM,
        scratch_shapes=[
            pltpu.VMEM((192, 1024), BF16),
            pltpu.VMEM((64, 128), F32),
            pltpu.VMEM((512, 128), F32),
        ],
        compiler_params=pltpu.CompilerParams(vmem_limit_bytes=12 * MIB),
        name="project",
    )(visible, cameras, params)


def spread_call(arrived):
    return pl.pallas_call(
        spread_kernel,
        out_shape=f32_shape(16, 72, 128),
        in_specs=[VMEM],
        out_specs=VMEM,
        compiler_params=pltpu.CompilerParams(vmem_limit_bytes=6 * MIB),
        name="spread",
    )(arrived)


def columns_call(after, visible):
    return pl.pallas_call(
        columns_kernel,
        out_shape=jax.ShapeDtypeStruct((1024, 1024), BF16),
        in_specs=[pl.BlockSpec(memory_space=pl.ANY), VMEM],
        out_specs=VMEM,
        compiler_params=pltpu.CompilerParams(vmem_limit_bytes=8 * MIB),
        name="columns",
    )(after, visible)


def prepare_call(after, visible, cameras, params, lists):
    return pl.pallas_call(
        prepare_kernel,
        out_shape=(
            f32_shape(PARAMS + 11, 8, 128),
            jax.ShapeDtypeStruct((256, 2048), BF16),
            jax.ShapeDtypeStruct((2048, 256), BF16),
            jax.ShapeDtypeStruct((1, 2048), jnp.int32),
            jax.ShapeDtypeStruct((1, 2048), jnp.int32),
        ),
        in_specs=[pl.BlockSpec(memory_space=pl.ANY), VMEM, SMEM, VMEM, VMEM],
        out_specs=(VMEM, VMEM, VMEM, VMEM, VMEM),
        scratch_shapes=[pltpu.VMEM((192, 1024), BF16), pltpu.VMEM((512, 128), F32)],
        compiler_params=pltpu.CompilerParams(vmem_limit_bytes=16 * MIB),
        name="prepare",
    )(after, visible, cameras, params, lists)


def render_call(place, counts, onehot, turned, lanes, groups, targets, everyone):
    return pl.pallas_call(
        render_kernel,
        out_shape=(f32_shape(3, 1, 512), f32_shape(16, 72, 128)),
        in_specs=[SMEM, SMEM, VMEM, VMEM, VMEM, VMEM, VMEM, VMEM],
        out_specs=(VMEM, VMEM),
        scratch_shapes=[
            pltpu.VMEM((16, 2048), F32),
            pltpu.VMEM((2, 1024, 256), F32),
            pltpu.VMEM((2, 1024, 256), F32),
            pltpu.VMEM((2, 1024, 256), F32),
            pltpu.VMEM((576, 256), F32),
            pltpu.VMEM((3, MIXED * 36, 256), BF16),
        ],
        compiler_params=pltpu.CompilerParams(vmem_limit_bytes=24 * MIB),
        name="render",
    )(place, counts, onehot, turned, lanes, groups, targets, everyone)


def merge_call(arrived):
    return pl.pallas_call(
        merge_kernel,
        out_shape=f32_shape(16, 8, 128),
        in_specs=[VMEM],
        out_specs=VMEM,
        compiler_params=pltpu.CompilerParams(vmem_limit_bytes=6 * MIB),
        name="merge",
    )(arrived)


def update_call(onehot, spread, arrived, params, first, second):
    shape = f32_shape(*params.shape)
    return pl.pallas_call(
        update_kernel,
        out_shape=(shape, shape, shape),
        in_specs=[VMEM] * 6,
        out_specs=(pl.BlockSpec(memory_space=pl.ANY),) * 3,
        scratch_shapes=[
            pltpu.VMEM((64, 128), F32),
            pltpu.VMEM((512, 128), F32),
            pltpu.VMEM((3, PARAMS, 1024), F32),
            pltpu.SemaphoreType.DMA((3, 4)),
        ],
        compiler_params=pltpu.CompilerParams(vmem_limit_bytes=16 * MIB),
        name="update",
    )(onehot, spread, arrived, params, first, second)


def kept(array):
    return pltpu.with_memory_space_constraint(array, pltpu.VMEM)


def exchanged(array, axis):
    return kept(lax.all_to_all(array, axis, 0, 0, tiled=True))


def shards(params, first, second, visible, cameras, tile_lists, tile_blocks, targets):
    outgoing = project_call(
        *[pltpu.with_memory_space_constraint(array, pltpu.HBM) for array in (visible, cameras, params)]
    )
    block = spread_call(exchanged(outgoing, "view"))
    everyone = exchanged(block, "tile")
    rows, onehot, turned, lanes, groups = [
        kept(table) for table in prepare_call(block, visible, cameras, params, tile_lists)
    ]
    place = lax.axis_index("tile").astype(jnp.int32).reshape(1)
    image, sums = render_call(
        place,
        tile_blocks,
        onehot,
        turned,
        lanes,
        groups,
        jnp.transpose(targets, (1, 0, 2)),
        everyone,
    )
    merged = merge_call(exchanged(sums, "tile"))
    returned = exchanged(merged, "view")
    columns = columns_call(merged, visible)
    new_params, new_first, new_second = update_call(
        kept(columns), rows, returned, kept(params), kept(first), kept(second)
    )
    return (new_params, new_first, new_second, jnp.transpose(image, (1, 0, 2)))


def solution(mesh):
    in_specs = (
        P(None, ("view", "tile")),
        P(None, ("view", "tile")),
        P(None, ("view", "tile")),
        P(None, ("view", "tile")),
        P(),
        P("view", "tile", None),
        P("view", "tile"),
        P("view", None, "tile"),
    )
    out_specs = (
        P(None, ("view", "tile")),
        P(None, ("view", "tile")),
        P(None, ("view", "tile")),
        P("view", None, "tile"),
    )
    return jax.shard_map(shards, mesh=mesh, in_specs=in_specs, out_specs=out_specs, check_vma=False)
```

```python
import functools

import jax
import jax.numpy as jnp
from jax import lax
from jax.experimental import pallas as pl
from jax.experimental.pallas import tpu as pltpu
from jax.sharding import PartitionSpec as P

SIDE = 16
PIX = 256
BLOCK = 128
WIN_COLS = 8


harm_zero = 0.28209479177387814
harm_one = 0.4886025119029199
harm_two = (
    1.0925484305920792,
    -1.0925484305920792,
    0.31539156525252005,
    -1.0925484305920792,
    0.5462742152960396,
)
harm_three = (
    -0.5900435899266435,
    2.890611442640554,
    -0.4570457994644658,
    0.3731763325901154,
    -0.4570457994644658,
    1.445305721320277,
    -0.5900435899266435,
)
learn_rate = 0.05
beta_first = 0.9
beta_second = 0.999
adam_eps = 1e-08
blur_add = 0.3


def rotation(real_part, axis_one, axis_two, axis_three):
    inverse = lax.rsqrt(
        real_part * real_part + axis_one * axis_one + axis_two * axis_two + axis_three * axis_three
    )
    real_unit = real_part * inverse
    unit_one = axis_one * inverse
    unit_two = axis_two * inverse
    unit_three = axis_three * inverse
    return (
        (
            1.0 - 2.0 * (unit_two * unit_two + unit_three * unit_three),
            2.0 * (unit_one * unit_two - real_unit * unit_three),
            2.0 * (unit_one * unit_three + real_unit * unit_two),
        ),
        (
            2.0 * (unit_one * unit_two + real_unit * unit_three),
            1.0 - 2.0 * (unit_one * unit_one + unit_three * unit_three),
            2.0 * (unit_two * unit_three - real_unit * unit_one),
        ),
        (
            2.0 * (unit_one * unit_three - real_unit * unit_two),
            2.0 * (unit_two * unit_three + real_unit * unit_one),
            1.0 - 2.0 * (unit_one * unit_one + unit_two * unit_two),
        ),
    )


def harmonics(first_dir, second_dir, third_dir):
    sq_first = first_dir * first_dir
    sq_second = second_dir * second_dir
    sq_third = third_dir * third_dir
    return [
        harm_zero,
        -harm_one * second_dir,
        harm_one * third_dir,
        -harm_one * first_dir,
        harm_two[0] * first_dir * second_dir,
        harm_two[1] * second_dir * third_dir,
        harm_two[2] * (2.0 * sq_third - sq_first - sq_second),
        harm_two[3] * first_dir * third_dir,
        harm_two[4] * (sq_first - sq_second),
        harm_three[0] * second_dir * (3.0 * sq_first - sq_second),
        harm_three[1] * first_dir * second_dir * third_dir,
        harm_three[2] * second_dir * (4.0 * sq_third - sq_first - sq_second),
        harm_three[3] * third_dir * (2.0 * sq_third - 3.0 * sq_first - 3.0 * sq_second),
        harm_three[4] * first_dir * (4.0 * sq_third - sq_first - sq_second),
        harm_three[5] * third_dir * (sq_first - sq_second),
        harm_three[6] * first_dir * (sq_first - 3.0 * sq_second),
    ]


def project(raw, camera):
    camera_turn = rotation(camera[0], camera[1], camera[2], camera[3])
    shift_vec = (camera[4], camera[5], camera[6])
    focal_x = camera[7]
    focal_y = camera[8]
    position = (raw[0], raw[1], raw[2])
    viewed = [
        camera_turn[across][0] * position[0]
        + camera_turn[across][1] * position[1]
        + camera_turn[across][2] * position[2]
        + shift_vec[across]
        for across in range(3)
    ]
    inverse = 1.0 / viewed[2]
    mean_x = focal_x * viewed[0] * inverse + camera[9]
    mean_y = focal_y * viewed[1] * inverse + camera[10]
    gauss_turn = rotation(raw[6], raw[7], raw[8], raw[9])
    stretch = [jnp.exp(raw[3 + column]) for column in range(3)]
    jac_xx = focal_x * inverse
    jac_xz = -focal_x * viewed[0] * inverse * inverse
    jac_yy = focal_y * inverse
    jac_yz = -focal_y * viewed[1] * inverse * inverse
    leading_x = [
        jac_xx * camera_turn[0][column] + jac_xz * camera_turn[2][column] for column in range(3)
    ]
    leading_y = [
        jac_yy * camera_turn[1][column] + jac_yz * camera_turn[2][column] for column in range(3)
    ]
    axes_x = [
        (
            leading_x[0] * gauss_turn[0][column]
            + leading_x[1] * gauss_turn[1][column]
            + leading_x[2] * gauss_turn[2][column]
        )
        * stretch[column]
        for column in range(3)
    ]
    axes_y = [
        (
            leading_y[0] * gauss_turn[0][column]
            + leading_y[1] * gauss_turn[1][column]
            + leading_y[2] * gauss_turn[2][column]
        )
        * stretch[column]
        for column in range(3)
    ]
    cov_xx = axes_x[0] * axes_x[0] + axes_x[1] * axes_x[1] + axes_x[2] * axes_x[2] + blur_add
    cov_xy = axes_x[0] * axes_y[0] + axes_x[1] * axes_y[1] + axes_x[2] * axes_y[2]
    cov_yy = axes_y[0] * axes_y[0] + axes_y[1] * axes_y[1] + axes_y[2] * axes_y[2] + blur_add
    determ = cov_xx * cov_yy - cov_xy * cov_xy
    opacity = jax.nn.sigmoid(raw[10])
    camera_eye = [
        -(
            camera_turn[0][column] * shift_vec[0]
            + camera_turn[1][column] * shift_vec[1]
            + camera_turn[2][column] * shift_vec[2]
        )
        for column in range(3)
    ]
    offset = [position[column] - camera_eye[column] for column in range(3)]
    length = lax.rsqrt(offset[0] * offset[0] + offset[1] * offset[1] + offset[2] * offset[2])
    harmonic_terms = harmonics(offset[0] * length, offset[1] * length, offset[2] * length)
    colours = []
    for channel in range(3):
        total = 0.5 + jnp.zeros_like(opacity)
        for harmonic in range(16):
            total = total + raw[11 + 16 * channel + harmonic] * harmonic_terms[harmonic]
        colours.append(total)
    return [mean_x, mean_y, cov_yy / determ, -cov_xy / determ, cov_xx / determ, opacity] + colours


F32 = jnp.float32
BF16 = jnp.bfloat16
PARAMS = 59
ROWS = 64
LOG2E = 1.4426950408889634
MIB = 1 << 20
MIXED = 6


def iota(shape, dim):
    return lax.broadcasted_iota(jnp.int32, shape, dim)


def parts_of(value, count):
    parts = []
    for _ in range(count):
        part = value.astype(BF16)
        parts.append(part)
        value = value - part.astype(F32)
    return parts


def mm(left, right, dims):
    return lax.dot_general(left, right, (dims, ((), ())), preferred_element_type=F32)


def stacked(rows, width):
    sub = iota((8, width), 0)
    out = jnp.zeros((8, width), F32)
    for place, row in enumerate(rows):
        out = jnp.where(sub == place, jnp.broadcast_to(row, (8, width)), out)
    return out


def seen_columns(ids_ref, first, width):
    row = jnp.concatenate(
        [ids_ref[first + step : first + step + 1, :] for step in range(width // 64)], axis=1
    )
    return (iota((1024, width), 0) == row).astype(BF16)


def camera_arrays(cameras_ref):
    view = 2 * iota((8, 128), 0) + (iota((8, 128), 1) >= 64).astype(jnp.int32)
    masks = [view == index for index in range(16)]
    arrays = []
    for field in range(11):
        array = jnp.full((8, 128), cameras_ref[0, field], F32)
        for index in range(1, 16):
            array = jnp.where(masks[index], cameras_ref[index, field], array)
        arrays.append(array)
    return arrays


def raw_rows(picked_ref):
    return [picked_ref[pl.ds(row, 8, stride=ROWS), :] for row in range(PARAMS)]


def pick_rows(ids_ref, params_ref, split, picked_ref):
    for place, part in enumerate(parts_of(params_ref[...], 3)):
        split[place * ROWS : place * ROWS + PARAMS, :] = part
    for pair in range(4):
        onehot = seen_columns(ids_ref, pair * 4, 256)
        three = mm(split[...], onehot, ((1,), (0,)))
        picked = three[0:ROWS] + three[ROWS : 2 * ROWS] + three[2 * ROWS :]
        picked_ref[pair * 128 : pair * 128 + ROWS, :] = picked[:, :128]
        picked_ref[pair * 128 + ROWS : pair * 128 + 2 * ROWS, :] = picked[:, 128:]


def project_kernel(ids_ref, cameras_ref, params_ref, send_ref, split, swap, picked_ref):
    pick_rows(ids_ref, params_ref, split, picked_ref)
    values = project(raw_rows(picked_ref), camera_arrays(cameras_ref))
    for place in range(8):
        swap[place * 8 : place * 8 + 8, :] = values[place]
    low = iota((8, 128), 1) < 64
    for pair in range(8):
        main = swap[pl.ds(pair, 8, stride=8), :]
        last = jnp.broadcast_to(values[8][pair : pair + 1, :], (8, 128))
        send_ref[2 * pair] = jnp.where(low, main, pltpu.roll(last, 64, 1))
        send_ref[2 * pair + 1] = jnp.where(low, pltpu.roll(main, 64, 1), last)


def unpack_pair(even, odd):
    low = iota((8, 128), 1) < 64
    main = jnp.where(low, even, pltpu.roll(odd, 64, 1))
    last = jnp.where(low, pltpu.roll(even, 64, 1), odd)
    return main, last[0:1, :]


def spread_kernel(after_ref, place_ref, arrived_ref, out_ref):
    for pair in range(8):
        main, last = unpack_pair(arrived_ref[2 * pair], arrived_ref[2 * pair + 1])
        for peer in range(16):
            out_ref[peer, pair * 8 : pair * 8 + 8, :] = main
            out_ref[peer, 64 + pair : 65 + pair, :] = last


def as_columns(row):
    return jnp.transpose(jnp.broadcast_to(row.astype(F32), (128, 128))).astype(jnp.int32)


def columns_kernel(
    after_ref, ids_ref, cameras_ref, params_ref, columns_ref, rows_ref, split, picked_ref
):
    pick_rows(ids_ref, params_ref, split, picked_ref)
    for place, array in enumerate(raw_rows(picked_ref) + camera_arrays(cameras_ref)):
        rows_ref[place] = array
    for pair in range(8):
        row = jnp.concatenate(
            [ids_ref[2 * pair : 2 * pair + 1, :], ids_ref[2 * pair + 1 : 2 * pair + 2, :]], axis=1
        )
        column = as_columns(row)
        for start in range(0, 1024, 128):
            hot = (iota((128, 128), 1) + start == column).astype(BF16)
            columns_ref[pair * 128 : pair * 128 + 128, start : start + 128] = hot


def prepare_kernel(
    after_ref,
    lists_ref,
    onehot_ref,
    turned_ref,
    lanes_ref,
    groups_ref,
):

    turn = (iota((128, 1024), 0) == (iota((128, 1024), 1) >> 3)).astype(BF16)
    pick_block = iota((8, 1024), 0) == (iota((8, 1024), 1) & 7)
    for tile in range(2):
        blocks = [lists_ref[0, tile : tile + 1, start : start + 128] for start in range(0, 1024, 128)]
        low_part = stacked([(row & 127).astype(F32) for row in blocks], 128)
        high_part = stacked([(row >> 7).astype(F32) for row in blocks], 128)
        low_part = mm(low_part.astype(BF16), turn, ((1,), (0,)))
        high_part = mm(high_part.astype(BF16), turn, ((1,), (0,)))
        low_row = jnp.sum(jnp.where(pick_block, low_part, 0.0), axis=0, keepdims=True)
        high_row = jnp.sum(jnp.where(pick_block, high_part, 0.0), axis=0, keepdims=True)
        low_row = low_row.astype(jnp.int32)
        high_row = high_row.astype(jnp.int32)
        lane_index = ((high_row >> 3) & 1) * 128 + low_row
        span = slice(tile * 1024, tile * 1024 + 1024)
        onehot_ref[:, span] = (iota((256, 1024), 0) == lane_index).astype(BF16)
        for start in range(0, 1024, 128):
            column = as_columns(lane_index[:, start : start + 128])
            lanes = iota((128, 128), 1)
            rows = slice(tile * 1024 + start, tile * 1024 + start + 128)
            turned_ref[rows, 0:128] = (lanes == column).astype(BF16)
            turned_ref[rows, 128:256] = (lanes + 128 == column).astype(BF16)
        lanes_ref[:, span] = low_row
        groups_ref[:, span] = high_row


def render_kernel(
    place_ref,
    counts_ref,
    onehot,
    turned,
    lanes_of,
    chosen,
    targets_ref,
    everyone_ref,
    image_ref,
    out_ref,
    picked,
    alphas,
    weights,
    shades,
    summed,
    table,
):
    count = 2048
    for half in range(MIXED // 2):
        for side in range(2):
            lanes = slice(side * 128, side * 128 + 128)
            main = parts_of(everyone_ref[2 * half + side, 0:64, :], 3)
            last = parts_of(everyone_ref[2 * half + side, 64:72, :], 3)
            for part in range(3):
                table[part, half * 64 : half * 64 + 64, lanes] = main[part]
                start = MIXED * 32 + half * 8
                table[part, start : start + 8, lanes] = last[part]

    def gather_chunk(chunk, carry):
        lanes = pl.ds(chunk * 256, 256)
        hot = onehot[:, lanes]
        found = mm(table[0], hot, ((1,), (0,)))
        found = found + mm(table[1], hot, ((1,), (0,)))
        found = found + mm(table[2], hot, ((1,), (0,)))
        both = jnp.broadcast_to(chosen[:, lanes], (8, 256))
        pair = (both >> 4) * 8 + (both & 7)
        sub = iota((8, 256), 0)
        zero = jnp.zeros((8, 256), F32)
        main = [zero, zero]
        last = zero
        for half in range(MIXED // 2):
            for place in range(8):
                start = half * 64 + place * 8
                main[place % 2] = jnp.where(
                    pair == half * 8 + place, found[start : start + 8, :], main[place % 2]
                )
            start = MIXED * 32 + half * 8
            last = jnp.where(pair == half * 8 + sub, found[start : start + 8, :], last)
        main = main[0] + main[1]
        sub = iota((8, 128), 0)
        zero = jnp.zeros((8, 128), F32)
        for side in range(2):
            cut = slice(side * 128, side * 128 + 128)
            lanes = pl.ds(chunk * 256 + side * 128, 128)
            lane = jnp.broadcast_to(lanes_of[:, lanes], (8, 128))
            group = both[:, cut]
            chains = [main[:, cut], zero, zero, zero]
            ends = [last[:, cut], zero]
            for peer in range(MIXED, 16):
                for place in range(8):
                    value = jnp.take_along_axis(
                        everyone_ref[peer, place * 8 : place * 8 + 8, :], lane, axis=1
                    )
                    chain = place % 4
                    chains[chain] = jnp.where(group == peer * 8 + place, value, chains[chain])
                value = jnp.take_along_axis(everyone_ref[peer, 64:72, :], lane, axis=1)
                ends[peer % 2] = jnp.where(group == peer * 8 + sub, value, ends[peer % 2])
            picked[0:8, lanes] = (chains[0] + chains[1]) + (chains[2] + chains[3])
            picked[8:16, lanes] = jnp.broadcast_to(
                jnp.sum(ends[0] + ends[1], axis=0, keepdims=True), (8, 128)
            )
        return carry

    for chunk in range(8):
        gather_chunk(chunk, 0)

    pixel = iota((8, PIX), 1)
    pixel_x = (pixel & (SIDE - 1)).astype(F32) + (0.5 - SIDE / 2)
    pixel_y = (pixel >> 4).astype(F32) + (0.5 - SIDE / 2)
    sub = iota((8, PIX), 0)
    basis = jnp.where(sub == 0, 1.0, 0.0)
    for place, row in enumerate(
        [pixel_x, pixel_y, pixel_x * pixel_x, pixel_x * pixel_y, pixel_y * pixel_y]
    ):
        basis = jnp.where(sub == place + 1, row, basis)
    blank = jnp.zeros((8, PIX), F32)
    basis_three = jnp.concatenate([basis, basis, basis, blank], axis=0).astype(BF16)
    basis_once = jnp.concatenate([basis, blank], axis=0).astype(BF16)

    def rows_of(tile):
        span = slice(tile * 1024, tile * 1024 + 1024)
        held = picked[:, span]
        global_tile = place_ref[0] * 2 + tile
        centre_x = (global_tile % WIN_COLS * SIDE + SIDE // 2).astype(F32)
        centre_y = (global_tile // WIN_COLS * SIDE + SIDE // 2).astype(F32)
        rows = [held[place : place + 1, :] for place in range(9)]
        rows[0] = rows[0] - centre_x
        rows[1] = rows[1] - centre_y
        return rows

    block = iota((1, 1024), 1) & 7
    blank_row = jnp.zeros((8, 1024), F32)
    colour_rows = []
    for tile in range(2):
        mean_x, mean_y, con_a, con_b, con_c, opacity, *colour = rows_of(tile)
        live = block < counts_ref[0, tile]
        slope_x = con_a * mean_x + con_b * mean_y
        slope_y = con_b * mean_x + con_c * mean_y
        scale = -0.5 * LOG2E
        level = scale * (slope_x * mean_x + slope_y * mean_y) + jnp.log(opacity) * LOG2E
        terms = [
            jnp.where(live, level, -1000.0),
            jnp.where(live, (-2.0 * scale) * slope_x, 0.0),
            jnp.where(live, (-2.0 * scale) * slope_y, 0.0),
            jnp.where(live, scale * con_a, 0.0),
            jnp.where(live, (2.0 * scale) * con_b, 0.0),
            jnp.where(live, scale * con_c, 0.0),
        ]
        split = [part.astype(F32) for part in parts_of(stacked(terms, 1024), 3)]
        coefficients = jnp.concatenate(split + [blank_row], axis=0).astype(BF16)
        alphas[tile] = mm(coefficients, basis_three, ((0,), (0,)))
        colour_rows.append(stacked(colour, 1024))

    steps = 16

    def advance(outer, held):
        held = list(held)
        for inner in range(steps):
            start = pl.multiple_of((outer * steps + inner) * 8, 8)
            for tile in range(2):
                alpha = jnp.exp2(alphas[tile, pl.ds(start, 8), :])
                weight = alpha * held[tile]
                held[tile] = held[tile] * (1.0 - alpha)
                weights[tile, pl.ds(start, 8), :] = weight
        return tuple(held)

    ones = jnp.ones((8, PIX), F32)
    left = lax.fori_loop(0, 128 // steps, advance, (ones, ones))

    behind = []
    ahead = []
    blame = []
    sub_wide = iota((8, 1024), 0)
    block_wide = iota((8, 1024), 1) & 7
    for tile in range(2):
        colour = colour_rows[tile]
        separate = []
        for channel in range(3):
            row = jnp.broadcast_to(colour[channel : channel + 1, :], (8, 1024))
            separate.append(jnp.where(sub_wide == block_wide, row, 0.0))
        fine, rough = parts_of(jnp.concatenate(separate, axis=0), 2)
        both = jnp.concatenate([fine.astype(F32), rough.astype(F32)], axis=0).astype(BF16)
        first_part, second_part = parts_of(weights[tile], 2)
        sums = mm(both, first_part, ((1,), (0,))) + mm(both, second_part, ((1,), (0,)))
        passed = left[tile]
        total = passed
        for shift in (1, 2, 4):
            total = total * jnp.where(sub >= shift, pltpu.roll(total, shift, 0), 1.0)
        before = jnp.where(sub >= 1, pltpu.roll(total, 1, 0), 1.0)
        ahead.append(before)
        value = jnp.zeros((8, PIX), F32)
        slopes = []
        for channel in range(3):
            own = sums[channel * 8 : channel * 8 + 8, :]
            own = own + sums[24 + channel * 8 : 32 + channel * 8, :]
            image = jnp.sum(own * before, axis=0, keepdims=True)
            lanes = slice(tile * PIX, tile * PIX + PIX)
            image_ref[channel, :, lanes] = image
            slope = 2.0 * (image - targets_ref[channel, :, lanes])
            slopes.append(slope)
            value = value + slope * own
        factor = passed
        for shift in (1, 2, 4):
            inside = sub < 8 - shift
            value = value + factor * jnp.where(inside, pltpu.roll(value, 8 - shift, 0), 0.0)
            factor = factor * jnp.where(inside, pltpu.roll(factor, 8 - shift, 0), 1.0)
        behind.append(jnp.where(sub < 7, pltpu.roll(value, 7, 0), 0.0))
        slope_parts = [part.astype(F32) for part in parts_of(stacked(slopes, PIX), 3)]
        colour_parts = [part.astype(F32) for part in parts_of(colour, 3)]
        pairs = [(0, 0), (0, 1), (1, 0), (1, 1), (0, 2), (2, 0)]
        left_side = jnp.concatenate([colour_parts[a] for a, _ in pairs], axis=0).astype(BF16)
        right_side = jnp.concatenate([slope_parts[b] for _, b in pairs], axis=0).astype(BF16)
        shades[tile] = mm(left_side, right_side, ((0,), (0,)))
        blame.append(jnp.concatenate(slope_parts[:2], axis=0).astype(BF16))

    def retreat(outer, held):
        held = list(held)
        for inner in range(steps):
            start = pl.multiple_of((127 - (outer * steps + inner)) * 8, 8)
            for tile in range(2):
                alpha = jnp.exp2(alphas[tile, pl.ds(start, 8), :])
                weight = weights[tile, pl.ds(start, 8), :] * ahead[tile]
                shade = shades[tile, pl.ds(start, 8), :]
                shades[tile, pl.ds(start, 8), :] = weight * (shade - held[tile])
                held[tile] = held[tile] * (1.0 - alpha) + alpha * shade
                weights[tile, pl.ds(start, 8), :] = weight
        return tuple(held)

    lax.fori_loop(0, 128 // steps, retreat, tuple(behind))

    for tile in range(2):
        moments = sum(
            mm(basis_once, part, ((1,), (1,))) for part in parts_of(shades[tile], 2)
        )
        tints = sum(mm(blame[tile], part, ((1,), (1,))) for part in parts_of(weights[tile], 2))
        tints = tints[0:8, :] + tints[8:16, :]
        mean_x, mean_y, con_a, con_b, con_c, opacity, *_ = rows_of(tile)
        sum_one, sum_x, sum_y, sum_xx, sum_xy, sum_yy = [
            moments[place : place + 1, :] for place in range(6)
        ]
        near_x = sum_x - mean_x * sum_one
        near_y = sum_y - mean_y * sum_one
        near_xx = sum_xx - mean_x * (sum_x + near_x)
        near_xy = sum_xy - mean_x * sum_y - mean_y * near_x
        near_yy = sum_yy - mean_y * (sum_y + near_y)
        grads = [
            con_a * near_x + con_b * near_y,
            con_b * near_x + con_c * near_y,
            -0.5 * near_xx,
            -near_xy,
            -0.5 * near_yy,
            sum_one / opacity,
            tints[0:1, :],
            tints[1:2, :],
        ]
        span = slice(tile * 1024, tile * 1024 + 1024)
        picked[0:8, span] = stacked(grads, 1024)
        picked[8:16, span] = jnp.broadcast_to(tints[2:3, :], (8, 1024))

    wide = 512
    for chunk in range(count // wide):
        lanes = slice(chunk * wide, chunk * wide + wide)
        group = chosen[:, lanes]
        group = jnp.broadcast_to((group >> 4) * 8 + (group & 7), (8, wide))
        sub = iota((8, wide), 0)
        main = [part.astype(F32) for part in parts_of(picked[0:8, lanes], 2)]
        last = [part.astype(F32) for part in parts_of(picked[8:16, lanes], 2)]
        sides = []
        for part in range(2):
            rows = [jnp.where(group == place, main[part], 0.0) for place in range(64)]
            rows += [jnp.where(group == half * 8 + sub, last[part], 0.0) for half in range(8)]
            sides += [
                jnp.concatenate(rows[place : place + 2], axis=0).astype(BF16)
                for place in range(0, 72, 2)
            ]
        total = mm(jnp.concatenate(sides, axis=0), turned[lanes, :], ((1,), (0,)))
        total = total[0:576] + total[576:]
        if chunk == 0:
            summed[...] = total
        elif chunk < count // wide - 1:
            summed[...] = summed[...] + total
        else:
            total = summed[...] + total
    for half in range(8):
        for side in range(2):
            lanes = slice(side * 128, side * 128 + 128)
            out_ref[2 * half + side, 0:64, :] = total[half * 64 : half * 64 + 64, lanes]
            out_ref[2 * half + side, 64:72, :] = total[512 + half * 8 : 520 + half * 8, lanes]


def merge_kernel(arrived_ref, send_ref):
    low = iota((8, 128), 1) < 64
    total = arrived_ref[0]
    for peer in range(1, 16):
        total = total + arrived_ref[peer]
    for pair in range(8):
        main = total[pair * 8 : pair * 8 + 8, :]
        last = jnp.broadcast_to(total[64 + pair : 65 + pair, :], (8, 128))
        send_ref[2 * pair] = jnp.where(low, main, pltpu.roll(last, 64, 1))
        send_ref[2 * pair + 1] = jnp.where(low, pltpu.roll(main, 64, 1), last)


def update_kernel(
    onehot_ref,
    spread_ref,
    arrived_ref,
    params_ref,
    first_ref,
    second_ref,
    new_params_ref,
    new_first_ref,
    new_second_ref,
    swap,
    turned,
    stage,
    leaving,
):
    lasts = []
    for pair in range(8):
        main, last = unpack_pair(arrived_ref[2 * pair], arrived_ref[2 * pair + 1])
        swap[pair * 8 : pair * 8 + 8, :] = main
        lasts.append(last)
    slopes = [swap[pl.ds(place, 8, stride=8), :] for place in range(8)]
    sub = iota((8, 128), 0)
    final = jnp.zeros((8, 128), F32)
    for pair in range(8):
        final = jnp.where(sub == pair, jnp.broadcast_to(lasts[pair], (8, 128)), final)
    slopes.append(final)
    arrays = [spread_ref[place] for place in range(PARAMS + 11)]
    cameras = arrays[PARAMS:]
    _, pullback = jax.vjp(lambda source: project(source, cameras), arrays[:PARAMS])
    (raw_grads,) = pullback(slopes)
    for row in range(PARAMS):
        turned[pl.ds(row, 8, stride=ROWS), :] = raw_grads[row]
    for row in range(PARAMS, ROWS):
        turned[pl.ds(row, 8, stride=ROWS), :] = jnp.ones((8, 128), F32)
    wide = jnp.concatenate([turned[pair * ROWS : pair * ROWS + ROWS, :] for pair in range(8)], axis=1)
    split = [part.astype(F32) for part in parts_of(wide, 3)]
    three = mm(jnp.concatenate(split, axis=0).astype(BF16), onehot_ref[...], ((1,), (0,)))
    summed = three[0:ROWS] + three[ROWS : 2 * ROWS] + three[2 * ROWS :]
    seen = summed[PARAMS : PARAMS + 1, :] > 0.5
    outs = (new_params_ref, new_first_ref, new_second_ref)
    copies = []
    for place, start in enumerate(range(0, PARAMS, 16)):
        rows = slice(start, min(start + 16, PARAMS))
        grad = summed[rows, :]
        first = first_ref[rows, :]
        second = second_ref[rows, :]
        params = params_ref[rows, :]
        moved_first = beta_first * first + (1.0 - beta_first) * grad
        moved_second = beta_second * second + (1.0 - beta_second) * grad * grad
        moved_params = params - learn_rate * moved_first / (jnp.sqrt(moved_second) + adam_eps)
        values = (
            jnp.where(seen, moved_params, params),
            jnp.where(seen, moved_first, first),
            jnp.where(seen, moved_second, second),
        )
        for kind in range(3):
            stage[kind, rows, :] = values[kind]
            copy = pltpu.make_async_copy(
                stage.at[kind, rows, :], outs[kind].at[rows, :], leaving.at[kind, place]
            )
            copy.start()
            copies.append(copy)
    for copy in copies:
        copy.wait()


SMEM = pl.BlockSpec(memory_space=pltpu.SMEM)
VMEM = pl.BlockSpec(memory_space=pltpu.VMEM)


def f32_shape(*shape):
    return jax.ShapeDtypeStruct(shape, F32)


def project_call(visible, cameras, params):
    return pl.pallas_call(
        project_kernel,
        out_shape=f32_shape(16, 8, 128),
        in_specs=[VMEM, SMEM, VMEM],
        out_specs=VMEM,
        scratch_shapes=[
            pltpu.VMEM((192, 1024), BF16),
            pltpu.VMEM((64, 128), F32),
            pltpu.VMEM((512, 128), F32),
        ],
        compiler_params=pltpu.CompilerParams(vmem_limit_bytes=12 * MIB),
        name="project",
    )(visible, cameras, params)


def spread_call(after, place, arrived):
    return pl.pallas_call(
        spread_kernel,
        out_shape=f32_shape(16, 72, 128),
        in_specs=[pl.BlockSpec(memory_space=pl.ANY), SMEM, VMEM],
        out_specs=VMEM,
        compiler_params=pltpu.CompilerParams(vmem_limit_bytes=6 * MIB),
        name="spread",
    )(after, place, arrived)


def columns_call(after, visible, cameras, params):
    return pl.pallas_call(
        columns_kernel,
        out_shape=(jax.ShapeDtypeStruct((1024, 1024), BF16), f32_shape(PARAMS + 11, 8, 128)),
        in_specs=[pl.BlockSpec(memory_space=pl.ANY), VMEM, SMEM, VMEM],
        out_specs=(VMEM, VMEM),
        scratch_shapes=[pltpu.VMEM((192, 1024), BF16), pltpu.VMEM((512, 128), F32)],
        compiler_params=pltpu.CompilerParams(vmem_limit_bytes=12 * MIB),
        name="columns",
    )(after, visible, cameras, params)


def prepare_call(after, lists):
    return pl.pallas_call(
        prepare_kernel,
        out_shape=(
            jax.ShapeDtypeStruct((256, 2048), BF16),
            jax.ShapeDtypeStruct((2048, 256), BF16),
            jax.ShapeDtypeStruct((1, 2048), jnp.int32),
            jax.ShapeDtypeStruct((1, 2048), jnp.int32),
        ),
        in_specs=[pl.BlockSpec(memory_space=pl.ANY), VMEM],
        out_specs=(VMEM, VMEM, VMEM, VMEM),
        compiler_params=pltpu.CompilerParams(vmem_limit_bytes=16 * MIB),
        name="prepare",
    )(after, lists)


def render_call(place, counts, onehot, turned, lanes, groups, targets, everyone):
    return pl.pallas_call(
        render_kernel,
        out_shape=(f32_shape(3, 1, 512), f32_shape(16, 72, 128)),
        in_specs=[SMEM, SMEM, VMEM, VMEM, VMEM, VMEM, VMEM, VMEM],
        out_specs=(VMEM, VMEM),
        scratch_shapes=[
            pltpu.VMEM((16, 2048), F32),
            pltpu.VMEM((2, 1024, 256), F32),
            pltpu.VMEM((2, 1024, 256), F32),
            pltpu.VMEM((2, 1024, 256), F32),
            pltpu.VMEM((576, 256), F32),
            pltpu.VMEM((3, MIXED * 36, 256), BF16),
        ],
        compiler_params=pltpu.CompilerParams(vmem_limit_bytes=24 * MIB),
        name="render",
    )(place, counts, onehot, turned, lanes, groups, targets, everyone)


def merge_call(arrived):
    return pl.pallas_call(
        merge_kernel,
        out_shape=f32_shape(16, 8, 128),
        in_specs=[VMEM],
        out_specs=VMEM,
        compiler_params=pltpu.CompilerParams(vmem_limit_bytes=6 * MIB),
        name="merge",
    )(arrived)


def update_call(onehot, spread, arrived, params, first, second):
    shape = f32_shape(*params.shape)
    return pl.pallas_call(
        update_kernel,
        out_shape=(shape, shape, shape),
        in_specs=[VMEM] * 6,
        out_specs=(pl.BlockSpec(memory_space=pl.ANY),) * 3,
        scratch_shapes=[
            pltpu.VMEM((64, 128), F32),
            pltpu.VMEM((512, 128), F32),
            pltpu.VMEM((3, PARAMS, 1024), F32),
            pltpu.SemaphoreType.DMA((3, 4)),
        ],
        compiler_params=pltpu.CompilerParams(vmem_limit_bytes=16 * MIB),
        name="update",
    )(onehot, spread, arrived, params, first, second)


def kept(array):
    return pltpu.with_memory_space_constraint(array, pltpu.VMEM)


def exchanged(array, axis):
    return kept(lax.all_to_all(array, axis, 0, 0, tiled=True))


def shards(params, first, second, visible, cameras, tile_lists, tile_blocks, targets):
    held = [
        pltpu.with_memory_space_constraint(array, pltpu.HBM)
        for array in (visible, cameras, params, tile_lists)
    ]
    outgoing = project_call(*held[:3])
    onehot, turned, lanes, groups = [kept(table) for table in prepare_call(outgoing, held[3])]
    place = lax.axis_index("tile").astype(jnp.int32).reshape(1)
    everyone = exchanged(spread_call(groups, place, exchanged(outgoing, "view")), "tile")
    image, sums = render_call(
        place,
        tile_blocks,
        onehot,
        turned,
        lanes,
        groups,
        jnp.transpose(targets, (1, 0, 2)),
        everyone,
    )
    merged = merge_call(exchanged(sums, "tile"))
    returned = exchanged(merged, "view")
    columns, rows = columns_call(merged, visible, cameras, kept(params))
    new_params, new_first, new_second = update_call(
        kept(columns), kept(rows), returned, kept(params), kept(first), kept(second)
    )
    return (new_params, new_first, new_second, jnp.transpose(image, (1, 0, 2)))


def solution(mesh):
    in_specs = (
        P(None, ("view", "tile")),
        P(None, ("view", "tile")),
        P(None, ("view", "tile")),
        P(None, ("view", "tile")),
        P(),
        P("view", "tile", None),
        P("view", "tile"),
        P("view", None, "tile"),
    )
    out_specs = (
        P(None, ("view", "tile")),
        P(None, ("view", "tile")),
        P(None, ("view", "tile")),
        P("view", None, "tile"),
    )
    return jax.shard_map(shards, mesh=mesh, in_specs=in_specs, out_specs=out_specs, check_vma=False)
```

```python
import functools

import jax
import jax.numpy as jnp
from jax import lax
from jax.experimental import pallas as pl
from jax.experimental.pallas import tpu as pltpu
from jax.sharding import PartitionSpec as P

SIDE = 16
PIX = 256
BLOCK = 128
WIN_COLS = 8


harm_zero = 0.28209479177387814
harm_one = 0.4886025119029199
harm_two = (
    1.0925484305920792,
    -1.0925484305920792,
    0.31539156525252005,
    -1.0925484305920792,
    0.5462742152960396,
)
harm_three = (
    -0.5900435899266435,
    2.890611442640554,
    -0.4570457994644658,
    0.3731763325901154,
    -0.4570457994644658,
    1.445305721320277,
    -0.5900435899266435,
)
learn_rate = 0.05
beta_first = 0.9
beta_second = 0.999
adam_eps = 1e-08
blur_add = 0.3


def rotation(real_part, axis_one, axis_two, axis_three):
    inverse = lax.rsqrt(
        real_part * real_part + axis_one * axis_one + axis_two * axis_two + axis_three * axis_three
    )
    real_unit = real_part * inverse
    unit_one = axis_one * inverse
    unit_two = axis_two * inverse
    unit_three = axis_three * inverse
    return (
        (
            1.0 - 2.0 * (unit_two * unit_two + unit_three * unit_three),
            2.0 * (unit_one * unit_two - real_unit * unit_three),
            2.0 * (unit_one * unit_three + real_unit * unit_two),
        ),
        (
            2.0 * (unit_one * unit_two + real_unit * unit_three),
            1.0 - 2.0 * (unit_one * unit_one + unit_three * unit_three),
            2.0 * (unit_two * unit_three - real_unit * unit_one),
        ),
        (
            2.0 * (unit_one * unit_three - real_unit * unit_two),
            2.0 * (unit_two * unit_three + real_unit * unit_one),
            1.0 - 2.0 * (unit_one * unit_one + unit_two * unit_two),
        ),
    )


def harmonics(first_dir, second_dir, third_dir):
    sq_first = first_dir * first_dir
    sq_second = second_dir * second_dir
    sq_third = third_dir * third_dir
    return [
        harm_zero,
        -harm_one * second_dir,
        harm_one * third_dir,
        -harm_one * first_dir,
        harm_two[0] * first_dir * second_dir,
        harm_two[1] * second_dir * third_dir,
        harm_two[2] * (2.0 * sq_third - sq_first - sq_second),
        harm_two[3] * first_dir * third_dir,
        harm_two[4] * (sq_first - sq_second),
        harm_three[0] * second_dir * (3.0 * sq_first - sq_second),
        harm_three[1] * first_dir * second_dir * third_dir,
        harm_three[2] * second_dir * (4.0 * sq_third - sq_first - sq_second),
        harm_three[3] * third_dir * (2.0 * sq_third - 3.0 * sq_first - 3.0 * sq_second),
        harm_three[4] * first_dir * (4.0 * sq_third - sq_first - sq_second),
        harm_three[5] * third_dir * (sq_first - sq_second),
        harm_three[6] * first_dir * (sq_first - 3.0 * sq_second),
    ]


def project(raw, camera):
    camera_turn = rotation(camera[0], camera[1], camera[2], camera[3])
    shift_vec = (camera[4], camera[5], camera[6])
    focal_x = camera[7]
    focal_y = camera[8]
    position = (raw[0], raw[1], raw[2])
    viewed = [
        camera_turn[across][0] * position[0]
        + camera_turn[across][1] * position[1]
        + camera_turn[across][2] * position[2]
        + shift_vec[across]
        for across in range(3)
    ]
    inverse = 1.0 / viewed[2]
    mean_x = focal_x * viewed[0] * inverse + camera[9]
    mean_y = focal_y * viewed[1] * inverse + camera[10]
    gauss_turn = rotation(raw[6], raw[7], raw[8], raw[9])
    stretch = [jnp.exp(raw[3 + column]) for column in range(3)]
    jac_xx = focal_x * inverse
    jac_xz = -focal_x * viewed[0] * inverse * inverse
    jac_yy = focal_y * inverse
    jac_yz = -focal_y * viewed[1] * inverse * inverse
    leading_x = [
        jac_xx * camera_turn[0][column] + jac_xz * camera_turn[2][column] for column in range(3)
    ]
    leading_y = [
        jac_yy * camera_turn[1][column] + jac_yz * camera_turn[2][column] for column in range(3)
    ]
    axes_x = [
        (
            leading_x[0] * gauss_turn[0][column]
            + leading_x[1] * gauss_turn[1][column]
            + leading_x[2] * gauss_turn[2][column]
        )
        * stretch[column]
        for column in range(3)
    ]
    axes_y = [
        (
            leading_y[0] * gauss_turn[0][column]
            + leading_y[1] * gauss_turn[1][column]
            + leading_y[2] * gauss_turn[2][column]
        )
        * stretch[column]
        for column in range(3)
    ]
    cov_xx = axes_x[0] * axes_x[0] + axes_x[1] * axes_x[1] + axes_x[2] * axes_x[2] + blur_add
    cov_xy = axes_x[0] * axes_y[0] + axes_x[1] * axes_y[1] + axes_x[2] * axes_y[2]
    cov_yy = axes_y[0] * axes_y[0] + axes_y[1] * axes_y[1] + axes_y[2] * axes_y[2] + blur_add
    determ = cov_xx * cov_yy - cov_xy * cov_xy
    opacity = jax.nn.sigmoid(raw[10])
    camera_eye = [
        -(
            camera_turn[0][column] * shift_vec[0]
            + camera_turn[1][column] * shift_vec[1]
            + camera_turn[2][column] * shift_vec[2]
        )
        for column in range(3)
    ]
    offset = [position[column] - camera_eye[column] for column in range(3)]
    length = lax.rsqrt(offset[0] * offset[0] + offset[1] * offset[1] + offset[2] * offset[2])
    harmonic_terms = harmonics(offset[0] * length, offset[1] * length, offset[2] * length)
    colours = []
    for channel in range(3):
        total = 0.5 + jnp.zeros_like(opacity)
        for harmonic in range(16):
            total = total + raw[11 + 16 * channel + harmonic] * harmonic_terms[harmonic]
        colours.append(total)
    return [mean_x, mean_y, cov_yy / determ, -cov_xy / determ, cov_xx / determ, opacity] + colours


F32 = jnp.float32
BF16 = jnp.bfloat16
PARAMS = 59
ROWS = 64
LOG2E = 1.4426950408889634
MIB = 1 << 20
MIXED = 8


def iota(shape, dim):
    return lax.broadcasted_iota(jnp.int32, shape, dim)


def parts_of(value, count):
    parts = []
    for _ in range(count):
        part = value.astype(BF16)
        parts.append(part)
        value = value - part.astype(F32)
    return parts


def mm(left, right, dims):
    return lax.dot_general(left, right, (dims, ((), ())), preferred_element_type=F32)


def stacked(rows, width):
    sub = iota((8, width), 0)
    out = jnp.zeros((8, width), F32)
    for place, row in enumerate(rows):
        out = jnp.where(sub == place, jnp.broadcast_to(row, (8, width)), out)
    return out


def seen_columns(ids_ref, first, width):
    row = jnp.concatenate(
        [ids_ref[first + step : first + step + 1, :] for step in range(width // 64)], axis=1
    )
    return (iota((1024, width), 0) == row).astype(BF16)


def camera_arrays(cameras_ref):
    view = 2 * iota((8, 128), 0) + (iota((8, 128), 1) >= 64).astype(jnp.int32)
    masks = [view == index for index in range(16)]
    arrays = []
    for field in range(11):
        array = jnp.full((8, 128), cameras_ref[0, field], F32)
        for index in range(1, 16):
            array = jnp.where(masks[index], cameras_ref[index, field], array)
        arrays.append(array)
    return arrays


def raw_rows(picked_ref):
    return [picked_ref[pl.ds(row, 8, stride=ROWS), :] for row in range(PARAMS)]


def pick_rows(ids_ref, params_ref, split, picked_ref):
    for place, part in enumerate(parts_of(params_ref[...], 3)):
        split[place * ROWS : place * ROWS + PARAMS, :] = part
    for pair in range(4):
        onehot = seen_columns(ids_ref, pair * 4, 256)
        three = mm(split[...], onehot, ((1,), (0,)))
        picked = three[0:ROWS] + three[ROWS : 2 * ROWS] + three[2 * ROWS :]
        picked_ref[pair * 128 : pair * 128 + ROWS, :] = picked[:, :128]
        picked_ref[pair * 128 + ROWS : pair * 128 + 2 * ROWS, :] = picked[:, 128:]


def project_kernel(place_ref, ids_ref, cameras_ref, params_ref, send_ref, split, swap, picked_ref):
    pick_rows(ids_ref, params_ref, split, picked_ref)
    values = project(raw_rows(picked_ref), camera_arrays(cameras_ref))
    for place in range(8):
        swap[place * 8 : place * 8 + 8, :] = values[place]
    low = iota((8, 128), 1) < 64
    for pair in range(8):
        main = swap[pl.ds(pair, 8, stride=8), :]
        last = jnp.broadcast_to(values[8][pair : pair + 1, :], (8, 128))
        send_ref[2 * pair] = jnp.where(low, main, pltpu.roll(last, 64, 1))
        send_ref[2 * pair + 1] = jnp.where(low, pltpu.roll(main, 64, 1), last)


def unpack_pair(even, odd):
    low = iota((8, 128), 1) < 64
    main = jnp.where(low, even, pltpu.roll(odd, 64, 1))
    last = jnp.where(low, pltpu.roll(even, 64, 1), odd)
    return main, last[0:1, :]


def spread_kernel(arrived_ref, out_ref):
    for pair in range(8):
        main, last = unpack_pair(arrived_ref[2 * pair], arrived_ref[2 * pair + 1])
        for peer in range(16):
            out_ref[peer, pair * 8 : pair * 8 + 8, :] = main
            out_ref[peer, 64 + pair : 65 + pair, :] = last


def as_columns(row):
    return jnp.transpose(jnp.broadcast_to(row.astype(F32), (128, 128))).astype(jnp.int32)


def columns_kernel(
    after_ref, ids_ref, cameras_ref, params_ref, columns_ref, rows_ref, split, picked_ref
):
    pick_rows(ids_ref, params_ref, split, picked_ref)
    for place, array in enumerate(raw_rows(picked_ref) + camera_arrays(cameras_ref)):
        rows_ref[place] = array
    for pair in range(8):
        row = jnp.concatenate(
            [ids_ref[2 * pair : 2 * pair + 1, :], ids_ref[2 * pair + 1 : 2 * pair + 2, :]], axis=1
        )
        column = as_columns(row)
        for start in range(0, 1024, 128):
            hot = (iota((128, 128), 1) + start == column).astype(BF16)
            columns_ref[pair * 128 : pair * 128 + 128, start : start + 128] = hot


def prepare_kernel(
    after_ref,
    lists_ref,
    onehot_ref,
    turned_ref,
    lanes_ref,
    groups_ref,
):

    turn = (iota((128, 1024), 0) == (iota((128, 1024), 1) >> 3)).astype(BF16)
    pick_block = iota((8, 1024), 0) == (iota((8, 1024), 1) & 7)
    for tile in range(2):
        blocks = [lists_ref[0, tile : tile + 1, start : start + 128] for start in range(0, 1024, 128)]
        low_part = stacked([(row & 127).astype(F32) for row in blocks], 128)
        high_part = stacked([(row >> 7).astype(F32) for row in blocks], 128)
        low_part = mm(low_part.astype(BF16), turn, ((1,), (0,)))
        high_part = mm(high_part.astype(BF16), turn, ((1,), (0,)))
        low_row = jnp.sum(jnp.where(pick_block, low_part, 0.0), axis=0, keepdims=True)
        high_row = jnp.sum(jnp.where(pick_block, high_part, 0.0), axis=0, keepdims=True)
        low_row = low_row.astype(jnp.int32)
        high_row = high_row.astype(jnp.int32)
        lane_index = ((high_row >> 3) & 1) * 128 + low_row
        span = slice(tile * 1024, tile * 1024 + 1024)
        onehot_ref[:, span] = (iota((256, 1024), 0) == lane_index).astype(BF16)
        for start in range(0, 1024, 128):
            column = as_columns(lane_index[:, start : start + 128])
            lanes = iota((128, 128), 1)
            rows = slice(tile * 1024 + start, tile * 1024 + start + 128)
            turned_ref[rows, 0:128] = (lanes == column).astype(BF16)
            turned_ref[rows, 128:256] = (lanes + 128 == column).astype(BF16)
        lanes_ref[:, span] = low_row
        groups_ref[:, span] = high_row


def render_kernel(
    place_ref,
    counts_ref,
    onehot,
    turned,
    lanes_of,
    chosen,
    targets_ref,
    everyone_ref,
    image_ref,
    out_ref,
    picked,
    alphas,
    weights,
    shades,
    summed,
    table,
):
    count = 2048
    for half in range(MIXED // 2):
        for side in range(2):
            lanes = slice(side * 128, side * 128 + 128)
            main = parts_of(everyone_ref[2 * half + side, 0:64, :], 3)
            last = parts_of(everyone_ref[2 * half + side, 64:72, :], 3)
            for part in range(3):
                table[part, half * 64 : half * 64 + 64, lanes] = main[part]
                start = MIXED * 32 + half * 8
                table[part, start : start + 8, lanes] = last[part]

    def gather_chunk(chunk, carry):
        lanes = pl.ds(chunk * 256, 256)
        hot = onehot[:, lanes]
        found = mm(table[0], hot, ((1,), (0,)))
        found = found + mm(table[1], hot, ((1,), (0,)))
        found = found + mm(table[2], hot, ((1,), (0,)))
        both = jnp.broadcast_to(chosen[:, lanes], (8, 256))
        pair = (both >> 4) * 8 + (both & 7)
        sub = iota((8, 256), 0)
        zero = jnp.zeros((8, 256), F32)
        main = [zero, zero]
        last = zero
        for half in range(MIXED // 2):
            for place in range(8):
                start = half * 64 + place * 8
                main[place % 2] = jnp.where(
                    pair == half * 8 + place, found[start : start + 8, :], main[place % 2]
                )
            start = MIXED * 32 + half * 8
            last = jnp.where(pair == half * 8 + sub, found[start : start + 8, :], last)
        main = main[0] + main[1]
        sub = iota((8, 128), 0)
        zero = jnp.zeros((8, 128), F32)
        for side in range(2):
            cut = slice(side * 128, side * 128 + 128)
            lanes = pl.ds(chunk * 256 + side * 128, 128)
            lane = jnp.broadcast_to(lanes_of[:, lanes], (8, 128))
            group = both[:, cut]
            chains = [main[:, cut], zero, zero, zero]
            ends = [last[:, cut], zero]
            for peer in range(MIXED, 16):
                for place in range(8):
                    value = jnp.take_along_axis(
                        everyone_ref[peer, place * 8 : place * 8 + 8, :], lane, axis=1
                    )
                    chain = place % 4
                    chains[chain] = jnp.where(group == peer * 8 + place, value, chains[chain])
                value = jnp.take_along_axis(everyone_ref[peer, 64:72, :], lane, axis=1)
                ends[peer % 2] = jnp.where(group == peer * 8 + sub, value, ends[peer % 2])
            picked[0:8, lanes] = (chains[0] + chains[1]) + (chains[2] + chains[3])
            picked[8:16, lanes] = jnp.broadcast_to(
                jnp.sum(ends[0] + ends[1], axis=0, keepdims=True), (8, 128)
            )
        return carry

    for chunk in range(8):
        gather_chunk(chunk, 0)

    pixel = iota((8, PIX), 1)
    pixel_x = (pixel & (SIDE - 1)).astype(F32) + (0.5 - SIDE / 2)
    pixel_y = (pixel >> 4).astype(F32) + (0.5 - SIDE / 2)
    sub = iota((8, PIX), 0)
    basis = jnp.where(sub == 0, 1.0, 0.0)
    for place, row in enumerate(
        [pixel_x, pixel_y, pixel_x * pixel_x, pixel_x * pixel_y, pixel_y * pixel_y]
    ):
        basis = jnp.where(sub == place + 1, row, basis)
    blank = jnp.zeros((8, PIX), F32)
    basis_three = jnp.concatenate([basis, basis, basis, blank], axis=0).astype(BF16)
    basis_once = jnp.concatenate([basis, blank], axis=0).astype(BF16)

    def rows_of(tile):
        span = slice(tile * 1024, tile * 1024 + 1024)
        held = picked[:, span]
        global_tile = place_ref[0] * 2 + tile
        centre_x = (global_tile % WIN_COLS * SIDE + SIDE // 2).astype(F32)
        centre_y = (global_tile // WIN_COLS * SIDE + SIDE // 2).astype(F32)
        rows = [held[place : place + 1, :] for place in range(9)]
        rows[0] = rows[0] - centre_x
        rows[1] = rows[1] - centre_y
        return rows

    block = iota((1, 1024), 1) & 7
    blank_row = jnp.zeros((8, 1024), F32)
    colour_rows = []
    for tile in range(2):
        mean_x, mean_y, con_a, con_b, con_c, opacity, *colour = rows_of(tile)
        live = block < counts_ref[0, tile]
        slope_x = con_a * mean_x + con_b * mean_y
        slope_y = con_b * mean_x + con_c * mean_y
        scale = -0.5 * LOG2E
        level = scale * (slope_x * mean_x + slope_y * mean_y) + jnp.log(opacity) * LOG2E
        terms = [
            jnp.where(live, level, -1000.0),
            jnp.where(live, (-2.0 * scale) * slope_x, 0.0),
            jnp.where(live, (-2.0 * scale) * slope_y, 0.0),
            jnp.where(live, scale * con_a, 0.0),
            jnp.where(live, (2.0 * scale) * con_b, 0.0),
            jnp.where(live, scale * con_c, 0.0),
        ]
        split = [part.astype(F32) for part in parts_of(stacked(terms, 1024), 3)]
        coefficients = jnp.concatenate(split + [blank_row], axis=0).astype(BF16)
        alphas[tile] = mm(coefficients, basis_three, ((0,), (0,)))
        colour_rows.append(stacked(colour, 1024))

    steps = 8

    def advance(outer, held):
        held = list(held)
        for inner in range(steps):
            start = pl.multiple_of((outer * steps + inner) * 8, 8)
            for tile in range(2):
                alpha = jnp.exp2(alphas[tile, pl.ds(start, 8), :])
                weight = alpha * held[tile]
                held[tile] = held[tile] * (1.0 - alpha)
                weights[tile, pl.ds(start, 8), :] = weight
        return tuple(held)

    ones = jnp.ones((8, PIX), F32)
    left = lax.fori_loop(0, 128 // steps, advance, (ones, ones))

    behind = []
    ahead = []
    blame = []
    sub_wide = iota((8, 1024), 0)
    block_wide = iota((8, 1024), 1) & 7
    for tile in range(2):
        colour = colour_rows[tile]
        separate = []
        for channel in range(3):
            row = jnp.broadcast_to(colour[channel : channel + 1, :], (8, 1024))
            separate.append(jnp.where(sub_wide == block_wide, row, 0.0))
        fine, rough = parts_of(jnp.concatenate(separate, axis=0), 2)
        both = jnp.concatenate([fine.astype(F32), rough.astype(F32)], axis=0).astype(BF16)
        first_part, second_part = parts_of(weights[tile], 2)
        sums = mm(both, first_part, ((1,), (0,))) + mm(both, second_part, ((1,), (0,)))
        passed = left[tile]
        total = passed
        for shift in (1, 2, 4):
            total = total * jnp.where(sub >= shift, pltpu.roll(total, shift, 0), 1.0)
        before = jnp.where(sub >= 1, pltpu.roll(total, 1, 0), 1.0)
        ahead.append(before)
        value = jnp.zeros((8, PIX), F32)
        slopes = []
        for channel in range(3):
            own = sums[channel * 8 : channel * 8 + 8, :]
            own = own + sums[24 + channel * 8 : 32 + channel * 8, :]
            image = jnp.sum(own * before, axis=0, keepdims=True)
            lanes = slice(tile * PIX, tile * PIX + PIX)
            image_ref[channel, :, lanes] = image
            slope = 2.0 * (image - targets_ref[channel, :, lanes])
            slopes.append(slope)
            value = value + slope * own
        factor = passed
        for shift in (1, 2, 4):
            inside = sub < 8 - shift
            value = value + factor * jnp.where(inside, pltpu.roll(value, 8 - shift, 0), 0.0)
            factor = factor * jnp.where(inside, pltpu.roll(factor, 8 - shift, 0), 1.0)
        behind.append(jnp.where(sub < 7, pltpu.roll(value, 7, 0), 0.0))
        slope_parts = [part.astype(F32) for part in parts_of(stacked(slopes, PIX), 3)]
        colour_parts = [part.astype(F32) for part in parts_of(colour, 3)]
        pairs = [(0, 0), (0, 1), (1, 0), (1, 1), (0, 2), (2, 0)]
        left_side = jnp.concatenate([colour_parts[a] for a, _ in pairs], axis=0).astype(BF16)
        right_side = jnp.concatenate([slope_parts[b] for _, b in pairs], axis=0).astype(BF16)
        shades[tile] = mm(left_side, right_side, ((0,), (0,)))
        blame.append(jnp.concatenate(slope_parts[:2], axis=0).astype(BF16))

    def retreat(outer, held):
        held = list(held)
        for inner in range(steps):
            start = pl.multiple_of((127 - (outer * steps + inner)) * 8, 8)
            for tile in range(2):
                alpha = jnp.exp2(alphas[tile, pl.ds(start, 8), :])
                weight = weights[tile, pl.ds(start, 8), :] * ahead[tile]
                shade = shades[tile, pl.ds(start, 8), :]
                shades[tile, pl.ds(start, 8), :] = weight * (shade - held[tile])
                held[tile] = held[tile] * (1.0 - alpha) + alpha * shade
                weights[tile, pl.ds(start, 8), :] = weight
        return tuple(held)

    lax.fori_loop(0, 128 // steps, retreat, tuple(behind))

    for tile in range(2):
        moments = sum(
            mm(basis_once, part, ((1,), (1,))) for part in parts_of(shades[tile], 2)
        )
        tints = sum(mm(blame[tile], part, ((1,), (1,))) for part in parts_of(weights[tile], 2))
        tints = tints[0:8, :] + tints[8:16, :]
        mean_x, mean_y, con_a, con_b, con_c, opacity, *_ = rows_of(tile)
        sum_one, sum_x, sum_y, sum_xx, sum_xy, sum_yy = [
            moments[place : place + 1, :] for place in range(6)
        ]
        near_x = sum_x - mean_x * sum_one
        near_y = sum_y - mean_y * sum_one
        near_xx = sum_xx - mean_x * (sum_x + near_x)
        near_xy = sum_xy - mean_x * sum_y - mean_y * near_x
        near_yy = sum_yy - mean_y * (sum_y + near_y)
        grads = [
            con_a * near_x + con_b * near_y,
            con_b * near_x + con_c * near_y,
            -0.5 * near_xx,
            -near_xy,
            -0.5 * near_yy,
            sum_one / opacity,
            tints[0:1, :],
            tints[1:2, :],
        ]
        span = slice(tile * 1024, tile * 1024 + 1024)
        picked[0:8, span] = stacked(grads, 1024)
        picked[8:16, span] = jnp.broadcast_to(tints[2:3, :], (8, 1024))

    wide = 512
    for chunk in range(count // wide):
        lanes = slice(chunk * wide, chunk * wide + wide)
        group = chosen[:, lanes]
        group = jnp.broadcast_to((group >> 4) * 8 + (group & 7), (8, wide))
        sub = iota((8, wide), 0)
        main = [part.astype(F32) for part in parts_of(picked[0:8, lanes], 2)]
        last = [part.astype(F32) for part in parts_of(picked[8:16, lanes], 2)]
        sides = []
        for part in range(2):
            rows = [jnp.where(group == place, main[part], 0.0) for place in range(64)]
            rows += [jnp.where(group == half * 8 + sub, last[part], 0.0) for half in range(8)]
            sides += [
                jnp.concatenate(rows[place : place + 2], axis=0).astype(BF16)
                for place in range(0, 72, 2)
            ]
        total = mm(jnp.concatenate(sides, axis=0), turned[lanes, :], ((1,), (0,)))
        total = total[0:576] + total[576:]
        if chunk == 0:
            summed[...] = total
        elif chunk < count // wide - 1:
            summed[...] = summed[...] + total
        else:
            total = summed[...] + total
    for half in range(8):
        for side in range(2):
            lanes = slice(side * 128, side * 128 + 128)
            out_ref[2 * half + side, 0:64, :] = total[half * 64 : half * 64 + 64, lanes]
            out_ref[2 * half + side, 64:72, :] = total[512 + half * 8 : 520 + half * 8, lanes]


def merge_kernel(arrived_ref, send_ref):
    low = iota((8, 128), 1) < 64
    total = arrived_ref[0]
    for peer in range(1, 16):
        total = total + arrived_ref[peer]
    for pair in range(8):
        main = total[pair * 8 : pair * 8 + 8, :]
        last = jnp.broadcast_to(total[64 + pair : 65 + pair, :], (8, 128))
        send_ref[2 * pair] = jnp.where(low, main, pltpu.roll(last, 64, 1))
        send_ref[2 * pair + 1] = jnp.where(low, pltpu.roll(main, 64, 1), last)


def update_kernel(
    onehot_ref,
    spread_ref,
    arrived_ref,
    params_ref,
    first_ref,
    second_ref,
    new_params_ref,
    new_first_ref,
    new_second_ref,
    swap,
    turned,
    stage,
    leaving,
):
    lasts = []
    for pair in range(8):
        main, last = unpack_pair(arrived_ref[2 * pair], arrived_ref[2 * pair + 1])
        swap[pair * 8 : pair * 8 + 8, :] = main
        lasts.append(last)
    slopes = [swap[pl.ds(place, 8, stride=8), :] for place in range(8)]
    sub = iota((8, 128), 0)
    final = jnp.zeros((8, 128), F32)
    for pair in range(8):
        final = jnp.where(sub == pair, jnp.broadcast_to(lasts[pair], (8, 128)), final)
    slopes.append(final)
    arrays = [spread_ref[place] for place in range(PARAMS + 11)]
    cameras = arrays[PARAMS:]
    _, pullback = jax.vjp(lambda source: project(source, cameras), arrays[:PARAMS])
    (raw_grads,) = pullback(slopes)
    for row in range(PARAMS):
        turned[pl.ds(row, 8, stride=ROWS), :] = raw_grads[row]
    for row in range(PARAMS, ROWS):
        turned[pl.ds(row, 8, stride=ROWS), :] = jnp.ones((8, 128), F32)
    wide = jnp.concatenate([turned[pair * ROWS : pair * ROWS + ROWS, :] for pair in range(8)], axis=1)
    split = [part.astype(F32) for part in parts_of(wide, 3)]
    three = mm(jnp.concatenate(split, axis=0).astype(BF16), onehot_ref[...], ((1,), (0,)))
    summed = three[0:ROWS] + three[ROWS : 2 * ROWS] + three[2 * ROWS :]
    seen = summed[PARAMS : PARAMS + 1, :] > 0.5
    outs = (new_params_ref, new_first_ref, new_second_ref)
    copies = []
    for place, start in enumerate(range(0, PARAMS, 16)):
        rows = slice(start, min(start + 16, PARAMS))
        grad = summed[rows, :]
        first = first_ref[rows, :]
        second = second_ref[rows, :]
        params = params_ref[rows, :]
        moved_first = beta_first * first + (1.0 - beta_first) * grad
        moved_second = beta_second * second + (1.0 - beta_second) * grad * grad
        moved_params = params - learn_rate * moved_first / (jnp.sqrt(moved_second) + adam_eps)
        values = (
            jnp.where(seen, moved_params, params),
            jnp.where(seen, moved_first, first),
            jnp.where(seen, moved_second, second),
        )
        for kind in range(3):
            stage[kind, rows, :] = values[kind]
            copy = pltpu.make_async_copy(
                stage.at[kind, rows, :], outs[kind].at[rows, :], leaving.at[kind, place]
            )
            copy.start()
            copies.append(copy)
    for copy in copies:
        copy.wait()


SMEM = pl.BlockSpec(memory_space=pltpu.SMEM)
VMEM = pl.BlockSpec(memory_space=pltpu.VMEM)


def f32_shape(*shape):
    return jax.ShapeDtypeStruct(shape, F32)


def project_call(place, visible, cameras, params):
    return pl.pallas_call(
        project_kernel,
        out_shape=f32_shape(16, 8, 128),
        in_specs=[SMEM, VMEM, SMEM, VMEM],
        out_specs=VMEM,
        scratch_shapes=[
            pltpu.VMEM((192, 1024), BF16),
            pltpu.VMEM((64, 128), F32),
            pltpu.VMEM((512, 128), F32),
        ],
        compiler_params=pltpu.CompilerParams(vmem_limit_bytes=12 * MIB),
        name="project",
    )(place, visible, cameras, params)


def spread_call(arrived):
    return pl.pallas_call(
        spread_kernel,
        out_shape=f32_shape(16, 72, 128),
        in_specs=[VMEM],
        out_specs=VMEM,
        compiler_params=pltpu.CompilerParams(vmem_limit_bytes=6 * MIB),
        name="spread",
    )(arrived)


def columns_call(after, visible, cameras, params):
    return pl.pallas_call(
        columns_kernel,
        out_shape=(jax.ShapeDtypeStruct((1024, 1024), BF16), f32_shape(PARAMS + 11, 8, 128)),
        in_specs=[pl.BlockSpec(memory_space=pl.ANY), VMEM, SMEM, VMEM],
        out_specs=(VMEM, VMEM),
        scratch_shapes=[pltpu.VMEM((192, 1024), BF16), pltpu.VMEM((512, 128), F32)],
        compiler_params=pltpu.CompilerParams(vmem_limit_bytes=12 * MIB),
        name="columns",
    )(after, visible, cameras, params)


def prepare_call(after, lists):
    return pl.pallas_call(
        prepare_kernel,
        out_shape=(
            jax.ShapeDtypeStruct((256, 2048), BF16),
            jax.ShapeDtypeStruct((2048, 256), BF16),
            jax.ShapeDtypeStruct((1, 2048), jnp.int32),
            jax.ShapeDtypeStruct((1, 2048), jnp.int32),
        ),
        in_specs=[pl.BlockSpec(memory_space=pl.ANY), VMEM],
        out_specs=(VMEM, VMEM, VMEM, VMEM),
        compiler_params=pltpu.CompilerParams(vmem_limit_bytes=16 * MIB),
        name="prepare",
    )(after, lists)


def render_call(place, counts, onehot, turned, lanes, groups, targets, everyone):
    return pl.pallas_call(
        render_kernel,
        out_shape=(f32_shape(3, 1, 512), f32_shape(16, 72, 128)),
        in_specs=[SMEM, SMEM, VMEM, VMEM, VMEM, VMEM, VMEM, VMEM],
        out_specs=(VMEM, VMEM),
        scratch_shapes=[
            pltpu.VMEM((16, 2048), F32),
            pltpu.VMEM((2, 1024, 256), F32),
            pltpu.VMEM((2, 1024, 256), F32),
            pltpu.VMEM((2, 1024, 256), F32),
            pltpu.VMEM((576, 256), F32),
            pltpu.VMEM((3, MIXED * 36, 256), BF16),
        ],
        compiler_params=pltpu.CompilerParams(vmem_limit_bytes=24 * MIB),
        name="render",
    )(place, counts, onehot, turned, lanes, groups, targets, everyone)


def merge_call(arrived):
    return pl.pallas_call(
        merge_kernel,
        out_shape=f32_shape(16, 8, 128),
        in_specs=[VMEM],
        out_specs=VMEM,
        compiler_params=pltpu.CompilerParams(vmem_limit_bytes=6 * MIB),
        name="merge",
    )(arrived)


def update_call(onehot, spread, arrived, params, first, second):
    shape = f32_shape(*params.shape)
    return pl.pallas_call(
        update_kernel,
        out_shape=(shape, shape, shape),
        in_specs=[VMEM] * 6,
        out_specs=(pl.BlockSpec(memory_space=pl.ANY),) * 3,
        scratch_shapes=[
            pltpu.VMEM((64, 128), F32),
            pltpu.VMEM((512, 128), F32),
            pltpu.VMEM((3, PARAMS, 1024), F32),
            pltpu.SemaphoreType.DMA((3, 4)),
        ],
        compiler_params=pltpu.CompilerParams(vmem_limit_bytes=16 * MIB),
        name="update",
    )(onehot, spread, arrived, params, first, second)


def kept(array):
    return pltpu.with_memory_space_constraint(array, pltpu.VMEM)


def exchanged(array, axis):
    return kept(lax.all_to_all(array, axis, 0, 0, tiled=True))


def shards(params, first, second, visible, cameras, tile_lists, tile_blocks, targets):
    place = lax.axis_index("tile").astype(jnp.int32).reshape(1)
    held = [
        pltpu.with_memory_space_constraint(array, pltpu.HBM)
        for array in (visible, cameras, params)
    ]
    outgoing = project_call(place, *held)
    everyone = exchanged(spread_call(exchanged(outgoing, "view")), "tile")
    onehot, turned, lanes, groups = [
        kept(table) for table in prepare_call(everyone, kept(tile_lists))
    ]
    image, sums = render_call(
        place,
        tile_blocks,
        onehot,
        turned,
        lanes,
        groups,
        jnp.transpose(targets, (1, 0, 2)),
        everyone,
    )
    merged = merge_call(exchanged(sums, "tile"))
    returned = exchanged(merged, "view")
    columns, rows = columns_call(merged, visible, cameras, kept(params))
    new_params, new_first, new_second = update_call(
        kept(columns), kept(rows), returned, kept(params), kept(first), kept(second)
    )
    return (new_params, new_first, new_second, jnp.transpose(image, (1, 0, 2)))


def solution(mesh):
    in_specs = (
        P(None, ("view", "tile")),
        P(None, ("view", "tile")),
        P(None, ("view", "tile")),
        P(None, ("view", "tile")),
        P(),
        P("view", "tile", None),
        P("view", "tile"),
        P("view", None, "tile"),
    )
    out_specs = (
        P(None, ("view", "tile")),
        P(None, ("view", "tile")),
        P(None, ("view", "tile")),
        P("view", None, "tile"),
    )
    return jax.shard_map(shards, mesh=mesh, in_specs=in_specs, out_specs=out_specs, check_vma=False)
```
